32 devices in a mesh: lon: 2 (over x), lat: 4 (over y, core), mem: 4 (over z).
Axes of the slice: x: 2, y: 2, z: 4, core: 2. Of those that a mesh axis runs over, the one named last changes fastest.
Arguments:
- anomalies: bfloat16 [32, 4, 128, 512], P('mem', None, 'lon', 'lat'), may hold values from -6 to 6
- spread: float32 [4, 128, 512], P(None, 'lon', 'lat'), may hold values from 0.5 to 2
- obs_index: int32 [2, 4, 2048], P('lon', 'lat'), may hold values from 0 to 32767
- innovation: float32 [2, 4, 2048], P('lon', 'lat'), may hold values from -6 to 6
- obs_weight: float32 [2, 4, 2048], P('lon', 'lat'), may hold values from 0.5 to 8
- band_width: int32 [2, 4], replicated, may hold values from 6 to 12, as said below
Outputs:
- control_ens: float32 [32, 4, 128, 512], P('mem', None, 'lon', 'lat')
- control_static: float32 [4, 128, 512], P(None, 'lon', 'lat')
The draws below stay inside these ranges and needn't reach their ends.
Inputs may be any that keep to these rules, and one draw needn't show every extreme that they name: `obs_index`: A cell of the tile's 4 x 64 x 128 block, flattened with latitude fastest. `band_width`: in each of the two rows some level has exactly 12.
All inputs are finite; a program needn't handle non-finite values.
Results may differ from the reference program's by a relative error of at most 0.0003.
Values may be sent and summed in bfloat16 or wider, within the bound.
A program may use at most 64 MiB of HBM per device.

```python
import math
import jax
import jax.numpy as jnp
from jax import lax

LON_DEV = 64
LAT_DEV = 128
LEVELS = 4
OBS_DEV = 2048
BAND = 12
ITERS = 2
MEMBERS = 32
NLON = 128
NLAT = 512
N_LON = 2
N_LAT = 4


def draw_band_width(key, part):
    lower = jax.random.randint(jax.random.fold_in(key, 11), (2, LEVELS), BAND // 2, BAND + 1)
    widest = jax.random.randint(jax.random.fold_in(key, 12), (2, 1), 0, LEVELS)
    level_iota = jnp.arange(LEVELS, dtype=jnp.int32)[None, :]
    return jnp.where(level_iota == widest, BAND, lower).astype(jnp.int32)


def with_ends(values, rng, least, largest):
    shape = values.shape
    index_at = [jax.random.randint(jax.random.fold_in(rng, axis), (), 0, shape[axis]) for axis in range(len(shape))]
    values = values.at[tuple(index_at)].set(least)
    longest = shape.index(max(shape))
    index_at[longest] = (index_at[longest] + 1) % shape[longest]
    return values.at[tuple(index_at)].set(largest)


def shard_levels(stream_key, dims, pieces, smallest, high):
    def one(position, blocks):
        draws = jax.random.uniform(jax.random.fold_in(jax.random.fold_in(stream_key, 6), position), (blocks,), jnp.float32, smallest / len(pieces), high / len(pieces))
        return jnp.repeat(jnp.exp(draws), dims[position] // blocks).reshape((-1,) + (1,) * (len(dims) - position - 1))

    loudness = one(*pieces[0])
    for cut in pieces[1:]:
        loudness = loudness * one(*cut)
    return loudness


def noise(key, dims, scale, reach, split=(), held_as=jnp.bfloat16):
    drawn = jax.random.normal(key, dims, jnp.float32) * scale
    if len(split) > 0:
        drawn = shard_levels(key, dims, split, -0.22, 0.18) * drawn
    return jnp.clip(drawn, min=-reach, max=reach).astype(held_as)


def setup_inputs(seed: int = 0) -> dict:
    streams_of = jax.random.split(jax.random.key(seed), 7)
    return {
        "anomalies": noise(streams_of[0], (MEMBERS, LEVELS, NLON, NLAT), 1.0, 6.0, ((0, 4), (2, 2), (3, 4))),
        "spread": jnp.clip(jnp.exp(math.log(2.0) - 1.3862944 * jax.random.uniform(streams_of[1], (LEVELS, NLON, NLAT), jnp.float32) ** shard_levels(streams_of[1], (LEVELS, NLON, NLAT), ((1, 2), (2, 4)), -0.2, 0.2)), 0.5, 2.0),
        "obs_index": with_ends(jax.random.randint(streams_of[2], (N_LON, N_LAT, OBS_DEV), 0, LEVELS * LON_DEV * LAT_DEV), jax.random.fold_in(streams_of[2], 1), 0, (LEVELS * LON_DEV * LAT_DEV) - 1).astype(jnp.int32),
        "innovation": noise(streams_of[3], (N_LON, N_LAT, OBS_DEV), 1.0, 6.0, ((0, 2), (1, 4)), jnp.float32),
        "obs_weight": jnp.clip(jnp.exp(math.log(8.0) - 2.7725887 * jax.random.uniform(streams_of[4], (N_LON, N_LAT, OBS_DEV), jnp.float32) ** shard_levels(streams_of[4], (N_LON, N_LAT, OBS_DEV), ((0, 2), (1, 4)), -0.2, 0.2)), 0.5, 8.0),
        "band_width": draw_band_width(jax.random.fold_in(streams_of[6], 71), 0),
    }


hybrid_ens = 0.75
hybrid_static = 0.25

def band_table(band_width):
    offsets = jnp.arange(-BAND, BAND + 1).astype(jnp.float32)
    widths = band_width.astype(jnp.float32)[..., None]
    shape_raw = jnp.exp(-0.5 * (offsets / (0.5 * widths)) ** 2)
    shape_raw = jnp.where(jnp.abs(offsets) <= widths, shape_raw, 0.0)
    return shape_raw / lax.optimization_barrier(jnp.sum(shape_raw, axis=-1, keepdims=True))

def localize(field, weights_lon, weights_lat):
    lon_smooth = jnp.zeros_like(field)
    for shift in range(2 * BAND + 1):
        lon_smooth = lon_smooth + weights_lon[:, shift][:, None, None] * jnp.roll(field, BAND - shift, axis=1)
    padded = jnp.pad(lon_smooth, ((0, 0), (0, 0), (BAND, BAND)))
    result = jnp.zeros_like(field)
    for shift in range(2 * BAND + 1):
        result = result + weights_lat[:, shift][:, None, None] * padded[:, :, shift:shift + NLAT]
    return result

def reference(anomalies, spread, obs_index, innovation, obs_weight, band_width):
    band_weights = band_table(band_width)
    coef_ens = math.sqrt(hybrid_ens / MEMBERS)
    coef_static = math.sqrt(hybrid_static)

    def smooth(fields):
        return lax.map(lambda member_field: localize(member_field, band_weights[0], band_weights[1]), fields)
    plane_cells = LON_DEV * LAT_DEV
    obs_level = obs_index // plane_cells
    in_plane = obs_index % plane_cells
    tile_lon = jnp.arange(N_LON, dtype=jnp.int32)[:, None, None]
    tile_lat = jnp.arange(N_LAT, dtype=jnp.int32)[None, :, None]
    flat_index = ((obs_level * NLON + tile_lon * LON_DEV + in_plane // LAT_DEV) * NLAT + tile_lat * LAT_DEV + in_plane % LAT_DEV).reshape(-1).astype(jnp.int32)
    weights = obs_weight.reshape(-1)
    values = innovation.reshape(-1)
    cell_count = LEVELS * NLON * NLAT

    def scatter(obs_term):
        return jnp.zeros((cell_count,), jnp.float32).at[flat_index].add(obs_term).reshape(LEVELS, NLON, NLAT)

    def adjoint(gradient):
        products = jnp.concatenate([coef_ens * anomalies.astype(jnp.float32) * gradient[None], (coef_static * spread * gradient)[None]], axis=0)
        return smooth(products)

    def hessian(direction):
        localized = smooth(direction)
        combined = coef_ens * lax.optimization_barrier(jnp.sum(anomalies.astype(jnp.float32) * localized[:MEMBERS], axis=0)) + coef_static * spread * localized[MEMBERS]
        gradient = scatter(weights * combined.reshape(-1)[flat_index])
        return direction + adjoint(gradient)
    right_side = adjoint(scatter(weights * values))
    control = jnp.zeros_like(right_side)
    residual = right_side
    direction = right_side
    norm_now = jnp.sum(residual * residual)
    for iteration in range(ITERS):
        hess_image = hessian(direction)
        step_size = norm_now / jnp.sum(direction * hess_image)
        control = control + step_size * direction
        residual = residual - step_size * hess_image
        norm_next = jnp.sum(residual * residual)
        direction = residual + norm_next / norm_now * direction
        norm_now = norm_next
    return (control[:MEMBERS], control[MEMBERS])
```

```python
import functools
import math

import jax
import jax.numpy as jnp
from jax import lax
from jax.experimental import pallas as pl
from jax.experimental.pallas import tpu as pltpu
from jax.sharding import PartitionSpec as P

BAND = 12
RIM = 2 * BAND

hybrid_ens = 0.75
hybrid_static = 0.25

MESH = pl.DeviceIdType.MESH
VMEM = pl.BlockSpec(memory_space=pltpu.VMEM)
F32 = jnp.float32
BF16 = jnp.bfloat16


def split2(x):
    hi = x.astype(BF16)
    return hi, (x - hi.astype(F32)).astype(BF16)


def dot3(left, right):
    lh, ll = left
    rh, rl = right
    d = functools.partial(jnp.dot, preferred_element_type=F32)
    return d(lh, rh) + (d(ll, rh) + d(lh, rl))


AXES = ("lon", "lat", "mem")


def fused(a_ref, s_ref, i_ref, w_ref, v_ref, bw_ref, ens_ref, static_ref, *scratch, dims):
    members, levels, lon_cells, lat_cells, sizes = dims
    (fc, fr, bc, br, qc, qr, send_al, send_ah, recv_al, recv_ah, pack_l, pack_h, recv_pl, recv_ph,
     fpack, xrh, xrl, two_c, two_r, two_l, one_c, one_r, one_l, bflat, dflat, cov, part,
     slots, slots2, dslots, dsend, smoothed_lat, send, recv, csend, crecv, dsems, drems) = scratch
    lon_n, lat_n, mem_n = sizes
    total = lon_n * lat_n * mem_n
    fields = members + 1
    ext = lon_cells + 2 * RIM
    rows = levels * lon_cells
    chunk = rows // mem_n
    coef_ens = math.sqrt(hybrid_ens / (members * mem_n))
    coef_static = math.sqrt(hybrid_static)
    mine = [lax.axis_index(a) for a in AXES]
    lat_at, me = mine[1], mine[2]
    has_low, has_high = lat_at > 0, lat_at < lat_n - 1

    def shifted(step):
        parts, rest = [], step
        for size in reversed(sizes):
            parts.append(rest % size)
            rest //= size
        return tuple(lax.rem(m + s, size) for m, s, size in zip(mine, reversed(parts), sizes))

    barrier = pltpu.get_barrier_semaphore()
    for step in range(1, total):
        pl.semaphore_signal(barrier, inc=1, device_id=shifted(step), device_id_type=MESH)

    used = [0]

    def remote(src, dst, where):
        k = used[0]
        used[0] += 1
        return pltpu.make_async_remote_copy(
            src_ref=src, dst_ref=dst, send_sem=send.at[k], recv_sem=recv.at[k],
            device_id=where, device_id_type=MESH,
        )

    lon_low = {"lon": lax.rem(mine[0] + lon_n - 1, lon_n)}
    lon_high = {"lon": lax.rem(mine[0] + 1, lon_n)}
    lat_low = {"lat": lax.rem(lat_at + lat_n - 1, lat_n)}
    lat_high = {"lat": lax.rem(lat_at + 1, lat_n)}
    own = pl.ds(0, lon_cells)
    rim = pl.ds(lon_cells, 2 * RIM)
    low_rows = pl.ds(lon_cells, RIM)
    high_rows = pl.ds(lon_cells + RIM, RIM)
    first_rows = pl.ds(0, RIM)
    last_rows = pl.ds(lon_cells - RIM, RIM)
    low_lanes = pl.ds(0, lat_cells)
    high_lanes = pl.ds(lat_cells, lat_cells)

    def lon_start(copies):
        for c in copies:
            c.start()

    def lon_wait(copies):
        for c in copies:
            c.wait()

    class Lat:
        def __init__(self, low_src, high_src, from_low, from_high):
            self.to_low = remote(low_src, from_high, lat_low)
            self.to_high = remote(high_src, from_low, lat_high)

        def start(self):
            pl.when(has_low)(self.to_low.start)
            pl.when(has_high)(self.to_high.start)

        def wait(self):
            pl.when(has_low)(self.to_low.wait_send)
            pl.when(has_high)(self.to_high.wait_send)
            pl.when(has_high)(self.to_low.wait_recv)
            pl.when(has_low)(self.to_high.wait_recv)

    def lane_pack(read, count):
        lane = lax.broadcasted_iota(jnp.int32, (count, lat_cells), 1)
        low = jnp.zeros((count, lat_cells), F32)
        high = low
        for l in range(levels):
            x = read(l)
            here = (lane >= l * RIM) & (lane < (l + 1) * RIM)
            low = jnp.where(here, pltpu.roll(x, (l * RIM) % lat_cells, 1), low)
            high = jnp.where(here, pltpu.roll(x, ((l + 1) * RIM) % lat_cells, 1), high)
        return low, high

    def zero_edges(ref, lead=()):
        @pl.when(jnp.logical_not(has_low))
        def _():
            ref[(*lead, slice(None), low_lanes)] = jnp.zeros((ext, lat_cells), F32)

        @pl.when(jnp.logical_not(has_high))
        def _():
            ref[(*lead, slice(None), high_lanes)] = jnp.zeros((ext, lat_cells), F32)

    def load_member(m, _):
        lows, highs = [], []
        for l in range(levels):
            x = a_ref[m, l].astype(F32)
            fc[l, m, :lon_cells, :] = x
            lows.append(x[:RIM])
            highs.append(x[lon_cells - RIM :])
        send_al[m] = jnp.concatenate(lows, axis=0).astype(BF16)
        send_ah[m] = jnp.concatenate(highs, axis=0).astype(BF16)
        return 0

    lax.fori_loop(0, members, load_member, 0)
    for l in range(levels):
        fc[l, members, :lon_cells, :] = s_ref[l]

    def pack_member(span, count):
        def go(m, _):
            low, high = lane_pack(lambda l: fc[l, m, span, :], count)
            pack_l[m, span, :] = low.astype(BF16)
            pack_h[m, span, :] = high.astype(BF16)
            return 0

        lax.fori_loop(0, members, go, 0)

    def lon_field(ref, lead):
        at = lambda span: ref.at[(slice(None), *lead, span, slice(None))]
        return [
            remote(at(first_rows), at(high_rows), lon_low),
            remote(at(last_rows), at(low_rows), lon_high),
        ]

    def lat_field(slot, dst, lead, span):
        at = lambda lanes: dst.at[(*lead, span, lanes)]
        return Lat(
            fpack.at[slot, 0, span, :], fpack.at[slot, 1, span, :], at(low_lanes), at(high_lanes)
        )

    def fill_pack(slot, read, span, count):
        low, high = lane_pack(lambda l: read(l, span), count)
        fpack[slot, 0, span, :] = low
        fpack[slot, 1, span, :] = high

    read_s = lambda l, span: fc[l, members, span, :]
    read_b = lambda l, span: bc[l, span, :]
    read_q = lambda l, span: qc[l, span, :]

    pl.semaphore_wait(barrier, total - 1)
    lon_a = [remote(send_al, recv_ah, lon_low), remote(send_ah, recv_al, lon_high)]
    lon_start(lon_a)
    lon_s = lon_field(fc, (members,))
    lon_start(lon_s)
    pack_member(own, lon_cells)
    lat_a = Lat(pack_l.at[:, own, :], pack_h.at[:, own, :], recv_pl.at[:, own, :], recv_ph.at[:, own, :])
    lat_a.start()

    idx, val_w = i_ref[...], w_ref[...]
    n_obs = idx.shape[1]
    row, lane = idx // lat_cells, idx % lat_cells
    at_row = (lax.broadcasted_iota(jnp.int32, (rows, n_obs), 0) == row).astype(F32).astype(BF16)
    at_lane = lax.broadcasted_iota(jnp.int32, (lat_cells, n_obs), 0) == lane
    for val, out in ((val_w, dflat), (val_w * v_ref[...], bflat)):
        acc = None
        for _ in range(3):
            piece_val = val.astype(BF16).astype(F32)
            val = val - piece_val
            placed = jnp.where(at_lane, piece_val, 0.0).astype(BF16)
            term = lax.dot_general(
                at_row, placed, (((1,), (1,)), ((), ())), preferred_element_type=F32
            )
            acc = term if acc is None else acc + term
        out[...] = acc
    for l in range(levels):
        bc[l, :lon_cells, :] = bflat[l * lon_cells : (l + 1) * lon_cells, :]
    lon_b = lon_field(bc, ())
    lon_start(lon_b)
    fill_pack(0, read_s, own, lon_cells)
    fill_pack(1, read_b, own, lon_cells)
    lat_sb = [lat_field(0, fr, (members,), own), lat_field(1, br, (), own)]
    for c in lat_sb:
        c.start()
    zero_edges(fr, (members,))
    zero_edges(br)
    zero_edges(qr)

    def iota(shape, dim):
        return lax.broadcasted_iota(jnp.int32, shape, dim)

    def ext_place(index, cells):
        return jnp.where(index < cells, index, jnp.where(index < cells + RIM, index - cells - RIM, index - RIM))

    def make_matrices(l, _):
        taps = (iota((8, 128), 1) - BAND).astype(F32)

        def weights(kind):
            width = bw_ref[kind, l].astype(F32) + jnp.zeros((1, 1), F32)

            def raw(o):
                return jnp.where(jnp.abs(o) <= width, jnp.exp(-0.5 * (o / (0.5 * width)) ** 2), 0.0)

            norm = jnp.sum(raw(taps)[:1], axis=1, keepdims=True)
            return lambda o: raw(o.astype(F32)) / norm

        def put(ref, where, value):
            hi, lo = split2(value)
            ref[(0, *where)] = hi
            ref[(1, *where)] = lo

        w = weights(0)
        mids = 128 * pl.cdiv(lon_cells + 2 * BAND, 128)
        near = w(iota((lon_cells, mids), 0) - (iota((lon_cells, mids), 1) - BAND))
        near = jnp.where(iota((lon_cells, mids), 1) < lon_cells + 2 * BAND, near, 0.0)
        far = w(iota((mids, ext), 0) - BAND - ext_place(iota((mids, ext), 1), lon_cells))
        put(two_l, (l,), dot3(split2(near), split2(far)))
        put(one_l, (l,), w(iota((lon_cells, ext), 0) - ext_place(iota((lon_cells, ext), 1), lon_cells)))

        w = weights(1)
        mids = 128 * pl.cdiv(lat_cells + 2 * BAND, 128)
        mid = iota((mids, lat_cells), 0) - BAND
        place = lat_at * lat_cells + mid
        keep = (place >= 0) & (place < lat_cells * lat_n) & (mid < lat_cells + BAND)
        back = split2(jnp.where(keep, w(mid - iota((mids, lat_cells), 1)), 0.0))
        out = iota((lat_cells, lat_cells), 1)
        here = iota((lat_cells, mids), 0) - (iota((lat_cells, mids), 1) - BAND)
        put(two_c, (l,), dot3(split2(w(here)), back))
        put(one_c, (l,), w(iota((lat_cells, lat_cells), 0) - out))
        columns = pl.ds(pl.multiple_of(l * lat_cells, lat_cells), lat_cells)
        for side in range(2):
            shift = -RIM if side == 0 else lat_cells
            span = pl.ds(side * lat_cells, lat_cells)

            def rim_at(shape):
                p = iota(shape, 0) - l * RIM
                return p + shift, (p >= 0) & (p < RIM)

            pos, ok = rim_at((lat_cells, mids))
            there = jnp.where(ok, w(pos - (iota((lat_cells, mids), 1) - BAND)), 0.0)
            put(two_r, (span, columns), dot3(split2(there), back))
            pos, ok = rim_at((lat_cells, lat_cells))
            put(one_r, (span, columns), jnp.where(ok, w(pos - out), 0.0))
        return 0

    lax.fori_loop(0, levels, make_matrices, 0)

    def lat_part(yc, yr, c_mat, r_mat, l, span, count):
        columns = pl.ds(pl.multiple_of(l * lat_cells, lat_cells), lat_cells)
        xc = split2((fc[l, :, span, :] * yc[l, span, :][None]).reshape(fields * count, lat_cells))
        xr = (
            xrh[:, span, :].reshape(fields * count, 2 * lat_cells),
            xrl[:, span, :].reshape(fields * count, 2 * lat_cells),
        )
        t = dot3(xc, (c_mat[0, l], c_mat[1, l]))
        t = t + dot3(xr, (r_mat[0, :, columns], r_mat[1, :, columns]))
        for h, half in enumerate(split2(t)):
            smoothed_lat[h, l, span, :] = jnp.concatenate(
                [half[f * count : (f + 1) * count] for f in range(fields)], axis=1
            )

    def rim_products(yr, span):
        def go(f, _):
            hi, lo = split2(fr[f, span, :] * yr[span, :])
            xrh[f, span, :], xrl[f, span, :] = hi, lo
            return 0

        lax.fori_loop(0, fields, go, 0)

    def apply_own(yc, yr, mats):
        rim_products(yr, own)

        def go(l, _):
            lat_part(yc, yr, mats[0], mats[1], l, own, lon_cells)
            return 0

        lax.fori_loop(0, levels, go, 0)

    def apply_rim(yc, yr, mats, finish):
        rim_products(yr, rim)

        def go(i, _):
            l = lax.rem(me + 1 + i, levels)
            lat_part(yc, yr, mats[0], mats[1], l, rim, 2 * RIM)
            u = dot3((mats[2][0, l], mats[2][1, l]), (smoothed_lat[0, l], smoothed_lat[1, l]))
            finish(i, l, [u[:, f * lat_cells : (f + 1) * lat_cells] for f in range(fields)])
            return 0

        lax.fori_loop(0, levels, go, 0)

    def unpack_lat(span, count):
        for ref, keep, lanes in ((recv_pl, has_low, low_lanes), (recv_ph, has_high, high_lanes)):
            def go(m, _):
                fr[m, span, lanes] = ref[m, span, :].astype(F32)
                return 0

            def clear(m, _):
                fr[m, span, lanes] = jnp.zeros((count, lat_cells), F32)
                return 0

            @pl.when(keep)
            def _():
                lax.fori_loop(0, members, go, 0)

            @pl.when(jnp.logical_not(keep))
            def _():
                lax.fori_loop(0, members, clear, 0)

    lat_a.wait()
    unpack_lat(own, lon_cells)
    for c in lat_sb:
        c.wait()
    apply_own(bc, br, (two_c, two_r, two_l))

    lon_wait(lon_a)

    def unpack_member(m, _):
        low, high = recv_al[m].astype(F32), recv_ah[m].astype(F32)
        for l in range(levels):
            fc[l, m, low_rows, :] = low[l * RIM : (l + 1) * RIM]
            fc[l, m, high_rows, :] = high[l * RIM : (l + 1) * RIM]
        return 0

    lax.fori_loop(0, members, unpack_member, 0)
    pack_member(rim, 2 * RIM)
    lat_a2 = Lat(pack_l.at[:, rim, :], pack_h.at[:, rim, :], recv_pl.at[:, rim, :], recv_ph.at[:, rim, :])
    lat_a2.start()
    lon_wait(lon_s)
    lon_wait(lon_b)
    fill_pack(0, read_s, rim, 2 * RIM)
    fill_pack(1, read_b, rim, 2 * RIM)
    lat_sb2 = [lat_field(0, fr, (members,), rim), lat_field(1, br, (), rim)]
    for c in lat_sb2:
        c.start()
    lat_a2.wait()
    unpack_lat(rim, 2 * RIM)
    for c in lat_sb2:
        c.wait()

    def piece(owner):
        return pl.ds(pl.multiple_of(owner * chunk, chunk), chunk)

    def mem_copy(src, dst, j, group):
        return pltpu.make_async_remote_copy(
            src_ref=src, dst_ref=dst, send_sem=csend.at[group, j], recv_sem=crecv.at[group, j],
            device_id={"mem": lax.rem(me + j, mem_n)}, device_id_type=MESH,
        )

    def sum_copy(dst, j, group):
        return mem_copy(part.at[piece(lax.rem(me + j, mem_n))], dst.at[j], j, group)

    by_level = levels == mem_n

    def finish_cov(dst, group):
        def finish(i, l, smoothed):
            acc = fc[l, 0, :lon_cells, :] * smoothed[0]
            for f in range(1, members):
                acc = acc + fc[l, f, :lon_cells, :] * smoothed[f]
            acc = acc * (coef_ens * coef_ens)
            acc = acc + fc[l, members, :lon_cells, :] * smoothed[members] * (coef_static**2 / mem_n)
            part[pl.ds(pl.multiple_of(l * lon_cells, lon_cells), lon_cells), :] = acc
            if by_level:
                @pl.when(i < mem_n - 1)
                def _():
                    sum_copy(dst, i + 1, group).start()

        return finish

    def scatter_sum(dst, group):
        copies = [sum_copy(dst, j, group) for j in range(1, mem_n)]
        if not by_level:
            for copy in copies:
                copy.start()
        acc = part[piece(me), :]
        for j, copy in enumerate(copies):
            copy.wait_recv()
            acc = acc + dst[j + 1]
        for copy in copies:
            copy.wait_send()
        return acc

    def dots_start(left, right, group):
        at = iota((2, lat_cells), 0)
        a = jnp.sum(left, axis=0, keepdims=True)
        b = jnp.sum(right, axis=0, keepdims=True)
        dsend[group] = jnp.where(at == 0, a, b)
        copies = []
        for step in range(1, total):
            copy = pltpu.make_async_remote_copy(
                src_ref=dsend.at[group], dst_ref=dslots.at[group, step],
                send_sem=dsems.at[group, step], recv_sem=drems.at[group, step],
                device_id=shifted(step), device_id_type=MESH,
            )
            copy.start()
            copies.append(copy)
        return copies

    def dots_end(copies, group):
        for copy in copies:
            copy.wait()
        block = dsend[group] + jnp.sum(dslots[group, 1:], axis=0)
        sums = jnp.sum(block, axis=1, keepdims=True)
        return sums[0:1], sums[1:2]

    two, one = (two_c, two_r, two_l), (one_c, one_r, one_l)
    apply_rim(bc, br, two, finish_cov(slots, 0))
    acc = scatter_sum(slots, 0)
    cov[piece(me), :] = acc
    back = [mem_copy(cov.at[piece(me)], cov.at[piece(me)], j, 1) for j in range(1, mem_n)]
    for copy in back:
        copy.start()
    rhs_mine, diag_mine, cov_mine = bflat[piece(me), :], dflat[piece(me), :], acc
    image_mine = rhs_mine + diag_mine * cov_mine
    dots0 = dots_start(rhs_mine * cov_mine, cov_mine * image_mine, 0)
    for copy in back:
        copy.wait()
    for l in range(levels):
        span = slice(l * lon_cells, (l + 1) * lon_cells)
        qc[l, :lon_cells, :] = bflat[span, :] + dflat[span, :] * cov[span, :]
    lon_q = lon_field(qc, ())
    lon_start(lon_q)
    fill_pack(2, read_q, own, lon_cells)
    lat_q = lat_field(2, qr, (), own)
    lat_q.start()
    lon_wait(lon_q)
    fill_pack(2, read_q, rim, 2 * RIM)
    lat_q2 = lat_field(2, qr, (), rim)
    lat_q2.start()
    lat_q.wait()

    apply_own(qc, qr, two)
    lat_q2.wait()
    apply_rim(qc, qr, two, finish_cov(slots2, 2))
    cov_q = scatter_sum(slots2, 2)
    norm0, curve0 = dots_end(dots0, 0)
    alpha0 = norm0 / curve0
    resid = rhs_mine - alpha0 * image_mine
    cov_r = cov_mine - alpha0 * cov_q
    norm1, curve1 = dots_end(dots_start(resid * cov_r, cov_r * (resid + diag_mine * cov_r), 1), 1)
    beta = norm1 / norm0
    alpha1 = norm1 / (curve1 - beta * norm1 / alpha0)

    def combine(b, q):
        return alpha0 * b + alpha1 * ((b - alpha0 * q) + beta * b)

    for l in range(levels):
        bc[l] = combine(bc[l], qc[l])
    br[...] = combine(br[...], qr[...])

    def finish_control(i, l, smoothed):
        for f in range(members):
            ens_ref[f, l] = coef_ens * smoothed[f]
        static_ref[l] = coef_static * smoothed[members]

    apply_own(bc, br, one)
    apply_rim(bc, br, one, finish_control)


def per_device(anomalies, spread, obs_index, innovation, obs_weight, band_width):
    members = anomalies.shape[0]
    levels, lon_cells, lat_cells = spread.shape
    sizes = tuple(lax.axis_size(a) for a in AXES)
    mem_n, total = sizes[2], math.prod(sizes)
    fields = members + 1
    ext = lon_cells + 2 * RIM
    rows = levels * lon_cells
    chunk = rows // mem_n
    v = pltpu.VMEM
    sem = pltpu.SemaphoreType.DMA
    edge = v((members, levels * RIM, lat_cells), BF16)
    packed = v((members, ext, lat_cells), BF16)
    field = v((levels, ext, lat_cells), F32)
    field_rim = v((ext, 2 * lat_cells), F32)
    mats = [
        v((2, levels, lat_cells, lat_cells), BF16),
        v((2, 2 * lat_cells, levels * lat_cells), BF16),
        v((2, levels, lon_cells, ext), BF16),
    ]
    flat = v((rows, lat_cells), F32)
    scratch = [
        v((levels, fields, ext, lat_cells), F32),
        v((fields, ext, 2 * lat_cells), F32),
        field, field_rim, field, field_rim,
        edge, edge, edge, edge,
        packed, packed, packed, packed,
        v((3, 2, ext, lat_cells), F32),
        v((fields, ext, 2 * lat_cells), BF16),
        v((fields, ext, 2 * lat_cells), BF16),
        *mats, *mats,
        flat, flat, flat, flat,
        v((mem_n, chunk, lat_cells), F32),
        v((mem_n, chunk, lat_cells), F32),
        v((2, total, 2, lat_cells), F32),
        v((2, 2, lat_cells), F32),
        v((2, levels, ext, fields * lat_cells), BF16),
        sem((32,)), sem((32,)), sem((3, mem_n)), sem((3, mem_n)), sem((2, total)), sem((2, total)),
    ]
    kernel = functools.partial(fused, dims=(members, levels, lon_cells, lat_cells, sizes))
    return pl.pallas_call(
        kernel,
        out_shape=[
            jax.ShapeDtypeStruct((members, levels, lon_cells, lat_cells), F32),
            jax.ShapeDtypeStruct((levels, lon_cells, lat_cells), F32),
        ],
        in_specs=[VMEM] * 5 + [pl.BlockSpec(memory_space=pltpu.SMEM)],
        out_specs=[VMEM] * 2,
        scratch_shapes=scratch,
        compiler_params=pltpu.CompilerParams(
            collective_id=0, has_side_effects=True, vmem_limit_bytes=60 * 2**20
        ),
    )(
        anomalies, spread, obs_index.reshape(1, -1), obs_weight.reshape(1, -1),
        innovation.reshape(1, -1), band_width,
    )


def paired(a_ref, s_ref, i_ref, w_ref, v_ref, bw_ref, ub_ref, uq_ref, st_ref, coef_ref, *scratch, dims):
    members, levels, lon_cells, lat_cells, sizes = dims
    (acen, arim, plo, phi, scen, srim, spack, oidx, ow, ov, at_row, grid, grim, gpack, cov, orecv,
     drecv, mat_c, mat_r, lon_t, lon_l, xr, ts, ubuf, stat, send, recv, done) = scratch
    lon_n, lat_n, mem_n = sizes
    half = members // lon_n
    full = lon_n * lon_cells
    group = lon_n * mem_n
    rows = levels * lon_cells
    wide = lat_cells
    n_obs = i_ref.shape[1]
    coef_ens = math.sqrt(hybrid_ens / (members * mem_n))
    coef_static = math.sqrt(hybrid_static)
    at_lon, lat_at, me = (lax.axis_index(a) for a in AXES)
    other = 1 - at_lon
    has_low, has_high = lat_at > 0, lat_at < lat_n - 1
    my_id = at_lon * mem_n + me

    def group_peer(step):
        peer = lax.rem(my_id + step, group)
        return {"lon": peer // mem_n, "mem": lax.rem(peer, mem_n)}

    def lat_peer(step):
        return {"lat": lax.rem(lat_at + step, lat_n)}

    barrier = pltpu.get_barrier_semaphore()
    for step in range(1, group):
        pl.semaphore_signal(barrier, inc=1, device_id=group_peer(step), device_id_type=MESH)
    for step in range(1, lat_n):
        pl.semaphore_signal(barrier, inc=1, device_id=lat_peer(step), device_id_type=MESH)

    used = [0]

    def remote(src, dst, where):
        k = used[0]
        used[0] += 1
        return pltpu.make_async_remote_copy(
            src_ref=src, dst_ref=dst, send_sem=send.at[k], recv_sem=recv.at[k],
            device_id=where, device_id_type=MESH,
        )

    partner = {"lon": other}
    lat_low = {"lat": lax.rem(lat_at + lat_n - 1, lat_n)}
    lat_high = {"lat": lax.rem(lat_at + 1, lat_n)}
    own_rows = pl.ds(pl.multiple_of(at_lon * lon_cells, lon_cells), lon_cells)
    far_rows = pl.ds(pl.multiple_of(other * lon_cells, lon_cells), lon_cells)
    all_rows = pl.ds(0, full)
    low_lanes = pl.ds(0, wide)
    high_lanes = pl.ds(wide, wide)

    class Lat:
        def __init__(self, low_src, high_src, from_low, from_high):
            self.to_low = remote(low_src, from_high, lat_low)
            self.to_high = remote(high_src, from_low, lat_high)

        def start(self):
            pl.when(has_low)(self.to_low.start)
            pl.when(has_high)(self.to_high.start)

        def wait(self):
            pl.when(has_low)(self.to_low.wait_send)
            pl.when(has_high)(self.to_high.wait_send)
            pl.when(has_high)(self.to_low.wait_recv)
            pl.when(has_low)(self.to_high.wait_recv)

    def iota(shape, dim):
        return lax.broadcasted_iota(jnp.int32, shape, dim)

    def lane_pack(read, count, at_levels=None):
        lane = iota((count, wide), 1)
        low = jnp.zeros((count, wide), F32)
        high = low
        for l in range(levels) if at_levels is None else at_levels:
            x = read(l)
            here = (lane >= l * RIM) & (lane < (l + 1) * RIM)
            low = jnp.where(here, pltpu.roll(x, lax.rem(l * RIM, wide), 1), low)
            high = jnp.where(here, pltpu.roll(x, lax.rem((l + 1) * RIM, wide), 1), high)
        return low, high

    def actual(p):
        return lax.rem(at_lon * half + p, members)

    def fill(p, _):
        acen[p, :, own_rows, :] = a_ref[actual(p)]
        return 0

    def pack_member(p, span, count):
        low, high = lane_pack(lambda l: acen[p, l, span, :].astype(F32), count)
        plo[p, span, :] = low.astype(BF16)
        phi[p, span, :] = high.astype(BF16)

    def pack_static(span, count):
        low, high = lane_pack(lambda l: scen[span, :], count, [me])
        spack[0, span, :] = low
        spack[1, span, :] = high

    def lat_members(which, span):
        return Lat(
            plo.at[which, span, :], phi.at[which, span, :],
            arim.at[which, span, low_lanes], arim.at[which, span, high_lanes],
        )

    def lat_static(span):
        return Lat(
            spack.at[0, span, :], spack.at[1, span, :],
            srim.at[span, low_lanes], srim.at[span, high_lanes],
        )

    def lat_grid(g):
        return Lat(gpack.at[g, 0], gpack.at[g, 1], grim.at[g, :, low_lanes], grim.at[g, :, high_lanes])

    first, second = pl.ds(0, half), pl.ds(half, half)
    x_obs = [
        remote(src, dst.at[1], partner) for src, dst in ((i_ref, oidx), (w_ref, ow), (v_ref, ov))
    ]
    x_static = remote(s_ref.at[me], scen.at[own_rows], partner)
    x_first = [
        remote(a_ref.at[other * half + p], acen.at[p, :, own_rows, :], partner) for p in range(half)
    ]
    x_second = remote(
        a_ref.at[pl.ds(at_lon * half, half)], acen.at[second, :, own_rows, :], partner
    )
    pl.semaphore_wait(barrier, group - 1 + lat_n - 1)
    for copy in [*x_obs, x_static, *x_first]:
        copy.start()

    lax.fori_loop(0, members, fill, 0)

    def pack_first(p, _):
        pack_member(p, own_rows, lon_cells)
        return 0

    lax.fori_loop(0, half, pack_first, 0)
    lat_a = lat_members(first, own_rows)
    lat_a.start()
    scen[own_rows, :] = s_ref[me]
    pack_static(own_rows, lon_cells)
    lat_s = lat_static(own_rows)
    lat_s.start()

    @pl.when(jnp.logical_not(has_low))
    def _():
        arim[:, :, low_lanes] = jnp.zeros((members, full, wide), BF16)
        srim[:, low_lanes] = jnp.zeros((full, wide), F32)
        grim[:, :, low_lanes] = jnp.zeros((2, full, wide), F32)

    @pl.when(jnp.logical_not(has_high))
    def _():
        arim[:, :, high_lanes] = jnp.zeros((members, full, wide), BF16)
        srim[:, high_lanes] = jnp.zeros((full, wide), F32)
        grim[:, :, high_lanes] = jnp.zeros((2, full, wide), F32)

    slot_rows = (own_rows, far_rows)
    slot_tile = (at_lon, other)

    def mark_rows(s):
        row = oidx[s] // wide
        at_row[s] = (iota((rows, n_obs), 0) == row).astype(F32).astype(BF16)

    def scatter(s, value, g):
        at_lane = iota((wide, n_obs), 0) == oidx[s] % wide
        hi = value.astype(BF16).astype(F32)
        lo = value - hi
        placed = jnp.concatenate(
            [jnp.where(at_lane, hi, 0.0).astype(BF16), jnp.where(at_lane, lo, 0.0).astype(BF16)], axis=0
        )
        out = lax.dot_general(
            at_row[s], placed, (((1,), (1,)), ((), ())), preferred_element_type=F32
        )
        out = out[:, :wide] + out[:, wide:]
        for l in range(levels):
            grid[g, l, slot_rows[s], :] = out[l * lon_cells : (l + 1) * lon_cells]

    def gather(s, g):
        hi, lo = split2(cov[slot_tile[s]].T)
        left = jnp.concatenate([hi, lo], axis=0)
        step = 512 if n_obs % 512 == 0 else n_obs
        for c in range(0, n_obs, step):
            part = jnp.dot(left, at_row[s, :, c : c + step], preferred_element_type=F32)
            lane = oidx[s, :, c : c + step] % wide
            here = iota((wide, step), 0) == lane
            value = jnp.where(here, part[:wide] + part[wide:], 0.0)
            orecv[g, my_id, slot_tile[s], :, c : c + step] = jnp.sum(value, axis=0, keepdims=True)

    def send_grid(g):
        low, high = lane_pack(lambda l: grid[g, l], full)
        gpack[g, 0] = low
        gpack[g, 1] = high
        copy = lat_grid(g)
        copy.start()
        return copy

    oidx[0], ow[0], ov[0] = i_ref[...], w_ref[...], v_ref[...]
    mark_rows(0)
    scatter(0, ow[0] * ov[0], 0)

    def make_matrices(l, _):
        taps = (iota((8, 128), 1) - BAND).astype(F32)

        def weights(kind):
            width = bw_ref[kind, l].astype(F32) + jnp.zeros((1, 1), F32)

            def raw(o):
                return jnp.where(jnp.abs(o) <= width, jnp.exp(-0.5 * (o / (0.5 * width)) ** 2), 0.0)

            norm = jnp.sum(raw(taps)[:1], axis=1, keepdims=True)
            return lambda o: raw(o.astype(F32)) / norm

        def put_lon(ref, count, value):
            hi, lo = split2(value)
            ref[l, :count, :full] = hi
            ref[l, :count, full:] = hi
            ref[l, count:, :full] = lo
            ref[l, count:, full:] = jnp.zeros((count, full), BF16)

        w = weights(0)

        def ring(count, base):
            d = iota((count, full), 1) - (iota((count, full), 0) + base)
            d = jnp.where(d > full // 2, d - full, d)
            return w(jnp.where(d < -(full // 2), d + full, d))

        circle = split2(ring(full, 0))
        put_lon(lon_t, full, dot3(circle, circle))
        put_lon(lon_l, lon_cells, ring(lon_cells, at_lon * lon_cells))

        def put_lat(ref, kind, hi_at, lo_at, value):
            hi, lo = split2(value)
            ref[kind, l, pl.ds(hi_at, wide), :wide] = hi
            ref[kind, l, pl.ds(hi_at, wide), wide:] = lo
            ref[kind, l, pl.ds(lo_at, wide), :wide] = hi
            ref[kind, l, pl.ds(lo_at, wide), wide:] = jnp.zeros((wide, wide), BF16)

        w = weights(1)
        mids = 128 * pl.cdiv(wide + 2 * BAND, 128)
        mid = iota((mids, wide), 0) - BAND
        place = lat_at * wide + mid
        keep = (place >= 0) & (place < wide * lat_n) & (mid < wide + BAND)
        back = split2(jnp.where(keep, w(mid - iota((mids, wide), 1)), 0.0))
        out = iota((wide, wide), 1)
        here = iota((wide, mids), 0) - (iota((wide, mids), 1) - BAND)
        put_lat(mat_c, 0, 0, wide, dot3(split2(w(here)), back))
        put_lat(mat_c, 1, 0, wide, w(iota((wide, wide), 0) - out))
        for side in range(2):
            shift = -RIM if side == 0 else wide

            def rim_at(shape):
                p = iota(shape, 0) - l * RIM
                return p + shift, (p >= 0) & (p < RIM)

            pos, ok = rim_at((wide, mids))
            there = jnp.where(ok, w(pos - (iota((wide, mids), 1) - BAND)), 0.0)
            put_lat(mat_r, 0, side * wide, (2 + side) * wide, dot3(split2(there), back))
            pos, ok = rim_at((wide, wide))
            put_lat(mat_r, 1, side * wide, (2 + side) * wide, jnp.where(ok, w(pos - out), 0.0))
        return 0

    lax.fori_loop(0, levels, make_matrices, 0)

    for copy in x_obs:
        copy.wait()
    mark_rows(1)
    scatter(1, ow[1] * ov[1], 0)
    lat_b = send_grid(0)

    x_static.wait()
    pack_static(far_rows, lon_cells)
    lat_s2 = lat_static(far_rows)
    lat_s2.start()
    lat_a2 = []
    for p in range(half):
        x_first[p].wait()
        pack_member(p, far_rows, lon_cells)
        copy = lat_members(p, far_rows)
        copy.start()
        lat_a2.append(copy)

    def dot(a, b):
        return jnp.dot(a, b, preferred_element_type=F32)

    def rim_split(x):
        hi, lo = split2(x)
        return jnp.concatenate([hi, lo], axis=1)

    def rim_member(g, p):
        xr[p] = rim_split(arim[p].astype(F32) * grim[g])

    def along_lat(x, rims, kind, l):
        t = dot(rim_split(x), mat_c[kind, l]) + dot(rims, mat_r[kind, l])
        return split2(t[:, :wide] + t[:, wide:])

    def lat_member(g, p, kind, l):
        hi, lo = along_lat(acen[p, l].astype(F32) * grid[g, l], xr[p], kind, l)
        ts[l, :full, p * wide : (p + 1) * wide] = hi
        ts[l, full:, p * wide : (p + 1) * wide] = lo

    def lat_own_static(g, kind):
        rims = rim_split(srim[...] * grim[g])
        hi, lo = along_lat(scen[...] * grid[g, me], rims, kind, me)
        return jnp.concatenate([hi, lo], axis=0)

    def cov_level(l):
        u = dot(lon_t[l], ts[l, :, : half * wide])
        u = u[:full] + u[full:]
        acc = acen[0, l].astype(F32) * u[:, :wide]
        for p in range(1, half):
            acc = acc + acen[p, l].astype(F32) * u[:, p * wide : (p + 1) * wide]
        acc = acc * (coef_ens * coef_ens)
        at = pl.ds(pl.multiple_of(l * lon_cells, lon_cells), lon_cells)
        for j in range(lon_n):
            cov[j, at, :] = acc[j * lon_cells : (j + 1) * lon_cells]

    def cov_static(g):
        u = dot(lon_t[me], lat_own_static(g, 0))
        acc = scen[...] * (u[:full] + u[full:]) * (coef_static**2 / lon_n)
        at = pl.ds(pl.multiple_of(me * lon_cells, lon_cells), lon_cells)
        for j in range(lon_n):
            cov[j, at, :] = cov[j, at, :] + acc[j * lon_cells : (j + 1) * lon_cells]

    def share(g):
        for s in range(lon_n):
            gather(s, g)
        copies = []
        for step in range(1, group):
            copy = remote(orecv.at[g, my_id], orecv.at[g, my_id], group_peer(step))
            copy.start()
            copies.append(copy)
        return copies

    def shared(copies, g):
        for copy in copies:
            copy.wait()
        sums = []
        for s in range(lon_n):
            acc = orecv[g, 0, slot_tile[s]]
            for k in range(1, group):
                acc = acc + orecv[g, k, slot_tile[s]]
            sums.append(acc)
        return sums

    def out_level(g, p0, n):
        def go(l, _):
            for p in range(p0, p0 + n):
                lat_member(g, p, 1, l)
            u = dot(lon_l[l], ts[l, :, p0 * wide : (p0 + n) * wide])
            u = (u[:lon_cells] + u[lon_cells:]) * coef_ens
            for p in range(n):
                ubuf[g, actual(p0 + p), l] = u[:, p * wide : (p + 1) * wide]
            return 0

        lax.fori_loop(0, levels, go, 0)

    def rim_span(g, p0, n):
        def go(p, _):
            rim_member(g, p)
            return 0

        lax.fori_loop(p0, p0 + n, go, 0)

    def out_static(g):
        u = dot(lon_l[me], lat_own_static(g, 1))
        stat[me, g] = (u[:lon_cells] + u[lon_cells:]) * coef_static
        copies = []
        for j in range(1, mem_n):
            copy = remote(stat.at[me, g], stat.at[me, g], {"mem": lax.rem(me + j, mem_n)})
            copy.start()
            copies.append(copy)
        return copies

    def dots_start(g, left, right):
        def total(pairs):
            acc = None
            for x in pairs:
                for c in range(0, n_obs, 128):
                    part = x[:, c : c + 128]
                    acc = part if acc is None else acc + part
            return acc

        at = iota((2, 128), 0)
        drecv[g, lat_at] = jnp.where(at == 0, total(left), total(right))
        copies = []
        for step in range(1, lat_n):
            copy = remote(drecv.at[g, lat_at], drecv.at[g, lat_at], lat_peer(step))
            copy.start()
            copies.append(copy)
        return copies

    def dots_end(copies, g):
        for copy in copies:
            copy.wait()
        block = drecv[g, 0]
        for k in range(1, lat_n):
            block = block + drecv[g, k]
        sums = jnp.sum(block, axis=1, keepdims=True)
        return sums[0:1], sums[1:2]

    lat_b.wait()
    lat_a.wait()
    for p in range(half):
        lat_a2[p].wait()
        rim_member(0, p)

        def go(l, _):
            lat_member(0, p, 0, l)
            return 0

        lax.fori_loop(0, levels, go, 0)

    def go_cov(l, _):
        cov_level(l)
        return 0

    lax.fori_loop(0, levels, go_cov, 0)
    lat_s.wait()
    lat_s2.wait()
    cov_static(0)
    sharing = share(0)
    x_second.start()

    out_level(0, 0, half)
    stat_b = out_static(0)
    cz = shared(sharing, 0)
    z = [ow[s] * ov[s] for s in range(lon_n)]
    q = [z[s] + ow[s] * cz[s] for s in range(lon_n)]
    for s in range(lon_n):
        scatter(s, q[s], 1)
    lat_q = send_grid(1)
    dots0 = dots_start(0, [z[s] * cz[s] for s in range(lon_n)], [cz[s] * q[s] for s in range(lon_n)])
    x_second.wait()

    def pack_second(p, _):
        pack_member(p, all_rows, full)
        return 0

    lax.fori_loop(half, members, pack_second, 0)
    lat_a3 = lat_members(second, all_rows)
    lat_a3.start()
    lat_q.wait()
    rim_span(1, 0, half)

    def go_q(l, _):
        for p in range(half):
            lat_member(1, p, 0, l)
        cov_level(l)
        return 0

    lax.fori_loop(0, levels, go_q, 0)
    cov_static(1)
    sharing = share(1)
    stat_q = out_static(1)
    out_level(1, 0, half)
    lat_a3.wait()
    rim_span(0, half, half)
    out_level(0, half, half)
    b_out = pltpu.make_async_copy(ubuf.at[0], ub_ref, done.at[0])
    b_out.start()
    rim_span(1, half, half)
    out_level(1, half, half)
    q_out = pltpu.make_async_copy(ubuf.at[1], uq_ref, done.at[1])
    q_out.start()

    cq = shared(sharing, 1)
    norm0, curve0 = dots_end(dots0, 0)
    alpha0 = norm0 / curve0
    resid = [z[s] - alpha0 * q[s] for s in range(lon_n)]
    cr = [cz[s] - alpha0 * cq[s] for s in range(lon_n)]
    dots1 = dots_start(
        1,
        [resid[s] * cr[s] for s in range(lon_n)],
        [cr[s] * (resid[s] + ow[s] * cr[s]) for s in range(lon_n)],
    )
    for copy in [*stat_b, *stat_q]:
        copy.wait()
    s_out = pltpu.make_async_copy(stat, st_ref, done.at[2])
    s_out.start()
    norm1, curve1 = dots_end(dots1, 1)
    beta = norm1 / norm0
    alpha1 = norm1 / (curve1 - beta * norm1 / alpha0)
    on_b = alpha0 + alpha1 * (1.0 + beta)
    on_q = -alpha0 * alpha1
    coef_ref[...] = jnp.where(iota((2, 128), 0) == 0, on_b, on_q)
    for copy in (b_out, q_out, s_out):
        copy.wait()


def paired_device(anomalies, spread, obs_index, innovation, obs_weight, band_width):
    members = anomalies.shape[0]
    levels, lon_cells, lat_cells = spread.shape
    sizes = tuple(lax.axis_size(a) for a in AXES)
    lon_n, lat_n, mem_n = sizes
    half = members // lon_n
    full = lon_n * lon_cells
    group = lon_n * mem_n
    n_obs = obs_index.shape[-1]
    v = pltpu.VMEM
    sem = pltpu.SemaphoreType.DMA
    wide = lat_cells
    copies = 9 + 2 * (2 + 2 + half + 2 + 1) + 2 * (group - 1 + lat_n - 1 + mem_n - 1)
    scratch = [
        v((members, levels, full, wide), BF16),
        v((members, full, 2 * wide), BF16),
        v((members, full, wide), BF16),
        v((members, full, wide), BF16),
        v((full, wide), F32),
        v((full, 2 * wide), F32),
        v((2, full, wide), F32),
        v((lon_n, 1, n_obs), jnp.int32),
        v((lon_n, 1, n_obs), F32),
        v((lon_n, 1, n_obs), F32),
        v((lon_n, levels * lon_cells, n_obs), BF16),
        v((2, levels, full, wide), F32),
        v((2, full, 2 * wide), F32),
        v((2, 2, full, wide), F32),
        v((lon_n, levels * lon_cells, wide), F32),
        v((2, group, lon_n, 1, n_obs), F32),
        v((2, lat_n, 2, 128), F32),
        v((2, levels, 2 * wide, 2 * wide), BF16),
        v((2, levels, 4 * wide, 2 * wide), BF16),
        v((levels, 2 * full, 2 * full), BF16),
        v((levels, 2 * lon_cells, 2 * full), BF16),
        v((members, full, 4 * wide), BF16),
        v((levels, 2 * full, members * wide), BF16),
        v((2, members, levels, lon_cells, wide), F32),
        v((mem_n, 2, lon_cells, wide), F32),
        sem((copies,)), sem((copies,)), sem((3,)),
    ]
    hbm = pl.BlockSpec(memory_space=pl.ANY)
    kernel = functools.partial(paired, dims=(members, levels, lon_cells, lat_cells, sizes))
    out = jax.ShapeDtypeStruct((members, levels, lon_cells, lat_cells), F32)
    ub, uq, st, coef = pl.pallas_call(
        kernel,
        out_shape=[
            out, out,
            jax.ShapeDtypeStruct((levels, 2, lon_cells, lat_cells), F32),
            jax.ShapeDtypeStruct((2, 128), F32),
        ],
        in_specs=[VMEM] * 5 + [pl.BlockSpec(memory_space=pltpu.SMEM)],
        out_specs=[hbm, hbm, hbm, VMEM],
        scratch_shapes=scratch,
        compiler_params=pltpu.CompilerParams(
            collective_id=0, has_side_effects=True, vmem_limit_bytes=48 * 2**20
        ),
    )(
        anomalies, spread, obs_index.reshape(1, -1), obs_weight.reshape(1, -1),
        innovation.reshape(1, -1), band_width,
    )
    on_b, on_q = coef[0, 0], coef[1, 0]
    return on_b * ub + on_q * uq, on_b * st[:, 0] + on_q * st[:, 1]


def pick(*args):
    members = args[0].shape[0]
    levels, lon_cells, lat_cells = args[1].shape
    lon_n, lat_n, mem_n = (lax.axis_size(a) for a in AXES)
    pairs = lon_n == 2 and members % 2 == 0 and levels == mem_n and lon_cells > BAND and lat_n > 1
    return (paired_device if pairs else per_device)(*args)


def solution(mesh):
    return jax.shard_map(
        pick,
        mesh=mesh,
        in_specs=(
            P("mem", None, "lon", "lat"),
            P(None, "lon", "lat"),
            P("lon", "lat", None),
            P("lon", "lat", None),
            P("lon", "lat", None),
            P(),
        ),
        out_specs=(P("mem", None, "lon", "lat"), P(None, "lon", "lat")),
        check_vma=False,
    )
```

```python
import functools
import math

import jax
import jax.numpy as jnp
from jax import lax
from jax.experimental import pallas as pl
from jax.experimental.pallas import tpu as pltpu
from jax.sharding import PartitionSpec as P

BAND = 12
RIM = 2 * BAND

hybrid_ens = 0.75
hybrid_static = 0.25

MESH = pl.DeviceIdType.MESH
VMEM = pl.BlockSpec(memory_space=pltpu.VMEM)
F32 = jnp.float32
BF16 = jnp.bfloat16


def split2(x):
    hi = x.astype(BF16)
    return hi, (x - hi.astype(F32)).astype(BF16)


def dot3(left, right):
    lh, ll = left
    rh, rl = right
    d = functools.partial(jnp.dot, preferred_element_type=F32)
    return d(lh, rh) + (d(ll, rh) + d(lh, rl))


AXES = ("lon", "lat", "mem")


def fused(a_ref, s_ref, i_ref, w_ref, v_ref, bw_ref, ens_ref, static_ref, *scratch, dims):
    members, levels, lon_cells, lat_cells, sizes = dims
    (fc, fr, bc, br, qc, qr, send_al, send_ah, recv_al, recv_ah, pack_l, pack_h, recv_pl, recv_ph,
     fpack, xrh, xrl, two_c, two_r, two_l, one_c, one_r, one_l, bflat, dflat, cov, part,
     slots, slots2, dslots, dsend, smoothed_lat, send, recv, csend, crecv, dsems, drems) = scratch
    lon_n, lat_n, mem_n = sizes
    total = lon_n * lat_n * mem_n
    fields = members + 1
    ext = lon_cells + 2 * RIM
    rows = levels * lon_cells
    chunk = rows // mem_n
    coef_ens = math.sqrt(hybrid_ens / (members * mem_n))
    coef_static = math.sqrt(hybrid_static)
    mine = [lax.axis_index(a) for a in AXES]
    lat_at, me = mine[1], mine[2]
    has_low, has_high = lat_at > 0, lat_at < lat_n - 1

    def shifted(step):
        parts, rest = [], step
        for size in reversed(sizes):
            parts.append(rest % size)
            rest //= size
        return tuple(lax.rem(m + s, size) for m, s, size in zip(mine, reversed(parts), sizes))

    barrier = pltpu.get_barrier_semaphore()
    for step in range(1, total):
        pl.semaphore_signal(barrier, inc=1, device_id=shifted(step), device_id_type=MESH)

    used = [0]

    def remote(src, dst, where):
        k = used[0]
        used[0] += 1
        return pltpu.make_async_remote_copy(
            src_ref=src, dst_ref=dst, send_sem=send.at[k], recv_sem=recv.at[k],
            device_id=where, device_id_type=MESH,
        )

    lon_low = {"lon": lax.rem(mine[0] + lon_n - 1, lon_n)}
    lon_high = {"lon": lax.rem(mine[0] + 1, lon_n)}
    lat_low = {"lat": lax.rem(lat_at + lat_n - 1, lat_n)}
    lat_high = {"lat": lax.rem(lat_at + 1, lat_n)}
    own = pl.ds(0, lon_cells)
    rim = pl.ds(lon_cells, 2 * RIM)
    low_rows = pl.ds(lon_cells, RIM)
    high_rows = pl.ds(lon_cells + RIM, RIM)
    first_rows = pl.ds(0, RIM)
    last_rows = pl.ds(lon_cells - RIM, RIM)
    low_lanes = pl.ds(0, lat_cells)
    high_lanes = pl.ds(lat_cells, lat_cells)

    def lon_start(copies):
        for c in copies:
            c.start()

    def lon_wait(copies):
        for c in copies:
            c.wait()

    class Lat:
        def __init__(self, low_src, high_src, from_low, from_high):
            self.to_low = remote(low_src, from_high, lat_low)
            self.to_high = remote(high_src, from_low, lat_high)

        def start(self):
            pl.when(has_low)(self.to_low.start)
            pl.when(has_high)(self.to_high.start)

        def wait(self):
            pl.when(has_low)(self.to_low.wait_send)
            pl.when(has_high)(self.to_high.wait_send)
            pl.when(has_high)(self.to_low.wait_recv)
            pl.when(has_low)(self.to_high.wait_recv)

    def lane_pack(read, count):
        lane = lax.broadcasted_iota(jnp.int32, (count, lat_cells), 1)
        low = jnp.zeros((count, lat_cells), F32)
        high = low
        for l in range(levels):
            x = read(l)
            here = (lane >= l * RIM) & (lane < (l + 1) * RIM)
            low = jnp.where(here, pltpu.roll(x, (l * RIM) % lat_cells, 1), low)
            high = jnp.where(here, pltpu.roll(x, ((l + 1) * RIM) % lat_cells, 1), high)
        return low, high

    def zero_edges(ref, lead=()):
        @pl.when(jnp.logical_not(has_low))
        def _():
            ref[(*lead, slice(None), low_lanes)] = jnp.zeros((ext, lat_cells), F32)

        @pl.when(jnp.logical_not(has_high))
        def _():
            ref[(*lead, slice(None), high_lanes)] = jnp.zeros((ext, lat_cells), F32)

    def load_member(m, _):
        lows, highs = [], []
        for l in range(levels):
            x = a_ref[m, l].astype(F32)
            fc[l, m, :lon_cells, :] = x
            lows.append(x[:RIM])
            highs.append(x[lon_cells - RIM :])
        send_al[m] = jnp.concatenate(lows, axis=0).astype(BF16)
        send_ah[m] = jnp.concatenate(highs, axis=0).astype(BF16)
        return 0

    lax.fori_loop(0, members, load_member, 0)
    for l in range(levels):
        fc[l, members, :lon_cells, :] = s_ref[l]

    def pack_member(span, count):
        def go(m, _):
            low, high = lane_pack(lambda l: fc[l, m, span, :], count)
            pack_l[m, span, :] = low.astype(BF16)
            pack_h[m, span, :] = high.astype(BF16)
            return 0

        lax.fori_loop(0, members, go, 0)

    def lon_field(ref, lead):
        at = lambda span: ref.at[(slice(None), *lead, span, slice(None))]
        return [
            remote(at(first_rows), at(high_rows), lon_low),
            remote(at(last_rows), at(low_rows), lon_high),
        ]

    def lat_field(slot, dst, lead, span):
        at = lambda lanes: dst.at[(*lead, span, lanes)]
        return Lat(
            fpack.at[slot, 0, span, :], fpack.at[slot, 1, span, :], at(low_lanes), at(high_lanes)
        )

    def fill_pack(slot, read, span, count):
        low, high = lane_pack(lambda l: read(l, span), count)
        fpack[slot, 0, span, :] = low
        fpack[slot, 1, span, :] = high

    read_s = lambda l, span: fc[l, members, span, :]
    read_b = lambda l, span: bc[l, span, :]
    read_q = lambda l, span: qc[l, span, :]

    pl.semaphore_wait(barrier, total - 1)
    lon_a = [remote(send_al, recv_ah, lon_low), remote(send_ah, recv_al, lon_high)]
    lon_start(lon_a)
    lon_s = lon_field(fc, (members,))
    lon_start(lon_s)
    pack_member(own, lon_cells)
    lat_a = Lat(pack_l.at[:, own, :], pack_h.at[:, own, :], recv_pl.at[:, own, :], recv_ph.at[:, own, :])
    lat_a.start()

    idx, val_w = i_ref[...], w_ref[...]
    n_obs = idx.shape[1]
    row, lane = idx // lat_cells, idx % lat_cells
    at_row = (lax.broadcasted_iota(jnp.int32, (rows, n_obs), 0) == row).astype(F32).astype(BF16)
    at_lane = lax.broadcasted_iota(jnp.int32, (lat_cells, n_obs), 0) == lane
    for val, out in ((val_w, dflat), (val_w * v_ref[...], bflat)):
        acc = None
        for _ in range(3):
            piece_val = val.astype(BF16).astype(F32)
            val = val - piece_val
            placed = jnp.where(at_lane, piece_val, 0.0).astype(BF16)
            term = lax.dot_general(
                at_row, placed, (((1,), (1,)), ((), ())), preferred_element_type=F32
            )
            acc = term if acc is None else acc + term
        out[...] = acc
    for l in range(levels):
        bc[l, :lon_cells, :] = bflat[l * lon_cells : (l + 1) * lon_cells, :]
    lon_b = lon_field(bc, ())
    lon_start(lon_b)
    fill_pack(0, read_s, own, lon_cells)
    fill_pack(1, read_b, own, lon_cells)
    lat_sb = [lat_field(0, fr, (members,), own), lat_field(1, br, (), own)]
    for c in lat_sb:
        c.start()
    zero_edges(fr, (members,))
    zero_edges(br)
    zero_edges(qr)

    def iota(shape, dim):
        return lax.broadcasted_iota(jnp.int32, shape, dim)

    def ext_place(index, cells):
        return jnp.where(index < cells, index, jnp.where(index < cells + RIM, index - cells - RIM, index - RIM))

    def make_matrices(l, _):
        taps = (iota((8, 128), 1) - BAND).astype(F32)

        def weights(kind):
            width = bw_ref[kind, l].astype(F32) + jnp.zeros((1, 1), F32)

            def raw(o):
                return jnp.where(jnp.abs(o) <= width, jnp.exp(-0.5 * (o / (0.5 * width)) ** 2), 0.0)

            norm = jnp.sum(raw(taps)[:1], axis=1, keepdims=True)
            return lambda o: raw(o.astype(F32)) / norm

        def put(ref, where, value):
            hi, lo = split2(value)
            ref[(0, *where)] = hi
            ref[(1, *where)] = lo

        w = weights(0)
        mids = 128 * pl.cdiv(lon_cells + 2 * BAND, 128)
        near = w(iota((lon_cells, mids), 0) - (iota((lon_cells, mids), 1) - BAND))
        near = jnp.where(iota((lon_cells, mids), 1) < lon_cells + 2 * BAND, near, 0.0)
        far = w(iota((mids, ext), 0) - BAND - ext_place(iota((mids, ext), 1), lon_cells))
        put(two_l, (l,), dot3(split2(near), split2(far)))
        put(one_l, (l,), w(iota((lon_cells, ext), 0) - ext_place(iota((lon_cells, ext), 1), lon_cells)))

        w = weights(1)
        mids = 128 * pl.cdiv(lat_cells + 2 * BAND, 128)
        mid = iota((mids, lat_cells), 0) - BAND
        place = lat_at * lat_cells + mid
        keep = (place >= 0) & (place < lat_cells * lat_n) & (mid < lat_cells + BAND)
        back = split2(jnp.where(keep, w(mid - iota((mids, lat_cells), 1)), 0.0))
        out = iota((lat_cells, lat_cells), 1)
        here = iota((lat_cells, mids), 0) - (iota((lat_cells, mids), 1) - BAND)
        put(two_c, (l,), dot3(split2(w(here)), back))
        put(one_c, (l,), w(iota((lat_cells, lat_cells), 0) - out))
        columns = pl.ds(pl.multiple_of(l * lat_cells, lat_cells), lat_cells)
        for side in range(2):
            shift = -RIM if side == 0 else lat_cells
            span = pl.ds(side * lat_cells, lat_cells)

            def rim_at(shape):
                p = iota(shape, 0) - l * RIM
                return p + shift, (p >= 0) & (p < RIM)

            pos, ok = rim_at((lat_cells, mids))
            there = jnp.where(ok, w(pos - (iota((lat_cells, mids), 1) - BAND)), 0.0)
            put(two_r, (span, columns), dot3(split2(there), back))
            pos, ok = rim_at((lat_cells, lat_cells))
            put(one_r, (span, columns), jnp.where(ok, w(pos - out), 0.0))
        return 0

    lax.fori_loop(0, levels, make_matrices, 0)

    def lat_part(yc, yr, c_mat, r_mat, l, span, count):
        columns = pl.ds(pl.multiple_of(l * lat_cells, lat_cells), lat_cells)
        xc = split2((fc[l, :, span, :] * yc[l, span, :][None]).reshape(fields * count, lat_cells))
        xr = (
            xrh[:, span, :].reshape(fields * count, 2 * lat_cells),
            xrl[:, span, :].reshape(fields * count, 2 * lat_cells),
        )
        t = dot3(xc, (c_mat[0, l], c_mat[1, l]))
        t = t + dot3(xr, (r_mat[0, :, columns], r_mat[1, :, columns]))
        for h, half in enumerate(split2(t)):
            smoothed_lat[h, l, span, :] = jnp.concatenate(
                [half[f * count : (f + 1) * count] for f in range(fields)], axis=1
            )

    def rim_products(yr, span):
        def go(f, _):
            hi, lo = split2(fr[f, span, :] * yr[span, :])
            xrh[f, span, :], xrl[f, span, :] = hi, lo
            return 0

        lax.fori_loop(0, fields, go, 0)

    def apply_own(yc, yr, mats):
        rim_products(yr, own)

        def go(l, _):
            lat_part(yc, yr, mats[0], mats[1], l, own, lon_cells)
            return 0

        lax.fori_loop(0, levels, go, 0)

    def apply_rim(yc, yr, mats, finish):
        rim_products(yr, rim)

        def go(i, _):
            l = lax.rem(me + 1 + i, levels)
            lat_part(yc, yr, mats[0], mats[1], l, rim, 2 * RIM)
            u = dot3((mats[2][0, l], mats[2][1, l]), (smoothed_lat[0, l], smoothed_lat[1, l]))
            finish(i, l, [u[:, f * lat_cells : (f + 1) * lat_cells] for f in range(fields)])
            return 0

        lax.fori_loop(0, levels, go, 0)

    def unpack_lat(span, count):
        for ref, keep, lanes in ((recv_pl, has_low, low_lanes), (recv_ph, has_high, high_lanes)):
            def go(m, _):
                fr[m, span, lanes] = ref[m, span, :].astype(F32)
                return 0

            def clear(m, _):
                fr[m, span, lanes] = jnp.zeros((count, lat_cells), F32)
                return 0

            @pl.when(keep)
            def _():
                lax.fori_loop(0, members, go, 0)

            @pl.when(jnp.logical_not(keep))
            def _():
                lax.fori_loop(0, members, clear, 0)

    lat_a.wait()
    unpack_lat(own, lon_cells)
    for c in lat_sb:
        c.wait()
    apply_own(bc, br, (two_c, two_r, two_l))

    lon_wait(lon_a)

    def unpack_member(m, _):
        low, high = recv_al[m].astype(F32), recv_ah[m].astype(F32)
        for l in range(levels):
            fc[l, m, low_rows, :] = low[l * RIM : (l + 1) * RIM]
            fc[l, m, high_rows, :] = high[l * RIM : (l + 1) * RIM]
        return 0

    lax.fori_loop(0, members, unpack_member, 0)
    pack_member(rim, 2 * RIM)
    lat_a2 = Lat(pack_l.at[:, rim, :], pack_h.at[:, rim, :], recv_pl.at[:, rim, :], recv_ph.at[:, rim, :])
    lat_a2.start()
    lon_wait(lon_s)
    lon_wait(lon_b)
    fill_pack(0, read_s, rim, 2 * RIM)
    fill_pack(1, read_b, rim, 2 * RIM)
    lat_sb2 = [lat_field(0, fr, (members,), rim), lat_field(1, br, (), rim)]
    for c in lat_sb2:
        c.start()
    lat_a2.wait()
    unpack_lat(rim, 2 * RIM)
    for c in lat_sb2:
        c.wait()

    def piece(owner):
        return pl.ds(pl.multiple_of(owner * chunk, chunk), chunk)

    def mem_copy(src, dst, j, group):
        return pltpu.make_async_remote_copy(
            src_ref=src, dst_ref=dst, send_sem=csend.at[group, j], recv_sem=crecv.at[group, j],
            device_id={"mem": lax.rem(me + j, mem_n)}, device_id_type=MESH,
        )

    def sum_copy(dst, j, group):
        return mem_copy(part.at[piece(lax.rem(me + j, mem_n))], dst.at[j], j, group)

    by_level = levels == mem_n

    def finish_cov(dst, group):
        def finish(i, l, smoothed):
            acc = fc[l, 0, :lon_cells, :] * smoothed[0]
            for f in range(1, members):
                acc = acc + fc[l, f, :lon_cells, :] * smoothed[f]
            acc = acc * (coef_ens * coef_ens)
            acc = acc + fc[l, members, :lon_cells, :] * smoothed[members] * (coef_static**2 / mem_n)
            part[pl.ds(pl.multiple_of(l * lon_cells, lon_cells), lon_cells), :] = acc
            if by_level:
                @pl.when(i < mem_n - 1)
                def _():
                    sum_copy(dst, i + 1, group).start()

        return finish

    def scatter_sum(dst, group):
        copies = [sum_copy(dst, j, group) for j in range(1, mem_n)]
        if not by_level:
            for copy in copies:
                copy.start()
        acc = part[piece(me), :]
        for j, copy in enumerate(copies):
            copy.wait_recv()
            acc = acc + dst[j + 1]
        for copy in copies:
            copy.wait_send()
        return acc

    def dots_start(left, right, group):
        at = iota((2, lat_cells), 0)
        a = jnp.sum(left, axis=0, keepdims=True)
        b = jnp.sum(right, axis=0, keepdims=True)
        dsend[group] = jnp.where(at == 0, a, b)
        copies = []
        for step in range(1, total):
            copy = pltpu.make_async_remote_copy(
                src_ref=dsend.at[group], dst_ref=dslots.at[group, step],
                send_sem=dsems.at[group, step], recv_sem=drems.at[group, step],
                device_id=shifted(step), device_id_type=MESH,
            )
            copy.start()
            copies.append(copy)
        return copies

    def dots_end(copies, group):
        for copy in copies:
            copy.wait()
        block = dsend[group] + jnp.sum(dslots[group, 1:], axis=0)
        sums = jnp.sum(block, axis=1, keepdims=True)
        return sums[0:1], sums[1:2]

    two, one = (two_c, two_r, two_l), (one_c, one_r, one_l)
    apply_rim(bc, br, two, finish_cov(slots, 0))
    acc = scatter_sum(slots, 0)
    cov[piece(me), :] = acc
    back = [mem_copy(cov.at[piece(me)], cov.at[piece(me)], j, 1) for j in range(1, mem_n)]
    for copy in back:
        copy.start()
    rhs_mine, diag_mine, cov_mine = bflat[piece(me), :], dflat[piece(me), :], acc
    image_mine = rhs_mine + diag_mine * cov_mine
    dots0 = dots_start(rhs_mine * cov_mine, cov_mine * image_mine, 0)
    for copy in back:
        copy.wait()
    for l in range(levels):
        span = slice(l * lon_cells, (l + 1) * lon_cells)
        qc[l, :lon_cells, :] = bflat[span, :] + dflat[span, :] * cov[span, :]
    lon_q = lon_field(qc, ())
    lon_start(lon_q)
    fill_pack(2, read_q, own, lon_cells)
    lat_q = lat_field(2, qr, (), own)
    lat_q.start()
    lon_wait(lon_q)
    fill_pack(2, read_q, rim, 2 * RIM)
    lat_q2 = lat_field(2, qr, (), rim)
    lat_q2.start()
    lat_q.wait()

    apply_own(qc, qr, two)
    lat_q2.wait()
    apply_rim(qc, qr, two, finish_cov(slots2, 2))
    cov_q = scatter_sum(slots2, 2)
    norm0, curve0 = dots_end(dots0, 0)
    alpha0 = norm0 / curve0
    resid = rhs_mine - alpha0 * image_mine
    cov_r = cov_mine - alpha0 * cov_q
    norm1, curve1 = dots_end(dots_start(resid * cov_r, cov_r * (resid + diag_mine * cov_r), 1), 1)
    beta = norm1 / norm0
    alpha1 = norm1 / (curve1 - beta * norm1 / alpha0)

    def combine(b, q):
        return alpha0 * b + alpha1 * ((b - alpha0 * q) + beta * b)

    for l in range(levels):
        bc[l] = combine(bc[l], qc[l])
    br[...] = combine(br[...], qr[...])

    def finish_control(i, l, smoothed):
        for f in range(members):
            ens_ref[f, l] = coef_ens * smoothed[f]
        static_ref[l] = coef_static * smoothed[members]

    apply_own(bc, br, one)
    apply_rim(bc, br, one, finish_control)


def per_device(anomalies, spread, obs_index, innovation, obs_weight, band_width):
    members = anomalies.shape[0]
    levels, lon_cells, lat_cells = spread.shape
    sizes = tuple(lax.axis_size(a) for a in AXES)
    mem_n, total = sizes[2], math.prod(sizes)
    fields = members + 1
    ext = lon_cells + 2 * RIM
    rows = levels * lon_cells
    chunk = rows // mem_n
    v = pltpu.VMEM
    sem = pltpu.SemaphoreType.DMA
    edge = v((members, levels * RIM, lat_cells), BF16)
    packed = v((members, ext, lat_cells), BF16)
    field = v((levels, ext, lat_cells), F32)
    field_rim = v((ext, 2 * lat_cells), F32)
    mats = [
        v((2, levels, lat_cells, lat_cells), BF16),
        v((2, 2 * lat_cells, levels * lat_cells), BF16),
        v((2, levels, lon_cells, ext), BF16),
    ]
    flat = v((rows, lat_cells), F32)
    scratch = [
        v((levels, fields, ext, lat_cells), F32),
        v((fields, ext, 2 * lat_cells), F32),
        field, field_rim, field, field_rim,
        edge, edge, edge, edge,
        packed, packed, packed, packed,
        v((3, 2, ext, lat_cells), F32),
        v((fields, ext, 2 * lat_cells), BF16),
        v((fields, ext, 2 * lat_cells), BF16),
        *mats, *mats,
        flat, flat, flat, flat,
        v((mem_n, chunk, lat_cells), F32),
        v((mem_n, chunk, lat_cells), F32),
        v((2, total, 2, lat_cells), F32),
        v((2, 2, lat_cells), F32),
        v((2, levels, ext, fields * lat_cells), BF16),
        sem((32,)), sem((32,)), sem((3, mem_n)), sem((3, mem_n)), sem((2, total)), sem((2, total)),
    ]
    kernel = functools.partial(fused, dims=(members, levels, lon_cells, lat_cells, sizes))
    return pl.pallas_call(
        kernel,
        out_shape=[
            jax.ShapeDtypeStruct((members, levels, lon_cells, lat_cells), F32),
            jax.ShapeDtypeStruct((levels, lon_cells, lat_cells), F32),
        ],
        in_specs=[VMEM] * 5 + [pl.BlockSpec(memory_space=pltpu.SMEM)],
        out_specs=[VMEM] * 2,
        scratch_shapes=scratch,
        compiler_params=pltpu.CompilerParams(
            collective_id=0, has_side_effects=True, vmem_limit_bytes=60 * 2**20
        ),
    )(
        anomalies, spread, obs_index.reshape(1, -1), obs_weight.reshape(1, -1),
        innovation.reshape(1, -1), band_width,
    )


def paired(a_hbm, s_hbm, i_hbm, w_hbm, v_hbm, bw_hbm, ub_ref, uq_ref, st_ref, coef_ref, *scratch, dims):
    members, levels, lon_cells, lat_cells, sizes = dims
    (acen, arim, plo, phi, scen, srim, spack, oidx, ow, ov, at_row, grid, grim, gpack, cov, orecv,
     drecv, mat_c, mat_r, lon_t, lon_l, xr, tc, ts, to, bw_ref, send, recv, load, relay) = scratch
    lon_n, lat_n, mem_n = sizes
    half = members // lon_n
    full = lon_n * lon_cells
    group = lon_n * mem_n
    rows = levels * lon_cells
    wide = lat_cells
    edge = 16 * pl.cdiv(BAND, 16)
    reach = lon_cells + 2 * edge
    n_obs = oidx.shape[2]
    coef_ens = math.sqrt(hybrid_ens / (members * mem_n))
    coef_static = math.sqrt(hybrid_static)
    at_lon, lat_at, me = (lax.axis_index(a) for a in AXES)
    other = 1 - at_lon
    has_low, has_high = lat_at > 0, lat_at < lat_n - 1
    my_id = at_lon * mem_n + me

    def group_peer(step):
        peer = lax.rem(my_id + step, group)
        return {"lon": peer // mem_n, "mem": lax.rem(peer, mem_n)}

    def lat_peer(step):
        return {"lat": lax.rem(lat_at + step, lat_n)}

    own_rows, far_rows = pl.ds(0, lon_cells), pl.ds(lon_cells, lon_cells)
    first, second = pl.ds(0, half), pl.ds(half, half)
    loads = [
        pltpu.make_async_copy(src, dst, load.at[k])
        for k, (src, dst) in enumerate((
            (i_hbm, oidx.at[0]),
            (w_hbm, ow.at[0]),
            (v_hbm, ov.at[0]),
            (s_hbm.at[me], scen.at[own_rows]),
            (a_hbm.at[pl.ds(other * half, half)], acen.at[second, :, own_rows, :]),
            (a_hbm.at[pl.ds(at_lon * half, half)], acen.at[first, :, own_rows, :]),
            (bw_hbm, bw_ref),
        ))
    ]
    for copy in loads:
        copy.start()

    near = [
        (True, {"lon": other}),
        (has_low, {"lat": lat_at - 1}),
        (has_high, {"lat": lat_at + 1}),
        (me > 0, {"mem": me - 1}),
        (me < mem_n - 1, {"mem": me + 1}),
    ]
    n_near = sum(jnp.asarray(there, jnp.int32) for there, _ in near)

    def greet(sem):
        for there, where in near:
            def go(where=where):
                pl.semaphore_signal(sem, inc=1, device_id=where, device_id_type=MESH)

            go() if there is True else pl.when(there)(go)

    def relay_round(r):
        pl.semaphore_wait(relay.at[r], n_near)
        if r + 1 < rounds:
            greet(relay.at[r + 1])

    rounds = max(lon_n + mem_n - 2, lat_n - 1) - 1
    barrier = pltpu.get_barrier_semaphore()
    greet(barrier)

    used = [0]

    def remote(src, dst, where):
        k = used[0]
        used[0] += 1
        return pltpu.make_async_remote_copy(
            src_ref=src, dst_ref=dst, send_sem=send.at[k], recv_sem=recv.at[k],
            device_id=where, device_id_type=MESH,
        )

    partner = {"lon": other}
    lat_low = {"lat": lax.rem(lat_at + lat_n - 1, lat_n)}
    lat_high = {"lat": lax.rem(lat_at + 1, lat_n)}
    all_rows = pl.ds(0, full)
    low_lanes = pl.ds(0, wide)
    high_lanes = pl.ds(wide, wide)

    class Lat:
        def __init__(self, low_src, high_src, from_low, from_high):
            self.to_low = remote(low_src, from_high, lat_low)
            self.to_high = remote(high_src, from_low, lat_high)

        def start(self):
            pl.when(has_low)(self.to_low.start)
            pl.when(has_high)(self.to_high.start)

        def wait(self):
            pl.when(has_low)(self.to_low.wait_send)
            pl.when(has_high)(self.to_high.wait_send)
            pl.when(has_high)(self.to_low.wait_recv)
            pl.when(has_low)(self.to_high.wait_recv)

    def iota(shape, dim):
        return lax.broadcasted_iota(jnp.int32, shape, dim)

    def lane_pack(read, count, at_levels=None):
        lane = iota((count, wide), 1)
        low = jnp.zeros((count, wide), F32)
        high = low
        for l in range(levels) if at_levels is None else at_levels:
            x = read(l)
            here = (lane >= l * RIM) & (lane < (l + 1) * RIM)
            low = jnp.where(here, pltpu.roll(x, lax.rem(l * RIM, wide), 1), low)
            high = jnp.where(here, pltpu.roll(x, lax.rem((l + 1) * RIM, wide), 1), high)
        return low, high

    def actual(p):
        return lax.rem(at_lon * half + p, members)

    def pack_member(p, span, count):
        low, high = lane_pack(lambda l: acen[p, l, span, :].astype(F32), count)
        plo[p, span, :] = low.astype(BF16)
        phi[p, span, :] = high.astype(BF16)

    def pack_static(span, count):
        low, high = lane_pack(lambda l: scen[span, :], count, [me])
        spack[0, span, :] = low
        spack[1, span, :] = high

    def lat_members(which, span):
        return Lat(
            plo.at[which, span, :], phi.at[which, span, :],
            arim.at[which, span, low_lanes], arim.at[which, span, high_lanes],
        )

    def lat_static(span):
        return Lat(
            spack.at[0, span, :], spack.at[1, span, :],
            srim.at[span, low_lanes], srim.at[span, high_lanes],
        )

    def lat_grid(g):
        return Lat(gpack.at[g, 0], gpack.at[g, 1], grim.at[g, :, low_lanes], grim.at[g, :, high_lanes])

    x_obs = [remote(ref.at[0], ref.at[1], partner) for ref in (oidx, ow, ov)]
    x_static = remote(scen.at[own_rows], scen.at[far_rows], partner)
    x_first = [
        remote(acen.at[half + p, :, own_rows, :], acen.at[p, :, far_rows, :], partner)
        for p in range(half)
    ]
    x_second = remote(acen.at[first, :, own_rows, :], acen.at[second, :, far_rows, :], partner)
    for copy in loads:
        copy.wait()
    pl.semaphore_wait(barrier, n_near)
    for copy in [*x_obs, *x_first, x_static]:
        copy.start()
    greet(relay.at[0])

    def pack_first(p, _):
        pack_member(p, own_rows, lon_cells)
        return 0

    lax.fori_loop(0, half, pack_first, 0)
    lat_a = lat_members(first, own_rows)
    lat_a.start()
    pack_static(own_rows, lon_cells)
    lat_s = lat_static(own_rows)
    lat_s.start()

    @pl.when(jnp.logical_not(has_low))
    def _():
        arim[:, :, low_lanes] = jnp.zeros((members, full, wide), BF16)
        srim[:, low_lanes] = jnp.zeros((full, wide), F32)
        grim[:, :, low_lanes] = jnp.zeros((2, full, wide), F32)

    @pl.when(jnp.logical_not(has_high))
    def _():
        arim[:, :, high_lanes] = jnp.zeros((members, full, wide), BF16)
        srim[:, high_lanes] = jnp.zeros((full, wide), F32)
        grim[:, :, high_lanes] = jnp.zeros((2, full, wide), F32)

    relay_round(0)
    slot_rows = (own_rows, far_rows)
    slot_tile = (at_lon, other)

    def mark_rows(s):
        row = oidx[s] // wide
        at_row[s] = (iota((rows, n_obs), 0) == row).astype(F32).astype(BF16)

    def scatter(s, value, g):
        at_lane = iota((wide, n_obs), 0) == oidx[s] % wide
        hi = value.astype(BF16).astype(F32)
        lo = value - hi
        placed = jnp.concatenate(
            [jnp.where(at_lane, hi, 0.0).astype(BF16), jnp.where(at_lane, lo, 0.0).astype(BF16)], axis=0
        )
        out = lax.dot_general(
            at_row[s], placed, (((1,), (1,)), ((), ())), preferred_element_type=F32
        )
        out = out[:, :wide] + out[:, wide:]
        for l in range(levels):
            grid[g, l, slot_rows[s], :] = out[l * lon_cells : (l + 1) * lon_cells]

    def gather(s, g):
        hi, lo = split2(cov[s].T)
        left = jnp.concatenate([hi, lo], axis=0)
        step = 512 if n_obs % 512 == 0 else n_obs
        for c in range(0, n_obs, step):
            part = jnp.dot(left, at_row[s, :, c : c + step], preferred_element_type=F32)
            lane = oidx[s, :, c : c + step] % wide
            here = iota((wide, step), 0) == lane
            value = jnp.where(here, part[:wide] + part[wide:], 0.0)
            orecv[g, my_id, slot_tile[s], :, c : c + step] = jnp.sum(value, axis=0, keepdims=True)

    def send_grid(g):
        low, high = lane_pack(lambda l: grid[g, l], full)
        gpack[g, 0] = low
        gpack[g, 1] = high
        copy = lat_grid(g)
        copy.start()
        return copy

    mark_rows(0)
    scatter(0, ow[0] * ov[0], 0)

    def make_matrices(l, _):
        taps = (iota((8, 128), 1) - BAND).astype(F32)

        def weights(kind):
            width = bw_ref[kind, l].astype(F32) + jnp.zeros((1, 1), F32)

            def raw(o):
                return jnp.where(jnp.abs(o) <= width, jnp.exp(-0.5 * (o / (0.5 * width)) ** 2), 0.0)

            norm = jnp.sum(raw(taps)[:1], axis=1, keepdims=True)
            return lambda o: raw(o.astype(F32)) / norm

        def put_lon(ref, count, value):
            hi, lo = split2(value)
            cols = value.shape[1]
            ref[l, :count, :] = jnp.concatenate([hi, hi], axis=1)
            ref[l, count:, :] = jnp.concatenate([lo, jnp.zeros((count, cols), BF16)], axis=1)

        w = weights(0)

        def ring(count, cols):
            c = iota((count, cols), 1)
            if cols < full:
                c = jnp.where(c < lon_cells + edge, c, c + full - cols)
            d = c - iota((count, cols), 0)
            d = jnp.where(d > full // 2, d - full, d)
            return w(jnp.where(d < -(full // 2), d + full, d))

        circle = split2(ring(full, full))
        put_lon(lon_t, full, dot3(circle, circle))
        put_lon(lon_l, lon_cells, ring(lon_cells, reach))

        def put_lat(ref, kind, hi_at, lo_at, value):
            hi, lo = split2(value)
            ref[kind, l, pl.ds(hi_at, wide), :wide] = hi
            ref[kind, l, pl.ds(hi_at, wide), wide:] = lo
            ref[kind, l, pl.ds(lo_at, wide), :wide] = hi
            ref[kind, l, pl.ds(lo_at, wide), wide:] = jnp.zeros((wide, wide), BF16)

        w = weights(1)
        mids = 128 * pl.cdiv(wide + 2 * BAND, 128)
        mid = iota((mids, wide), 0) - BAND
        place = lat_at * wide + mid
        keep = (place >= 0) & (place < wide * lat_n) & (mid < wide + BAND)
        back = split2(jnp.where(keep, w(mid - iota((mids, wide), 1)), 0.0))
        out = iota((wide, wide), 1)
        here = iota((wide, mids), 0) - (iota((wide, mids), 1) - BAND)
        put_lat(mat_c, 0, 0, wide, dot3(split2(w(here)), back))
        put_lat(mat_c, 1, 0, wide, w(iota((wide, wide), 0) - out))
        for side in range(2):
            shift = -RIM if side == 0 else wide

            def rim_at(shape):
                p = iota(shape, 0) - l * RIM
                return p + shift, (p >= 0) & (p < RIM)

            pos, ok = rim_at((wide, mids))
            there = jnp.where(ok, w(pos - (iota((wide, mids), 1) - BAND)), 0.0)
            put_lat(mat_r, 0, side * wide, (2 + side) * wide, dot3(split2(there), back))
            pos, ok = rim_at((wide, wide))
            put_lat(mat_r, 1, side * wide, (2 + side) * wide, jnp.where(ok, w(pos - out), 0.0))
        return 0

    lax.fori_loop(0, levels, make_matrices, 0)
    for r in range(1, rounds):
        relay_round(r)

    for copy in x_obs:
        copy.wait()
    mark_rows(1)
    scatter(1, ow[1] * ov[1], 0)
    lat_b = send_grid(0)

    def dot(a, b):
        return jnp.dot(a, b, preferred_element_type=F32)

    def fold(t):
        return t[:, :wide] + t[:, wide:]

    def pair(x):
        return jnp.concatenate(split2(x), axis=1)

    def stack(x):
        return jnp.concatenate(split2(x), axis=0)

    def reached(x):
        return jnp.concatenate([x[: lon_cells + edge], x[full - edge :]], axis=0)

    def rim_member(g, p):
        xr[p] = pair(arim[p].astype(F32) * grim[g])

    def center_member(g, p):
        for l in range(levels):
            tc[p, l] = fold(dot(pair(acen[p, l].astype(F32) * grid[g, l]), mat_c[0, l]))

    def lat_member(p, at):
        for l in range(levels):
            ts[l, :, at] = stack(tc[p, l] + fold(dot(xr[p], mat_r[0, l])))

    def cov_level(l):
        u = dot(lon_t[l], ts[l])
        u = u[:full] + u[full:]
        acc = acen[0, l].astype(F32) * u[:, :wide]
        for p in range(1, half):
            acc = acc + acen[p, l].astype(F32) * u[:, p * wide : (p + 1) * wide]
        acc = acc * (coef_ens * coef_ens)
        for j in range(lon_n):
            cov[j, l * lon_cells : (l + 1) * lon_cells, :] = acc[j * lon_cells : (j + 1) * lon_cells]

    def cov_static(g):
        t = dot(pair(scen[...] * grid[g, me]), mat_c[0, me])
        t = t + dot(pair(srim[...] * grim[g]), mat_r[0, me])
        u = dot(lon_t[me], stack(fold(t)))
        acc = scen[...] * (u[:full] + u[full:]) * (coef_static**2 / lon_n)
        at = pl.ds(pl.multiple_of(me * lon_cells, lon_cells), lon_cells)
        for j in range(lon_n):
            cov[j, at, :] = cov[j, at, :] + acc[j * lon_cells : (j + 1) * lon_cells]

    lat_a2 = []
    for p in range(half):
        x_first[p].wait()
        pack_member(p, far_rows, lon_cells)
        copy = lat_members(p, far_rows)
        copy.start()
        lat_a2.append(copy)
        center_member(0, p)
    x_static.wait()
    x_second.start()
    pack_static(far_rows, lon_cells)
    lat_s2 = lat_static(far_rows)
    lat_s2.start()

    def share(g):
        for s in range(lon_n):
            gather(s, g)
        copies = []
        for step in range(1, group):
            copy = remote(orecv.at[g, my_id], orecv.at[g, my_id], group_peer(step))
            copy.start()
            copies.append(copy)
        return copies

    def shared(copies, g):
        for copy in copies:
            copy.wait()
        sums = []
        for s in range(lon_n):
            acc = orecv[g, 0, slot_tile[s]]
            for k in range(1, group):
                acc = acc + orecv[g, k, slot_tile[s]]
            sums.append(acc)
        return sums

    def out_level(g, p0, n):
        out_ref = (ub_ref, uq_ref)[g]

        def go(l, _):
            for p in range(n):
                x = reached(acen[p0 + p, l]).astype(F32) * reached(grid[g, l])
                t = dot(pair(x), mat_c[1, l]) + dot(reached(xr[p0 + p]), mat_r[1, l])
                to[l, :, p * wide : (p + 1) * wide] = stack(fold(t))
            u = dot(lon_l[l], to[l])
            u = (u[:lon_cells] + u[lon_cells:]) * coef_ens
            for p in range(n):
                out_ref[actual(p0 + p), l] = u[:, p * wide : (p + 1) * wide]
            return 0

        lax.fori_loop(0, levels, go, 0)

    def rim_span(g, p0, n):
        def go(p, _):
            rim_member(g, p)
            return 0

        lax.fori_loop(p0, p0 + n, go, 0)

    def out_static(g):
        t = dot(pair(reached(scen[...] * grid[g, me])), mat_c[1, me])
        t = t + dot(pair(reached(srim[...] * grim[g])), mat_r[1, me])
        u = dot(lon_l[me], stack(fold(t)))
        st_ref[g, me] = (u[:lon_cells] + u[lon_cells:]) * coef_static
        copies = []
        for j in range(1, mem_n):
            copy = remote(st_ref.at[g, me], st_ref.at[g, me], {"mem": lax.rem(me + j, mem_n)})
            copy.start()
            copies.append(copy)
        return copies

    def dots_start(g, left, right):
        def total(pairs):
            acc = None
            for x in pairs:
                for c in range(0, n_obs, 128):
                    part = x[:, c : c + 128]
                    acc = part if acc is None else acc + part
            return acc

        at = iota((2, 128), 0)
        drecv[g, lat_at] = jnp.where(at == 0, total(left), total(right))
        copies = []
        for step in range(1, lat_n):
            copy = remote(drecv.at[g, lat_at], drecv.at[g, lat_at], lat_peer(step))
            copy.start()
            copies.append(copy)
        return copies

    def dots_end(copies, g):
        for copy in copies:
            copy.wait()
        block = drecv[g, 0]
        for k in range(1, lat_n):
            block = block + drecv[g, k]
        sums = jnp.sum(block, axis=1, keepdims=True)
        return sums[0:1], sums[1:2]

    def lat_all(p, _):
        lat_member(p, pl.ds(pl.multiple_of(p * wide, wide), wide))
        return 0

    lat_b.wait()
    lat_a.wait()
    for p in range(half):
        lat_a2[p].wait()
        rim_member(0, p)
        lat_member(p, slice(p * wide, (p + 1) * wide))
    for l in range(levels):
        cov_level(l)
    lat_s.wait()
    lat_s2.wait()
    cov_static(0)
    sharing = share(0)

    x_second.wait()

    def pack_second(p, _):
        pack_member(p, all_rows, full)
        return 0

    lax.fori_loop(half, members, pack_second, 0)
    lat_a3 = lat_members(second, all_rows)
    lat_a3.start()
    out_level(0, 0, half)
    stat_b = out_static(0)

    cz = shared(sharing, 0)
    z = [ow[s] * ov[s] for s in range(lon_n)]
    q = [z[s] + ow[s] * cz[s] for s in range(lon_n)]
    for s in range(lon_n):
        scatter(s, q[s], 1)
    lat_q = send_grid(1)
    dots0 = dots_start(0, [z[s] * cz[s] for s in range(lon_n)], [cz[s] * q[s] for s in range(lon_n)])

    def center_all(p, _):
        center_member(1, p)
        return 0

    lax.fori_loop(0, half, center_all, 0)
    lat_a3.wait()
    rim_span(0, half, half)
    out_level(0, half, half)

    lat_q.wait()
    rim_span(1, 0, half)
    lax.fori_loop(0, half, lat_all, 0)
    for l in range(levels):
        cov_level(l)
    cov_static(1)
    sharing = share(1)
    stat_q = out_static(1)
    out_level(1, 0, half)
    rim_span(1, half, half)
    out_level(1, half, half)

    cq = shared(sharing, 1)
    norm0, curve0 = dots_end(dots0, 0)
    alpha0 = norm0 / curve0
    resid = [z[s] - alpha0 * q[s] for s in range(lon_n)]
    cr = [cz[s] - alpha0 * cq[s] for s in range(lon_n)]
    dots1 = dots_start(
        1,
        [resid[s] * cr[s] for s in range(lon_n)],
        [cr[s] * (resid[s] + ow[s] * cr[s]) for s in range(lon_n)],
    )
    for copy in [*stat_b, *stat_q]:
        copy.wait()
    norm1, curve1 = dots_end(dots1, 1)
    beta = norm1 / norm0
    alpha1 = norm1 / (curve1 - beta * norm1 / alpha0)
    on_b = alpha0 + alpha1 * (1.0 + beta)
    on_q = -alpha0 * alpha1
    coef_ref[...] = jnp.where(iota((2, 128), 0) == 0, on_b, on_q)


def combine(ub_ref, uq_ref, st_ref, coef_ref, ens_ref, static_ref, ens, static, sems):
    on_b, on_q = coef_ref[0:1, :], coef_ref[1:2, :]
    members = ens.shape[0]
    copies = []
    for m in range(members):
        ens[m] = on_b * ub_ref[m] + on_q * uq_ref[m]
        copies.append(pltpu.make_async_copy(ens.at[m], ens_ref.at[m], sems.at[m]))
        copies[-1].start()
    static[...] = on_b * st_ref[0] + on_q * st_ref[1]
    copies.append(pltpu.make_async_copy(static, static_ref, sems.at[members]))
    copies[-1].start()
    for copy in copies:
        copy.wait()


def paired_device(anomalies, spread, obs_index, innovation, obs_weight, band_width):
    members = anomalies.shape[0]
    levels, lon_cells, lat_cells = spread.shape
    sizes = tuple(lax.axis_size(a) for a in AXES)
    lon_n, lat_n, mem_n = sizes
    half = members // lon_n
    full = lon_n * lon_cells
    group = lon_n * mem_n
    n_obs = obs_index.shape[-1]
    v = pltpu.VMEM
    sem = pltpu.SemaphoreType.DMA
    wide = lat_cells
    reach = lon_cells + 2 * 16 * pl.cdiv(BAND, 16)
    copies = 9 + 2 * (2 + 2 + half + 2 + 1) + 2 * (group - 1 + lat_n - 1 + mem_n - 1)
    scratch = [
        v((members, levels, full, wide), BF16),
        v((members, full, 2 * wide), BF16),
        v((members, full, wide), BF16),
        v((members, full, wide), BF16),
        v((full, wide), F32),
        v((full, 2 * wide), F32),
        v((2, full, wide), F32),
        v((lon_n, 1, n_obs), jnp.int32),
        v((lon_n, 1, n_obs), F32),
        v((lon_n, 1, n_obs), F32),
        v((lon_n, levels * lon_cells, n_obs), BF16),
        v((2, levels, full, wide), F32),
        v((2, full, 2 * wide), F32),
        v((2, 2, full, wide), F32),
        v((lon_n, levels * lon_cells, wide), F32),
        v((2, group, lon_n, 1, n_obs), F32),
        v((2, lat_n, 2, 128), F32),
        v((2, levels, 2 * wide, 2 * wide), BF16),
        v((2, levels, 4 * wide, 2 * wide), BF16),
        v((levels, 2 * full, 2 * full), BF16),
        v((levels, 2 * lon_cells, 2 * reach), BF16),
        v((members, full, 4 * wide), BF16),
        v((half, levels, full, wide), F32),
        v((levels, 2 * full, half * wide), BF16),
        v((levels, 2 * reach, half * wide), BF16),
        pltpu.SMEM(band_width.shape, jnp.int32),
        sem((copies,)), sem((copies,)), sem((7,)),
        pltpu.SemaphoreType.REGULAR((max(lon_n + mem_n - 2, lat_n - 1) - 1,)),
    ]
    hbm = pl.BlockSpec(memory_space=pltpu.HBM)
    kernel = functools.partial(paired, dims=(members, levels, lon_cells, lat_cells, sizes))
    ens = jax.ShapeDtypeStruct((members, levels, lon_cells, lat_cells), F32)
    static = jax.ShapeDtypeStruct((levels, lon_cells, lat_cells), F32)
    parts = pl.pallas_call(
        kernel,
        out_shape=[
            ens, ens,
            jax.ShapeDtypeStruct((2, levels, lon_cells, lat_cells), F32),
            jax.ShapeDtypeStruct((2, 128), F32),
        ],
        in_specs=[hbm] * 6,
        out_specs=[VMEM] * 4,
        scratch_shapes=scratch,
        compiler_params=pltpu.CompilerParams(
            collective_id=0, has_side_effects=True, vmem_limit_bytes=48 * 2**20
        ),
    )(*(
        pltpu.with_memory_space_constraint(x, pltpu.HBM)
        for x in (
            anomalies, spread, obs_index.reshape(1, -1), obs_weight.reshape(1, -1),
            innovation.reshape(1, -1), band_width,
        )
    ))
    return pl.pallas_call(
        combine,
        out_shape=[ens, static],
        in_specs=[VMEM] * 4,
        out_specs=[hbm] * 2,
        scratch_shapes=[
            v(ens.shape, F32), v(static.shape, F32), sem((members + 1,)),
        ],
        compiler_params=pltpu.CompilerParams(vmem_limit_bytes=8 * 2**20),
    )(*parts)


def pick(*args):
    members = args[0].shape[0]
    levels, lon_cells, lat_cells = args[1].shape
    lon_n, lat_n, mem_n = (lax.axis_size(a) for a in AXES)
    pairs = lon_n == 2 and members % 2 == 0 and levels == mem_n and lon_cells % 32 == 0 and lat_n > 2
    return (paired_device if pairs else per_device)(*args)


def solution(mesh):
    return jax.shard_map(
        pick,
        mesh=mesh,
        in_specs=(
            P("mem", None, "lon", "lat"),
            P(None, "lon", "lat"),
            P("lon", "lat", None),
            P("lon", "lat", None),
            P("lon", "lat", None),
            P(),
        ),
        out_specs=(P("mem", None, "lon", "lat"), P(None, "lon", "lat")),
        check_vma=False,
    )
```

```python
import functools
import math

import jax
import jax.numpy as jnp
from jax import lax
from jax.experimental import pallas as pl
from jax.experimental.pallas import tpu as pltpu
from jax.sharding import PartitionSpec as P

BAND = 12
RIM = 2 * BAND

hybrid_ens = 0.75
hybrid_static = 0.25

MESH = pl.DeviceIdType.MESH
VMEM = pl.BlockSpec(memory_space=pltpu.VMEM)
F32 = jnp.float32
BF16 = jnp.bfloat16


def split2(x):
    hi = x.astype(BF16)
    return hi, (x - hi.astype(F32)).astype(BF16)


def dot3(left, right):
    lh, ll = left
    rh, rl = right
    d = functools.partial(jnp.dot, preferred_element_type=F32)
    return d(lh, rh) + (d(ll, rh) + d(lh, rl))


AXES = ("lon", "lat", "mem")


def fused(a_ref, s_ref, i_ref, w_ref, v_ref, bw_ref, ens_ref, static_ref, *scratch, dims):
    members, levels, lon_cells, lat_cells, sizes = dims
    (fc, fr, bc, br, qc, qr, send_al, send_ah, recv_al, recv_ah, pack_l, pack_h, recv_pl, recv_ph,
     fpack, xrh, xrl, two_c, two_r, two_l, one_c, one_r, one_l, bflat, dflat, cov, part,
     slots, slots2, dslots, dsend, smoothed_lat, send, recv, csend, crecv, dsems, drems) = scratch
    lon_n, lat_n, mem_n = sizes
    total = lon_n * lat_n * mem_n
    fields = members + 1
    ext = lon_cells + 2 * RIM
    rows = levels * lon_cells
    chunk = rows // mem_n
    coef_ens = math.sqrt(hybrid_ens / (members * mem_n))
    coef_static = math.sqrt(hybrid_static)
    mine = [lax.axis_index(a) for a in AXES]
    lat_at, me = mine[1], mine[2]
    has_low, has_high = lat_at > 0, lat_at < lat_n - 1

    def shifted(step):
        parts, rest = [], step
        for size in reversed(sizes):
            parts.append(rest % size)
            rest //= size
        return tuple(lax.rem(m + s, size) for m, s, size in zip(mine, reversed(parts), sizes))

    barrier = pltpu.get_barrier_semaphore()
    for step in range(1, total):
        pl.semaphore_signal(barrier, inc=1, device_id=shifted(step), device_id_type=MESH)

    used = [0]

    def remote(src, dst, where):
        k = used[0]
        used[0] += 1
        return pltpu.make_async_remote_copy(
            src_ref=src, dst_ref=dst, send_sem=send.at[k], recv_sem=recv.at[k],
            device_id=where, device_id_type=MESH,
        )

    lon_low = {"lon": lax.rem(mine[0] + lon_n - 1, lon_n)}
    lon_high = {"lon": lax.rem(mine[0] + 1, lon_n)}
    lat_low = {"lat": lax.rem(lat_at + lat_n - 1, lat_n)}
    lat_high = {"lat": lax.rem(lat_at + 1, lat_n)}
    own = pl.ds(0, lon_cells)
    rim = pl.ds(lon_cells, 2 * RIM)
    low_rows = pl.ds(lon_cells, RIM)
    high_rows = pl.ds(lon_cells + RIM, RIM)
    first_rows = pl.ds(0, RIM)
    last_rows = pl.ds(lon_cells - RIM, RIM)
    low_lanes = pl.ds(0, lat_cells)
    high_lanes = pl.ds(lat_cells, lat_cells)

    def lon_start(copies):
        for c in copies:
            c.start()

    def lon_wait(copies):
        for c in copies:
            c.wait()

    class Lat:
        def __init__(self, low_src, high_src, from_low, from_high):
            self.to_low = remote(low_src, from_high, lat_low)
            self.to_high = remote(high_src, from_low, lat_high)

        def start(self):
            pl.when(has_low)(self.to_low.start)
            pl.when(has_high)(self.to_high.start)

        def wait(self):
            pl.when(has_low)(self.to_low.wait_send)
            pl.when(has_high)(self.to_high.wait_send)
            pl.when(has_high)(self.to_low.wait_recv)
            pl.when(has_low)(self.to_high.wait_recv)

    def lane_pack(read, count):
        lane = lax.broadcasted_iota(jnp.int32, (count, lat_cells), 1)
        low = jnp.zeros((count, lat_cells), F32)
        high = low
        for l in range(levels):
            x = read(l)
            here = (lane >= l * RIM) & (lane < (l + 1) * RIM)
            low = jnp.where(here, pltpu.roll(x, (l * RIM) % lat_cells, 1), low)
            high = jnp.where(here, pltpu.roll(x, ((l + 1) * RIM) % lat_cells, 1), high)
        return low, high

    def zero_edges(ref, lead=()):
        @pl.when(jnp.logical_not(has_low))
        def _():
            ref[(*lead, slice(None), low_lanes)] = jnp.zeros((ext, lat_cells), F32)

        @pl.when(jnp.logical_not(has_high))
        def _():
            ref[(*lead, slice(None), high_lanes)] = jnp.zeros((ext, lat_cells), F32)

    def load_member(m, _):
        lows, highs = [], []
        for l in range(levels):
            x = a_ref[m, l].astype(F32)
            fc[l, m, :lon_cells, :] = x
            lows.append(x[:RIM])
            highs.append(x[lon_cells - RIM :])
        send_al[m] = jnp.concatenate(lows, axis=0).astype(BF16)
        send_ah[m] = jnp.concatenate(highs, axis=0).astype(BF16)
        return 0

    lax.fori_loop(0, members, load_member, 0)
    for l in range(levels):
        fc[l, members, :lon_cells, :] = s_ref[l]

    def pack_member(span, count):
        def go(m, _):
            low, high = lane_pack(lambda l: fc[l, m, span, :], count)
            pack_l[m, span, :] = low.astype(BF16)
            pack_h[m, span, :] = high.astype(BF16)
            return 0

        lax.fori_loop(0, members, go, 0)

    def lon_field(ref, lead):
        at = lambda span: ref.at[(slice(None), *lead, span, slice(None))]
        return [
            remote(at(first_rows), at(high_rows), lon_low),
            remote(at(last_rows), at(low_rows), lon_high),
        ]

    def lat_field(slot, dst, lead, span):
        at = lambda lanes: dst.at[(*lead, span, lanes)]
        return Lat(
            fpack.at[slot, 0, span, :], fpack.at[slot, 1, span, :], at(low_lanes), at(high_lanes)
        )

    def fill_pack(slot, read, span, count):
        low, high = lane_pack(lambda l: read(l, span), count)
        fpack[slot, 0, span, :] = low
        fpack[slot, 1, span, :] = high

    read_s = lambda l, span: fc[l, members, span, :]
    read_b = lambda l, span: bc[l, span, :]
    read_q = lambda l, span: qc[l, span, :]

    pl.semaphore_wait(barrier, total - 1)
    lon_a = [remote(send_al, recv_ah, lon_low), remote(send_ah, recv_al, lon_high)]
    lon_start(lon_a)
    lon_s = lon_field(fc, (members,))
    lon_start(lon_s)
    pack_member(own, lon_cells)
    lat_a = Lat(pack_l.at[:, own, :], pack_h.at[:, own, :], recv_pl.at[:, own, :], recv_ph.at[:, own, :])
    lat_a.start()

    idx, val_w = i_ref[...], w_ref[...]
    n_obs = idx.shape[1]
    row, lane = idx // lat_cells, idx % lat_cells
    at_row = (lax.broadcasted_iota(jnp.int32, (rows, n_obs), 0) == row).astype(F32).astype(BF16)
    at_lane = lax.broadcasted_iota(jnp.int32, (lat_cells, n_obs), 0) == lane
    for val, out in ((val_w, dflat), (val_w * v_ref[...], bflat)):
        acc = None
        for _ in range(3):
            piece_val = val.astype(BF16).astype(F32)
            val = val - piece_val
            placed = jnp.where(at_lane, piece_val, 0.0).astype(BF16)
            term = lax.dot_general(
                at_row, placed, (((1,), (1,)), ((), ())), preferred_element_type=F32
            )
            acc = term if acc is None else acc + term
        out[...] = acc
    for l in range(levels):
        bc[l, :lon_cells, :] = bflat[l * lon_cells : (l + 1) * lon_cells, :]
    lon_b = lon_field(bc, ())
    lon_start(lon_b)
    fill_pack(0, read_s, own, lon_cells)
    fill_pack(1, read_b, own, lon_cells)
    lat_sb = [lat_field(0, fr, (members,), own), lat_field(1, br, (), own)]
    for c in lat_sb:
        c.start()
    zero_edges(fr, (members,))
    zero_edges(br)
    zero_edges(qr)

    def iota(shape, dim):
        return lax.broadcasted_iota(jnp.int32, shape, dim)

    def ext_place(index, cells):
        return jnp.where(index < cells, index, jnp.where(index < cells + RIM, index - cells - RIM, index - RIM))

    def make_matrices(l, _):
        taps = (iota((8, 128), 1) - BAND).astype(F32)

        def weights(kind):
            width = bw_ref[kind, l].astype(F32) + jnp.zeros((1, 1), F32)

            def raw(o):
                return jnp.where(jnp.abs(o) <= width, jnp.exp(-0.5 * (o / (0.5 * width)) ** 2), 0.0)

            norm = jnp.sum(raw(taps)[:1], axis=1, keepdims=True)
            return lambda o: raw(o.astype(F32)) / norm

        def put(ref, where, value):
            hi, lo = split2(value)
            ref[(0, *where)] = hi
            ref[(1, *where)] = lo

        w = weights(0)
        mids = 128 * pl.cdiv(lon_cells + 2 * BAND, 128)
        near = w(iota((lon_cells, mids), 0) - (iota((lon_cells, mids), 1) - BAND))
        near = jnp.where(iota((lon_cells, mids), 1) < lon_cells + 2 * BAND, near, 0.0)
        far = w(iota((mids, ext), 0) - BAND - ext_place(iota((mids, ext), 1), lon_cells))
        put(two_l, (l,), dot3(split2(near), split2(far)))
        put(one_l, (l,), w(iota((lon_cells, ext), 0) - ext_place(iota((lon_cells, ext), 1), lon_cells)))

        w = weights(1)
        mids = 128 * pl.cdiv(lat_cells + 2 * BAND, 128)
        mid = iota((mids, lat_cells), 0) - BAND
        place = lat_at * lat_cells + mid
        keep = (place >= 0) & (place < lat_cells * lat_n) & (mid < lat_cells + BAND)
        back = split2(jnp.where(keep, w(mid - iota((mids, lat_cells), 1)), 0.0))
        out = iota((lat_cells, lat_cells), 1)
        here = iota((lat_cells, mids), 0) - (iota((lat_cells, mids), 1) - BAND)
        put(two_c, (l,), dot3(split2(w(here)), back))
        put(one_c, (l,), w(iota((lat_cells, lat_cells), 0) - out))
        columns = pl.ds(pl.multiple_of(l * lat_cells, lat_cells), lat_cells)
        for side in range(2):
            shift = -RIM if side == 0 else lat_cells
            span = pl.ds(side * lat_cells, lat_cells)

            def rim_at(shape):
                p = iota(shape, 0) - l * RIM
                return p + shift, (p >= 0) & (p < RIM)

            pos, ok = rim_at((lat_cells, mids))
            there = jnp.where(ok, w(pos - (iota((lat_cells, mids), 1) - BAND)), 0.0)
            put(two_r, (span, columns), dot3(split2(there), back))
            pos, ok = rim_at((lat_cells, lat_cells))
            put(one_r, (span, columns), jnp.where(ok, w(pos - out), 0.0))
        return 0

    lax.fori_loop(0, levels, make_matrices, 0)

    def lat_part(yc, yr, c_mat, r_mat, l, span, count):
        columns = pl.ds(pl.multiple_of(l * lat_cells, lat_cells), lat_cells)
        xc = split2((fc[l, :, span, :] * yc[l, span, :][None]).reshape(fields * count, lat_cells))
        xr = (
            xrh[:, span, :].reshape(fields * count, 2 * lat_cells),
            xrl[:, span, :].reshape(fields * count, 2 * lat_cells),
        )
        t = dot3(xc, (c_mat[0, l], c_mat[1, l]))
        t = t + dot3(xr, (r_mat[0, :, columns], r_mat[1, :, columns]))
        for h, half in enumerate(split2(t)):
            smoothed_lat[h, l, span, :] = jnp.concatenate(
                [half[f * count : (f + 1) * count] for f in range(fields)], axis=1
            )

    def rim_products(yr, span):
        def go(f, _):
            hi, lo = split2(fr[f, span, :] * yr[span, :])
            xrh[f, span, :], xrl[f, span, :] = hi, lo
            return 0

        lax.fori_loop(0, fields, go, 0)

    def apply_own(yc, yr, mats):
        rim_products(yr, own)

        def go(l, _):
            lat_part(yc, yr, mats[0], mats[1], l, own, lon_cells)
            return 0

        lax.fori_loop(0, levels, go, 0)

    def apply_rim(yc, yr, mats, finish):
        rim_products(yr, rim)

        def go(i, _):
            l = lax.rem(me + 1 + i, levels)
            lat_part(yc, yr, mats[0], mats[1], l, rim, 2 * RIM)
            u = dot3((mats[2][0, l], mats[2][1, l]), (smoothed_lat[0, l], smoothed_lat[1, l]))
            finish(i, l, [u[:, f * lat_cells : (f + 1) * lat_cells] for f in range(fields)])
            return 0

        lax.fori_loop(0, levels, go, 0)

    def unpack_lat(span, count):
        for ref, keep, lanes in ((recv_pl, has_low, low_lanes), (recv_ph, has_high, high_lanes)):
            def go(m, _):
                fr[m, span, lanes] = ref[m, span, :].astype(F32)
                return 0

            def clear(m, _):
                fr[m, span, lanes] = jnp.zeros((count, lat_cells), F32)
                return 0

            @pl.when(keep)
            def _():
                lax.fori_loop(0, members, go, 0)

            @pl.when(jnp.logical_not(keep))
            def _():
                lax.fori_loop(0, members, clear, 0)

    lat_a.wait()
    unpack_lat(own, lon_cells)
    for c in lat_sb:
        c.wait()
    apply_own(bc, br, (two_c, two_r, two_l))

    lon_wait(lon_a)

    def unpack_member(m, _):
        low, high = recv_al[m].astype(F32), recv_ah[m].astype(F32)
        for l in range(levels):
            fc[l, m, low_rows, :] = low[l * RIM : (l + 1) * RIM]
            fc[l, m, high_rows, :] = high[l * RIM : (l + 1) * RIM]
        return 0

    lax.fori_loop(0, members, unpack_member, 0)
    pack_member(rim, 2 * RIM)
    lat_a2 = Lat(pack_l.at[:, rim, :], pack_h.at[:, rim, :], recv_pl.at[:, rim, :], recv_ph.at[:, rim, :])
    lat_a2.start()
    lon_wait(lon_s)
    lon_wait(lon_b)
    fill_pack(0, read_s, rim, 2 * RIM)
    fill_pack(1, read_b, rim, 2 * RIM)
    lat_sb2 = [lat_field(0, fr, (members,), rim), lat_field(1, br, (), rim)]
    for c in lat_sb2:
        c.start()
    lat_a2.wait()
    unpack_lat(rim, 2 * RIM)
    for c in lat_sb2:
        c.wait()

    def piece(owner):
        return pl.ds(pl.multiple_of(owner * chunk, chunk), chunk)

    def mem_copy(src, dst, j, group):
        return pltpu.make_async_remote_copy(
            src_ref=src, dst_ref=dst, send_sem=csend.at[group, j], recv_sem=crecv.at[group, j],
            device_id={"mem": lax.rem(me + j, mem_n)}, device_id_type=MESH,
        )

    def sum_copy(dst, j, group):
        return mem_copy(part.at[piece(lax.rem(me + j, mem_n))], dst.at[j], j, group)

    by_level = levels == mem_n

    def finish_cov(dst, group):
        def finish(i, l, smoothed):
            acc = fc[l, 0, :lon_cells, :] * smoothed[0]
            for f in range(1, members):
                acc = acc + fc[l, f, :lon_cells, :] * smoothed[f]
            acc = acc * (coef_ens * coef_ens)
            acc = acc + fc[l, members, :lon_cells, :] * smoothed[members] * (coef_static**2 / mem_n)
            part[pl.ds(pl.multiple_of(l * lon_cells, lon_cells), lon_cells), :] = acc
            if by_level:
                @pl.when(i < mem_n - 1)
                def _():
                    sum_copy(dst, i + 1, group).start()

        return finish

    def scatter_sum(dst, group):
        copies = [sum_copy(dst, j, group) for j in range(1, mem_n)]
        if not by_level:
            for copy in copies:
                copy.start()
        acc = part[piece(me), :]
        for j, copy in enumerate(copies):
            copy.wait_recv()
            acc = acc + dst[j + 1]
        for copy in copies:
            copy.wait_send()
        return acc

    def dots_start(left, right, group):
        at = iota((2, lat_cells), 0)
        a = jnp.sum(left, axis=0, keepdims=True)
        b = jnp.sum(right, axis=0, keepdims=True)
        dsend[group] = jnp.where(at == 0, a, b)
        copies = []
        for step in range(1, total):
            copy = pltpu.make_async_remote_copy(
                src_ref=dsend.at[group], dst_ref=dslots.at[group, step],
                send_sem=dsems.at[group, step], recv_sem=drems.at[group, step],
                device_id=shifted(step), device_id_type=MESH,
            )
            copy.start()
            copies.append(copy)
        return copies

    def dots_end(copies, group):
        for copy in copies:
            copy.wait()
        block = dsend[group] + jnp.sum(dslots[group, 1:], axis=0)
        sums = jnp.sum(block, axis=1, keepdims=True)
        return sums[0:1], sums[1:2]

    two, one = (two_c, two_r, two_l), (one_c, one_r, one_l)
    apply_rim(bc, br, two, finish_cov(slots, 0))
    acc = scatter_sum(slots, 0)
    cov[piece(me), :] = acc
    back = [mem_copy(cov.at[piece(me)], cov.at[piece(me)], j, 1) for j in range(1, mem_n)]
    for copy in back:
        copy.start()
    rhs_mine, diag_mine, cov_mine = bflat[piece(me), :], dflat[piece(me), :], acc
    image_mine = rhs_mine + diag_mine * cov_mine
    dots0 = dots_start(rhs_mine * cov_mine, cov_mine * image_mine, 0)
    for copy in back:
        copy.wait()
    for l in range(levels):
        span = slice(l * lon_cells, (l + 1) * lon_cells)
        qc[l, :lon_cells, :] = bflat[span, :] + dflat[span, :] * cov[span, :]
    lon_q = lon_field(qc, ())
    lon_start(lon_q)
    fill_pack(2, read_q, own, lon_cells)
    lat_q = lat_field(2, qr, (), own)
    lat_q.start()
    lon_wait(lon_q)
    fill_pack(2, read_q, rim, 2 * RIM)
    lat_q2 = lat_field(2, qr, (), rim)
    lat_q2.start()
    lat_q.wait()

    apply_own(qc, qr, two)
    lat_q2.wait()
    apply_rim(qc, qr, two, finish_cov(slots2, 2))
    cov_q = scatter_sum(slots2, 2)
    norm0, curve0 = dots_end(dots0, 0)
    alpha0 = norm0 / curve0
    resid = rhs_mine - alpha0 * image_mine
    cov_r = cov_mine - alpha0 * cov_q
    norm1, curve1 = dots_end(dots_start(resid * cov_r, cov_r * (resid + diag_mine * cov_r), 1), 1)
    beta = norm1 / norm0
    alpha1 = norm1 / (curve1 - beta * norm1 / alpha0)

    def combine(b, q):
        return alpha0 * b + alpha1 * ((b - alpha0 * q) + beta * b)

    for l in range(levels):
        bc[l] = combine(bc[l], qc[l])
    br[...] = combine(br[...], qr[...])

    def finish_control(i, l, smoothed):
        for f in range(members):
            ens_ref[f, l] = coef_ens * smoothed[f]
        static_ref[l] = coef_static * smoothed[members]

    apply_own(bc, br, one)
    apply_rim(bc, br, one, finish_control)


def per_device(anomalies, spread, obs_index, innovation, obs_weight, band_width):
    members = anomalies.shape[0]
    levels, lon_cells, lat_cells = spread.shape
    sizes = tuple(lax.axis_size(a) for a in AXES)
    mem_n, total = sizes[2], math.prod(sizes)
    fields = members + 1
    ext = lon_cells + 2 * RIM
    rows = levels * lon_cells
    chunk = rows // mem_n
    v = pltpu.VMEM
    sem = pltpu.SemaphoreType.DMA
    edge = v((members, levels * RIM, lat_cells), BF16)
    packed = v((members, ext, lat_cells), BF16)
    field = v((levels, ext, lat_cells), F32)
    field_rim = v((ext, 2 * lat_cells), F32)
    mats = [
        v((2, levels, lat_cells, lat_cells), BF16),
        v((2, 2 * lat_cells, levels * lat_cells), BF16),
        v((2, levels, lon_cells, ext), BF16),
    ]
    flat = v((rows, lat_cells), F32)
    scratch = [
        v((levels, fields, ext, lat_cells), F32),
        v((fields, ext, 2 * lat_cells), F32),
        field, field_rim, field, field_rim,
        edge, edge, edge, edge,
        packed, packed, packed, packed,
        v((3, 2, ext, lat_cells), F32),
        v((fields, ext, 2 * lat_cells), BF16),
        v((fields, ext, 2 * lat_cells), BF16),
        *mats, *mats,
        flat, flat, flat, flat,
        v((mem_n, chunk, lat_cells), F32),
        v((mem_n, chunk, lat_cells), F32),
        v((2, total, 2, lat_cells), F32),
        v((2, 2, lat_cells), F32),
        v((2, levels, ext, fields * lat_cells), BF16),
        sem((32,)), sem((32,)), sem((3, mem_n)), sem((3, mem_n)), sem((2, total)), sem((2, total)),
    ]
    kernel = functools.partial(fused, dims=(members, levels, lon_cells, lat_cells, sizes))
    return pl.pallas_call(
        kernel,
        out_shape=[
            jax.ShapeDtypeStruct((members, levels, lon_cells, lat_cells), F32),
            jax.ShapeDtypeStruct((levels, lon_cells, lat_cells), F32),
        ],
        in_specs=[VMEM] * 5 + [pl.BlockSpec(memory_space=pltpu.SMEM)],
        out_specs=[VMEM] * 2,
        scratch_shapes=scratch,
        compiler_params=pltpu.CompilerParams(
            collective_id=0, has_side_effects=True, vmem_limit_bytes=60 * 2**20
        ),
    )(
        anomalies, spread, obs_index.reshape(1, -1), obs_weight.reshape(1, -1),
        innovation.reshape(1, -1), band_width,
    )


def paired(a_hbm, s_hbm, i_hbm, w_hbm, v_hbm, bw_hbm, ub_ref, uq_ref, st_ref, coef_ref, *scratch, dims):
    members, levels, lon_cells, lat_cells, sizes = dims
    (acen, arim, plo, phi, sfull, sedge, srim, srims, spack, spacks, oidx, ow, ov, at_row, grid, grim, gpack, cov, orecv,
     drecv, mat_c, mat_r, lon_t, lon_l, xr, xq, xo, tc, ts, to, bw_ref, send, recv, load, relay) = scratch
    lon_n, lat_n, mem_n = sizes
    half = members // lon_n
    full = lon_n * lon_cells
    group = lon_n * mem_n
    rows = levels * lon_cells
    wide = lat_cells
    edge = 16 * pl.cdiv(BAND, 16)
    reach = lon_cells + 2 * edge
    n_obs = oidx.shape[2]
    coef_ens = math.sqrt(hybrid_ens / (members * mem_n))
    coef_static = math.sqrt(hybrid_static)
    at_lon, lat_at, me = (lax.axis_index(a) for a in AXES)
    other = 1 - at_lon
    has_low, has_high = lat_at > 0, lat_at < lat_n - 1
    my_id = at_lon * mem_n + me

    def group_peer(step):
        peer = lax.rem(my_id + step, group)
        return {"lon": peer // mem_n, "mem": lax.rem(peer, mem_n)}

    def lat_peer(step):
        return {"lat": lax.rem(lat_at + step, lat_n)}

    own_rows, far_rows = pl.ds(0, lon_cells), pl.ds(lon_cells, lon_cells)
    first, second = pl.ds(0, half), pl.ds(half, half)
    loads = [
        pltpu.make_async_copy(src, dst, load.at[k])
        for k, (src, dst) in enumerate((
            (i_hbm, oidx.at[0]),
            (w_hbm, ow.at[0]),
            (v_hbm, ov.at[0]),
            (s_hbm, sfull.at[:, own_rows]),
            (a_hbm.at[pl.ds(other * half, half)], acen.at[second, :, own_rows, :]),
            (a_hbm.at[pl.ds(at_lon * half, half)], acen.at[first, :, own_rows, :]),
            (bw_hbm, bw_ref),
        ))
    ]
    for copy in loads:
        copy.start()

    near = [
        (True, {"lon": other}),
        (has_low, {"lat": lat_at - 1}),
        (has_high, {"lat": lat_at + 1}),
        (me > 0, {"mem": me - 1}),
        (me < mem_n - 1, {"mem": me + 1}),
    ]
    n_near = sum(jnp.asarray(there, jnp.int32) for there, _ in near)

    def greet(sem):
        for there, where in near:
            def go(where=where):
                pl.semaphore_signal(sem, inc=1, device_id=where, device_id_type=MESH)

            go() if there is True else pl.when(there)(go)

    def relay_round(r):
        pl.semaphore_wait(relay.at[r], n_near)
        if r + 1 < rounds:
            greet(relay.at[r + 1])

    rounds = max(lon_n + mem_n - 2, lat_n - 1) - 1
    barrier = pltpu.get_barrier_semaphore()
    greet(barrier)

    used = [0]

    def remote(src, dst, where):
        k = used[0]
        used[0] += 1
        return pltpu.make_async_remote_copy(
            src_ref=src, dst_ref=dst, send_sem=send.at[k], recv_sem=recv.at[k],
            device_id=where, device_id_type=MESH,
        )

    partner = {"lon": other}
    lat_low = {"lat": lax.rem(lat_at + lat_n - 1, lat_n)}
    lat_high = {"lat": lax.rem(lat_at + 1, lat_n)}
    low_lanes = pl.ds(0, wide)
    high_lanes = pl.ds(wide, wide)

    class Lat:
        def __init__(self, low_src, high_src, from_low, from_high):
            self.to_low = remote(low_src, from_high, lat_low)
            self.to_high = remote(high_src, from_low, lat_high)

        def start(self):
            pl.when(has_low)(self.to_low.start)
            pl.when(has_high)(self.to_high.start)

        def wait(self):
            pl.when(has_low)(self.to_low.wait_send)
            pl.when(has_high)(self.to_high.wait_send)
            pl.when(has_high)(self.to_low.wait_recv)
            pl.when(has_low)(self.to_high.wait_recv)

    def iota(shape, dim):
        return lax.broadcasted_iota(jnp.int32, shape, dim)

    def lane_pack(read, count, at_levels=None):
        lane = iota((count, wide), 1)
        low = jnp.zeros((count, wide), F32)
        high = low
        for l in range(levels) if at_levels is None else at_levels:
            x = read(l)
            here = (lane >= l * RIM) & (lane < (l + 1) * RIM)
            low = jnp.where(here, pltpu.roll(x, lax.rem(l * RIM, wide), 1), low)
            high = jnp.where(here, pltpu.roll(x, lax.rem((l + 1) * RIM, wide), 1), high)
        return low, high

    def pack_member(p, span, count):
        low, high = lane_pack(lambda l: acen[p, l, span, :].astype(F32), count)
        plo[p, span, :] = low.astype(BF16)
        phi[p, span, :] = high.astype(BF16)

    def pack_static(span, count):
        low, high = lane_pack(lambda l: sfull[me, span, :], count, [me])
        spack[0, span, :] = low
        spack[1, span, :] = high

    def pack_statics(ref, span, to_span, count):
        low, high = lane_pack(lambda l: ref[l, span, :], count)
        spacks[0, to_span, :] = low
        spacks[1, to_span, :] = high

    def lat_members(which, span):
        return Lat(
            plo.at[which, span, :], phi.at[which, span, :],
            arim.at[which, span, low_lanes], arim.at[which, span, high_lanes],
        )

    def lat_static(span, pack=spack, rim=srim):
        return Lat(
            pack.at[0, span, :], pack.at[1, span, :],
            rim.at[span, low_lanes], rim.at[span, high_lanes],
        )

    def lat_grid(g):
        return Lat(gpack.at[g, 0], gpack.at[g, 1], grim.at[g, :, low_lanes], grim.at[g, :, high_lanes])

    x_obs = [remote(ref.at[0], ref.at[1], partner) for ref in (oidx, ow, ov)]
    x_static = remote(sfull.at[me, own_rows], sfull.at[me, far_rows], partner)
    x_first = [
        remote(acen.at[half + p, :, own_rows, :], acen.at[p, :, far_rows, :], partner)
        for p in range(half)
    ]
    edges = pl.ds(lon_cells, 2 * edge)
    x_edge = []
    for src, k in ((0, 0), (lon_cells - edge, edge)):
        src, dst = pl.ds(src, edge), pl.ds(lon_cells + k, edge)
        x_edge.append(remote(acen.at[first, :, src, :], acen.at[second, :, dst, :], partner))
        x_edge.append(remote(sfull.at[:, src], sedge.at[:, pl.ds(k, edge)], partner))
    for copy in loads:
        copy.wait()
    pl.semaphore_wait(barrier, n_near)
    for copy in [*x_obs, *x_first, x_static]:
        copy.start()
    greet(relay.at[0])

    def pack_first(p, _):
        pack_member(p, own_rows, lon_cells)
        return 0

    lax.fori_loop(0, half, pack_first, 0)
    lat_a = lat_members(first, own_rows)
    lat_a.start()
    pack_static(own_rows, lon_cells)
    lat_s = lat_static(own_rows)
    lat_s.start()
    lax.fori_loop(half, members, pack_first, 0)
    lat_a3 = lat_members(second, own_rows)
    lat_a3.start()
    pack_statics(sfull, own_rows, own_rows, lon_cells)
    lat_s3 = lat_static(own_rows, spacks, srims)
    lat_s3.start()

    @pl.when(jnp.logical_not(has_low))
    def _():
        arim[:, :, low_lanes] = jnp.zeros((members, full, wide), BF16)
        srim[:, low_lanes] = jnp.zeros((full, wide), F32)
        srims[:, low_lanes] = jnp.zeros((reach, wide), F32)
        grim[:, :, low_lanes] = jnp.zeros((2, full, wide), F32)

    @pl.when(jnp.logical_not(has_high))
    def _():
        arim[:, :, high_lanes] = jnp.zeros((members, full, wide), BF16)
        srim[:, high_lanes] = jnp.zeros((full, wide), F32)
        srims[:, high_lanes] = jnp.zeros((reach, wide), F32)
        grim[:, :, high_lanes] = jnp.zeros((2, full, wide), F32)

    relay_round(0)
    slot_rows = (own_rows, far_rows)
    slot_tile = (at_lon, other)

    def mark_rows(s):
        row = oidx[s] // wide
        at_row[s] = (iota((rows, n_obs), 0) == row).astype(F32).astype(BF16)

    def scatter(s, value, g):
        at_lane = iota((wide, n_obs), 0) == oidx[s] % wide
        hi = value.astype(BF16).astype(F32)
        lo = value - hi
        placed = jnp.concatenate(
            [jnp.where(at_lane, hi, 0.0).astype(BF16), jnp.where(at_lane, lo, 0.0).astype(BF16)], axis=0
        )
        out = lax.dot_general(
            at_row[s], placed, (((1,), (1,)), ((), ())), preferred_element_type=F32
        )
        out = out[:, :wide] + out[:, wide:]
        for l in range(levels):
            grid[g, l, slot_rows[s], :] = out[l * lon_cells : (l + 1) * lon_cells]

    def gather(s, g):
        hi, lo = split2(cov[s].T)
        left = jnp.concatenate([hi, lo], axis=0)
        step = 512 if n_obs % 512 == 0 else n_obs
        for c in range(0, n_obs, step):
            part = jnp.dot(left, at_row[s, :, c : c + step], preferred_element_type=F32)
            lane = oidx[s, :, c : c + step] % wide
            here = iota((wide, step), 0) == lane
            value = jnp.where(here, part[:wide] + part[wide:], 0.0)
            orecv[g, my_id, slot_tile[s], :, c : c + step] = jnp.sum(value, axis=0, keepdims=True)

    def send_grid(g):
        low, high = lane_pack(lambda l: grid[g, l], full)
        gpack[g, 0] = low
        gpack[g, 1] = high
        copy = lat_grid(g)
        copy.start()
        return copy

    mark_rows(0)
    scatter(0, ow[0] * ov[0], 0)

    def make_matrices(l, _):
        taps = (iota((8, 128), 1) - BAND).astype(F32)

        def weights(kind):
            width = bw_ref[kind, l].astype(F32) + jnp.zeros((1, 1), F32)

            def raw(o):
                return jnp.where(jnp.abs(o) <= width, jnp.exp(-0.5 * (o / (0.5 * width)) ** 2), 0.0)

            norm = jnp.sum(raw(taps)[:1], axis=1, keepdims=True)
            return lambda o: raw(o.astype(F32)) / norm

        def put_lon(ref, count, value):
            hi, lo = split2(value)
            cols = value.shape[1]
            ref[l, :count, :] = jnp.concatenate([hi, hi], axis=1)
            ref[l, count:, :] = jnp.concatenate([lo, jnp.zeros((count, cols), BF16)], axis=1)

        w = weights(0)

        def ring(count, cols):
            c = iota((count, cols), 1)
            if cols < full:
                c = jnp.where(c < lon_cells + edge, c, c + full - cols)
            d = c - iota((count, cols), 0)
            d = jnp.where(d > full // 2, d - full, d)
            return w(jnp.where(d < -(full // 2), d + full, d))

        circle = split2(ring(full, full))
        put_lon(lon_t, full, dot3(circle, circle))
        put_lon(lon_l, lon_cells, ring(lon_cells, reach))

        def put_lat(ref, kind, hi_at, lo_at, value):
            hi, lo = split2(value)
            ref[kind, l, pl.ds(hi_at, wide), :wide] = hi
            ref[kind, l, pl.ds(hi_at, wide), wide:] = lo
            ref[kind, l, pl.ds(lo_at, wide), :wide] = hi
            ref[kind, l, pl.ds(lo_at, wide), wide:] = jnp.zeros((wide, wide), BF16)

        w = weights(1)
        mids = 128 * pl.cdiv(wide + 2 * BAND, 128)
        mid = iota((mids, wide), 0) - BAND
        place = lat_at * wide + mid
        keep = (place >= 0) & (place < wide * lat_n) & (mid < wide + BAND)
        back = split2(jnp.where(keep, w(mid - iota((mids, wide), 1)), 0.0))
        out = iota((wide, wide), 1)
        here = iota((wide, mids), 0) - (iota((wide, mids), 1) - BAND)
        put_lat(mat_c, 0, 0, wide, dot3(split2(w(here)), back))
        put_lat(mat_c, 1, 0, wide, w(iota((wide, wide), 0) - out))
        for side in range(2):
            shift = -RIM if side == 0 else wide

            def rim_at(shape):
                p = iota(shape, 0) - l * RIM
                return p + shift, (p >= 0) & (p < RIM)

            pos, ok = rim_at((wide, mids))
            there = jnp.where(ok, w(pos - (iota((wide, mids), 1) - BAND)), 0.0)
            put_lat(mat_r, 0, side * wide, (2 + side) * wide, dot3(split2(there), back))
            pos, ok = rim_at((wide, wide))
            put_lat(mat_r, 1, side * wide, (2 + side) * wide, jnp.where(ok, w(pos - out), 0.0))
        return 0

    lax.fori_loop(0, levels, make_matrices, 0)
    for r in range(1, rounds):
        relay_round(r)

    for copy in x_obs:
        copy.wait()
    mark_rows(1)
    scatter(1, ow[1] * ov[1], 0)
    lat_b = send_grid(0)

    def dot(a, b):
        return jnp.dot(a, b, preferred_element_type=F32)

    def fold(t):
        return t[:, :wide] + t[:, wide:]

    def pair(x):
        return jnp.concatenate(split2(x), axis=1)

    def stack(x):
        return jnp.concatenate(split2(x), axis=0)

    def reached(x):
        return jnp.concatenate([x[: lon_cells + edge], x[full - edge :]], axis=0)

    def rim_member(g, p):
        xr[p] = pair(arim[p].astype(F32) * grim[g])

    def center_member(g, p):
        for l in range(levels):
            tc[p, l] = fold(dot(pair(acen[p, l].astype(F32) * grid[g, l]), mat_c[0, l]))

    def lat_member(p, at):
        for l in range(levels):
            ts[l, :, at] = stack(tc[p, l] + fold(dot(xr[p], mat_r[0, l])))

    def cov_level(l):
        u = dot(lon_t[l], ts[l])
        u = u[:full] + u[full:]
        acc = acen[0, l].astype(F32) * u[:, :wide]
        for p in range(1, half):
            acc = acc + acen[p, l].astype(F32) * u[:, p * wide : (p + 1) * wide]
        acc = acc * (coef_ens * coef_ens)
        for j in range(lon_n):
            cov[j, l * lon_cells : (l + 1) * lon_cells, :] = acc[j * lon_cells : (j + 1) * lon_cells]

    def cov_static(g):
        t = dot(pair(sfull[me] * grid[g, me]), mat_c[0, me])
        t = t + dot(pair(srim[...] * grim[g]), mat_r[0, me])
        u = dot(lon_t[me], stack(fold(t)))
        acc = sfull[me] * (u[:full] + u[full:]) * (coef_static**2 / lon_n)
        at = pl.ds(pl.multiple_of(me * lon_cells, lon_cells), lon_cells)
        for j in range(lon_n):
            cov[j, at, :] = cov[j, at, :] + acc[j * lon_cells : (j + 1) * lon_cells]

    lat_a2 = []
    for p in range(half):
        x_first[p].wait()
        pack_member(p, far_rows, lon_cells)
        copy = lat_members(p, far_rows)
        copy.start()
        lat_a2.append(copy)
        center_member(0, p)
    x_static.wait()
    for copy in x_edge:
        copy.start()
    pack_static(far_rows, lon_cells)
    lat_s2 = lat_static(far_rows)
    lat_s2.start()

    def share(g):
        for s in range(lon_n):
            gather(s, g)
        copies = []
        for step in range(1, group):
            copy = remote(orecv.at[g, my_id], orecv.at[g, my_id], group_peer(step))
            copy.start()
            copies.append(copy)
        return copies

    def shared(copies, g):
        for copy in copies:
            copy.wait()
        sums = []
        for s in range(lon_n):
            acc = orecv[g, 0, slot_tile[s]]
            for k in range(1, group):
                acc = acc + orecv[g, k, slot_tile[s]]
            sums.append(acc)
        return sums

    def out_rows(l, cells, reads):
        n = len(reads)
        for p, read in enumerate(reads):
            xo[p * reach : (p + 1) * reach] = pair(read() * cells)
        t = fold(dot(xo[: n * reach], mat_c[1, l]) + dot(xq[: n * reach], mat_r[1, l]))
        for p in range(n):
            to[l, :, p * wide : (p + 1) * wide] = stack(t[p * reach : (p + 1) * reach])
        u = dot(lon_l[l], to[l, :, : n * wide])
        u = u[:lon_cells] + u[lon_cells:]
        return [u[:, p * wide : (p + 1) * wide] for p in range(n)]

    def out_first(g):
        out_ref = (ub_ref, uq_ref)[g]
        for p in range(half):
            xq[p * reach : (p + 1) * reach] = reached(xr[p])

        def go(l, _):
            reads = [lambda p=p: reached(acen[p, l]).astype(F32) for p in range(half)]
            for p, u in enumerate(out_rows(l, reached(grid[g, l]), reads)):
                out_ref[at_lon * half + p, l] = u * coef_ens
            return 0

        lax.fori_loop(0, levels, go, 0)

    def out_second(g):
        out_ref = (ub_ref, uq_ref)[g]
        near_rim = reached(grim[g])
        for p in range(half):
            xq[p * reach : (p + 1) * reach] = pair(arim[half + p, :reach].astype(F32) * near_rim)
        xq[half * reach :] = pair(srims[...] * near_rim)

        def go(l, _):
            reads = [lambda p=p: acen[half + p, l, :reach].astype(F32) for p in range(half)]
            reads.append(lambda: jnp.concatenate([sfull[l, :lon_cells], sedge[l]], axis=0))
            us = out_rows(l, reached(grid[g, l]), reads)
            for p in range(half):
                out_ref[other * half + p, l] = us[p] * coef_ens
            st_ref[g, l] = us[half] * coef_static
            return 0

        lax.fori_loop(0, levels, go, 0)

    def dots_start(g, left, right):
        def total(pairs):
            acc = None
            for x in pairs:
                for c in range(0, n_obs, 128):
                    part = x[:, c : c + 128]
                    acc = part if acc is None else acc + part
            return acc

        at = iota((2, 128), 0)
        drecv[g, lat_at] = jnp.where(at == 0, total(left), total(right))
        copies = []
        for step in range(1, lat_n):
            copy = remote(drecv.at[g, lat_at], drecv.at[g, lat_at], lat_peer(step))
            copy.start()
            copies.append(copy)
        return copies

    def dots_end(copies, g):
        for copy in copies:
            copy.wait()
        block = drecv[g, 0]
        for k in range(1, lat_n):
            block = block + drecv[g, k]
        sums = jnp.sum(block, axis=1, keepdims=True)
        return sums[0:1], sums[1:2]

    def rim_and_cov(g):
        for p in range(half):
            if g == 0:
                lat_a2[p].wait()
            rim_member(g, p)
            if g == 0:
                lat_member(p, slice(p * wide, (p + 1) * wide))
        if g > 0:
            rims = xr[:half].reshape(half * full, 4 * wide)
            for l in range(levels):
                t = fold(dot(rims, mat_r[0, l]))
                for p in range(half):
                    part = tc[p, l] + t[p * full : (p + 1) * full]
                    ts[l, :, p * wide : (p + 1) * wide] = stack(part)
        for l in range(levels):
            cov_level(l)
        if g == 0:
            lat_s.wait()
            lat_s2.wait()
        cov_static(g)
        return share(g)

    lat_b.wait()
    lat_a.wait()
    sharing = rim_and_cov(0)

    for copy in x_edge:
        copy.wait()

    def pack_second(p, _):
        pack_member(p, edges, 2 * edge)
        return 0

    lax.fori_loop(half, members, pack_second, 0)
    lat_a4 = lat_members(second, edges)
    lat_a4.start()
    pack_statics(sedge, slice(None), edges, 2 * edge)
    lat_s4 = lat_static(edges, spacks, srims)
    lat_s4.start()
    out_first(0)

    cz = shared(sharing, 0)
    z = [ow[s] * ov[s] for s in range(lon_n)]
    q = [z[s] + ow[s] * cz[s] for s in range(lon_n)]
    for s in range(lon_n):
        scatter(s, q[s], 1)
    lat_q = send_grid(1)
    dots0 = dots_start(0, [z[s] * cz[s] for s in range(lon_n)], [cz[s] * q[s] for s in range(lon_n)])

    def center_all(l, _):
        for p in range(half):
            xo[p * full : (p + 1) * full] = pair(acen[p, l].astype(F32) * grid[1, l])
        t = fold(dot(xo[: half * full], mat_c[0, l]))
        for p in range(half):
            tc[p, l] = t[p * full : (p + 1) * full]
        return 0

    lax.fori_loop(0, levels, center_all, 0)
    for copy in (lat_a3, lat_a4, lat_s3, lat_s4):
        copy.wait()
    out_second(0)

    lat_q.wait()
    sharing = rim_and_cov(1)
    out_first(1)
    out_second(1)

    cq = shared(sharing, 1)
    norm0, curve0 = dots_end(dots0, 0)
    alpha0 = norm0 / curve0
    resid = [z[s] - alpha0 * q[s] for s in range(lon_n)]
    cr = [cz[s] - alpha0 * cq[s] for s in range(lon_n)]
    dots1 = dots_start(
        1,
        [resid[s] * cr[s] for s in range(lon_n)],
        [cr[s] * (resid[s] + ow[s] * cr[s]) for s in range(lon_n)],
    )
    norm1, curve1 = dots_end(dots1, 1)
    beta = norm1 / norm0
    alpha1 = norm1 / (curve1 - beta * norm1 / alpha0)
    on_b = alpha0 + alpha1 * (1.0 + beta)
    on_q = -alpha0 * alpha1
    coef_ref[...] = jnp.where(iota((2, 128), 0) == 0, on_b, on_q)


def combine(ub_ref, uq_ref, st_ref, coef_ref, ens_ref, static_ref, ens, static, sems):
    on_b, on_q = coef_ref[0:1, :], coef_ref[1:2, :]
    members = ens.shape[0]
    copies = []
    for m in range(members):
        ens[m] = on_b * ub_ref[m] + on_q * uq_ref[m]
        copies.append(pltpu.make_async_copy(ens.at[m], ens_ref.at[m], sems.at[m]))
        copies[-1].start()
    static[...] = on_b * st_ref[0] + on_q * st_ref[1]
    copies.append(pltpu.make_async_copy(static, static_ref, sems.at[members]))
    copies[-1].start()
    for copy in copies:
        copy.wait()


def paired_device(anomalies, spread, obs_index, innovation, obs_weight, band_width):
    members = anomalies.shape[0]
    levels, lon_cells, lat_cells = spread.shape
    sizes = tuple(lax.axis_size(a) for a in AXES)
    lon_n, lat_n, mem_n = sizes
    half = members // lon_n
    full = lon_n * lon_cells
    group = lon_n * mem_n
    n_obs = obs_index.shape[-1]
    v = pltpu.VMEM
    sem = pltpu.SemaphoreType.DMA
    wide = lat_cells
    reach = lon_cells + 2 * 16 * pl.cdiv(BAND, 16)
    copies = 8 + half + 2 * (9 + half) + 2 * (group - 1 + lat_n - 1)
    scratch = [
        v((members, levels, full, wide), BF16),
        v((members, full, 2 * wide), BF16),
        v((members, full, wide), BF16),
        v((members, full, wide), BF16),
        v((levels, full, wide), F32),
        v((levels, reach - lon_cells, wide), F32),
        v((full, 2 * wide), F32),
        v((reach, 2 * wide), F32),
        v((2, full, wide), F32),
        v((2, reach, wide), F32),
        v((lon_n, 1, n_obs), jnp.int32),
        v((lon_n, 1, n_obs), F32),
        v((lon_n, 1, n_obs), F32),
        v((lon_n, levels * lon_cells, n_obs), BF16),
        v((2, levels, full, wide), F32),
        v((2, full, 2 * wide), F32),
        v((2, 2, full, wide), F32),
        v((lon_n, levels * lon_cells, wide), F32),
        v((2, group, lon_n, 1, n_obs), F32),
        v((2, lat_n, 2, 128), F32),
        v((2, levels, 2 * wide, 2 * wide), BF16),
        v((2, levels, 4 * wide, 2 * wide), BF16),
        v((levels, 2 * full, 2 * full), BF16),
        v((levels, 2 * lon_cells, 2 * reach), BF16),
        v((half, full, 4 * wide), BF16),
        v(((half + 1) * reach, 4 * wide), BF16),
        v((max(half * full, (half + 1) * reach), 2 * wide), BF16),
        v((half, levels, full, wide), F32),
        v((levels, 2 * full, half * wide), BF16),
        v((levels, 2 * reach, (half + 1) * wide), BF16),
        pltpu.SMEM(band_width.shape, jnp.int32),
        sem((copies,)), sem((copies,)), sem((7,)),
        pltpu.SemaphoreType.REGULAR((max(lon_n + mem_n - 2, lat_n - 1) - 1,)),
    ]
    hbm = pl.BlockSpec(memory_space=pltpu.HBM)
    kernel = functools.partial(paired, dims=(members, levels, lon_cells, lat_cells, sizes))
    ens = jax.ShapeDtypeStruct((members, levels, lon_cells, lat_cells), F32)
    static = jax.ShapeDtypeStruct((levels, lon_cells, lat_cells), F32)
    parts = pl.pallas_call(
        kernel,
        out_shape=[
            ens, ens,
            jax.ShapeDtypeStruct((2, levels, lon_cells, lat_cells), F32),
            jax.ShapeDtypeStruct((2, 128), F32),
        ],
        in_specs=[hbm] * 6,
        out_specs=[VMEM] * 4,
        scratch_shapes=scratch,
        compiler_params=pltpu.CompilerParams(
            collective_id=0, has_side_effects=True, vmem_limit_bytes=48 * 2**20
        ),
    )(*(
        pltpu.with_memory_space_constraint(x, pltpu.HBM)
        for x in (
            anomalies, spread, obs_index.reshape(1, -1), obs_weight.reshape(1, -1),
            innovation.reshape(1, -1), band_width,
        )
    ))
    return pl.pallas_call(
        combine,
        out_shape=[ens, static],
        in_specs=[VMEM] * 4,
        out_specs=[hbm] * 2,
        scratch_shapes=[
            v(ens.shape, F32), v(static.shape, F32), sem((members + 1,)),
        ],
        compiler_params=pltpu.CompilerParams(vmem_limit_bytes=8 * 2**20),
    )(*parts)


def pick(*args):
    members = args[0].shape[0]
    levels, lon_cells, lat_cells = args[1].shape
    lon_n, lat_n, mem_n = (lax.axis_size(a) for a in AXES)
    pairs = lon_n == 2 and members % 2 == 0 and levels == mem_n and lon_cells % 32 == 0 and lat_n > 2
    return (paired_device if pairs else per_device)(*args)


def solution(mesh):
    return jax.shard_map(
        pick,
        mesh=mesh,
        in_specs=(
            P("mem", None, "lon", "lat"),
            P(None, "lon", "lat"),
            P("lon", "lat", None),
            P("lon", "lat", None),
            P("lon", "lat", None),
            P(),
        ),
        out_specs=(P("mem", None, "lon", "lat"), P(None, "lon", "lat")),
        check_vma=False,
    )
```

```python
import functools
import math

import jax
import jax.numpy as jnp
from jax import lax
from jax.experimental import pallas as pl
from jax.experimental.pallas import tpu as pltpu
from jax.sharding import PartitionSpec as P

BAND = 12
RIM = 2 * BAND

hybrid_ens = 0.75
hybrid_static = 0.25

MESH = pl.DeviceIdType.MESH
VMEM = pl.BlockSpec(memory_space=pltpu.VMEM)
F32 = jnp.float32
BF16 = jnp.bfloat16


def split2(x):
    hi = x.astype(BF16)
    return hi, (x - hi.astype(F32)).astype(BF16)


def dot3(left, right):
    lh, ll = left
    rh, rl = right
    d = functools.partial(jnp.dot, preferred_element_type=F32)
    return d(lh, rh) + (d(ll, rh) + d(lh, rl))


AXES = ("lon", "lat", "mem")


def fused(a_ref, s_ref, i_ref, w_ref, v_ref, bw_ref, ens_ref, static_ref, *scratch, dims):
    members, levels, lon_cells, lat_cells, sizes = dims
    (fc, fr, bc, br, qc, qr, send_al, send_ah, recv_al, recv_ah, pack_l, pack_h, recv_pl, recv_ph,
     fpack, xrh, xrl, two_c, two_r, two_l, one_c, one_r, one_l, bflat, dflat, cov, part,
     slots, slots2, dslots, dsend, smoothed_lat, send, recv, csend, crecv, dsems, drems) = scratch
    lon_n, lat_n, mem_n = sizes
    total = lon_n * lat_n * mem_n
    fields = members + 1
    ext = lon_cells + 2 * RIM
    rows = levels * lon_cells
    chunk = rows // mem_n
    coef_ens = math.sqrt(hybrid_ens / (members * mem_n))
    coef_static = math.sqrt(hybrid_static)
    mine = [lax.axis_index(a) for a in AXES]
    lat_at, me = mine[1], mine[2]
    has_low, has_high = lat_at > 0, lat_at < lat_n - 1

    def shifted(step):
        parts, rest = [], step
        for size in reversed(sizes):
            parts.append(rest % size)
            rest //= size
        return tuple(lax.rem(m + s, size) for m, s, size in zip(mine, reversed(parts), sizes))

    barrier = pltpu.get_barrier_semaphore()
    for step in range(1, total):
        pl.semaphore_signal(barrier, inc=1, device_id=shifted(step), device_id_type=MESH)

    used = [0]

    def remote(src, dst, where):
        k = used[0]
        used[0] += 1
        return pltpu.make_async_remote_copy(
            src_ref=src, dst_ref=dst, send_sem=send.at[k], recv_sem=recv.at[k],
            device_id=where, device_id_type=MESH,
        )

    lon_low = {"lon": lax.rem(mine[0] + lon_n - 1, lon_n)}
    lon_high = {"lon": lax.rem(mine[0] + 1, lon_n)}
    lat_low = {"lat": lax.rem(lat_at + lat_n - 1, lat_n)}
    lat_high = {"lat": lax.rem(lat_at + 1, lat_n)}
    own = pl.ds(0, lon_cells)
    rim = pl.ds(lon_cells, 2 * RIM)
    low_rows = pl.ds(lon_cells, RIM)
    high_rows = pl.ds(lon_cells + RIM, RIM)
    first_rows = pl.ds(0, RIM)
    last_rows = pl.ds(lon_cells - RIM, RIM)
    low_lanes = pl.ds(0, lat_cells)
    high_lanes = pl.ds(lat_cells, lat_cells)

    def lon_start(copies):
        for c in copies:
            c.start()

    def lon_wait(copies):
        for c in copies:
            c.wait()

    class Lat:
        def __init__(self, low_src, high_src, from_low, from_high):
            self.to_low = remote(low_src, from_high, lat_low)
            self.to_high = remote(high_src, from_low, lat_high)

        def start(self):
            pl.when(has_low)(self.to_low.start)
            pl.when(has_high)(self.to_high.start)

        def wait(self):
            pl.when(has_low)(self.to_low.wait_send)
            pl.when(has_high)(self.to_high.wait_send)
            pl.when(has_high)(self.to_low.wait_recv)
            pl.when(has_low)(self.to_high.wait_recv)

    def lane_pack(read, count):
        lane = lax.broadcasted_iota(jnp.int32, (count, lat_cells), 1)
        low = jnp.zeros((count, lat_cells), F32)
        high = low
        for l in range(levels):
            x = read(l)
            here = (lane >= l * RIM) & (lane < (l + 1) * RIM)
            low = jnp.where(here, pltpu.roll(x, (l * RIM) % lat_cells, 1), low)
            high = jnp.where(here, pltpu.roll(x, ((l + 1) * RIM) % lat_cells, 1), high)
        return low, high

    def zero_edges(ref, lead=()):
        @pl.when(jnp.logical_not(has_low))
        def _():
            ref[(*lead, slice(None), low_lanes)] = jnp.zeros((ext, lat_cells), F32)

        @pl.when(jnp.logical_not(has_high))
        def _():
            ref[(*lead, slice(None), high_lanes)] = jnp.zeros((ext, lat_cells), F32)

    def load_member(m, _):
        lows, highs = [], []
        for l in range(levels):
            x = a_ref[m, l].astype(F32)
            fc[l, m, :lon_cells, :] = x
            lows.append(x[:RIM])
            highs.append(x[lon_cells - RIM :])
        send_al[m] = jnp.concatenate(lows, axis=0).astype(BF16)
        send_ah[m] = jnp.concatenate(highs, axis=0).astype(BF16)
        return 0

    lax.fori_loop(0, members, load_member, 0)
    for l in range(levels):
        fc[l, members, :lon_cells, :] = s_ref[l]

    def pack_member(span, count):
        def go(m, _):
            low, high = lane_pack(lambda l: fc[l, m, span, :], count)
            pack_l[m, span, :] = low.astype(BF16)
            pack_h[m, span, :] = high.astype(BF16)
            return 0

        lax.fori_loop(0, members, go, 0)

    def lon_field(ref, lead):
        at = lambda span: ref.at[(slice(None), *lead, span, slice(None))]
        return [
            remote(at(first_rows), at(high_rows), lon_low),
            remote(at(last_rows), at(low_rows), lon_high),
        ]

    def lat_field(slot, dst, lead, span):
        at = lambda lanes: dst.at[(*lead, span, lanes)]
        return Lat(
            fpack.at[slot, 0, span, :], fpack.at[slot, 1, span, :], at(low_lanes), at(high_lanes)
        )

    def fill_pack(slot, read, span, count):
        low, high = lane_pack(lambda l: read(l, span), count)
        fpack[slot, 0, span, :] = low
        fpack[slot, 1, span, :] = high

    read_s = lambda l, span: fc[l, members, span, :]
    read_b = lambda l, span: bc[l, span, :]
    read_q = lambda l, span: qc[l, span, :]

    pl.semaphore_wait(barrier, total - 1)
    lon_a = [remote(send_al, recv_ah, lon_low), remote(send_ah, recv_al, lon_high)]
    lon_start(lon_a)
    lon_s = lon_field(fc, (members,))
    lon_start(lon_s)
    pack_member(own, lon_cells)
    lat_a = Lat(pack_l.at[:, own, :], pack_h.at[:, own, :], recv_pl.at[:, own, :], recv_ph.at[:, own, :])
    lat_a.start()

    idx, val_w = i_ref[...], w_ref[...]
    n_obs = idx.shape[1]
    row, lane = idx // lat_cells, idx % lat_cells
    at_row = (lax.broadcasted_iota(jnp.int32, (rows, n_obs), 0) == row).astype(F32).astype(BF16)
    at_lane = lax.broadcasted_iota(jnp.int32, (lat_cells, n_obs), 0) == lane
    for val, out in ((val_w, dflat), (val_w * v_ref[...], bflat)):
        acc = None
        for _ in range(3):
            piece_val = val.astype(BF16).astype(F32)
            val = val - piece_val
            placed = jnp.where(at_lane, piece_val, 0.0).astype(BF16)
            term = lax.dot_general(
                at_row, placed, (((1,), (1,)), ((), ())), preferred_element_type=F32
            )
            acc = term if acc is None else acc + term
        out[...] = acc
    for l in range(levels):
        bc[l, :lon_cells, :] = bflat[l * lon_cells : (l + 1) * lon_cells, :]
    lon_b = lon_field(bc, ())
    lon_start(lon_b)
    fill_pack(0, read_s, own, lon_cells)
    fill_pack(1, read_b, own, lon_cells)
    lat_sb = [lat_field(0, fr, (members,), own), lat_field(1, br, (), own)]
    for c in lat_sb:
        c.start()
    zero_edges(fr, (members,))
    zero_edges(br)
    zero_edges(qr)

    def iota(shape, dim):
        return lax.broadcasted_iota(jnp.int32, shape, dim)

    def ext_place(index, cells):
        return jnp.where(index < cells, index, jnp.where(index < cells + RIM, index - cells - RIM, index - RIM))

    def make_matrices(l, _):
        taps = (iota((8, 128), 1) - BAND).astype(F32)

        def weights(kind):
            width = bw_ref[kind, l].astype(F32) + jnp.zeros((1, 1), F32)

            def raw(o):
                return jnp.where(jnp.abs(o) <= width, jnp.exp(-0.5 * (o / (0.5 * width)) ** 2), 0.0)

            norm = jnp.sum(raw(taps)[:1], axis=1, keepdims=True)
            return lambda o: raw(o.astype(F32)) / norm

        def put(ref, where, value):
            hi, lo = split2(value)
            ref[(0, *where)] = hi
            ref[(1, *where)] = lo

        w = weights(0)
        mids = 128 * pl.cdiv(lon_cells + 2 * BAND, 128)
        near = w(iota((lon_cells, mids), 0) - (iota((lon_cells, mids), 1) - BAND))
        near = jnp.where(iota((lon_cells, mids), 1) < lon_cells + 2 * BAND, near, 0.0)
        far = w(iota((mids, ext), 0) - BAND - ext_place(iota((mids, ext), 1), lon_cells))
        put(two_l, (l,), dot3(split2(near), split2(far)))
        put(one_l, (l,), w(iota((lon_cells, ext), 0) - ext_place(iota((lon_cells, ext), 1), lon_cells)))

        w = weights(1)
        mids = 128 * pl.cdiv(lat_cells + 2 * BAND, 128)
        mid = iota((mids, lat_cells), 0) - BAND
        place = lat_at * lat_cells + mid
        keep = (place >= 0) & (place < lat_cells * lat_n) & (mid < lat_cells + BAND)
        back = split2(jnp.where(keep, w(mid - iota((mids, lat_cells), 1)), 0.0))
        out = iota((lat_cells, lat_cells), 1)
        here = iota((lat_cells, mids), 0) - (iota((lat_cells, mids), 1) - BAND)
        put(two_c, (l,), dot3(split2(w(here)), back))
        put(one_c, (l,), w(iota((lat_cells, lat_cells), 0) - out))
        columns = pl.ds(pl.multiple_of(l * lat_cells, lat_cells), lat_cells)
        for side in range(2):
            shift = -RIM if side == 0 else lat_cells
            span = pl.ds(side * lat_cells, lat_cells)

            def rim_at(shape):
                p = iota(shape, 0) - l * RIM
                return p + shift, (p >= 0) & (p < RIM)

            pos, ok = rim_at((lat_cells, mids))
            there = jnp.where(ok, w(pos - (iota((lat_cells, mids), 1) - BAND)), 0.0)
            put(two_r, (span, columns), dot3(split2(there), back))
            pos, ok = rim_at((lat_cells, lat_cells))
            put(one_r, (span, columns), jnp.where(ok, w(pos - out), 0.0))
        return 0

    lax.fori_loop(0, levels, make_matrices, 0)

    def lat_part(yc, yr, c_mat, r_mat, l, span, count):
        columns = pl.ds(pl.multiple_of(l * lat_cells, lat_cells), lat_cells)
        xc = split2((fc[l, :, span, :] * yc[l, span, :][None]).reshape(fields * count, lat_cells))
        xr = (
            xrh[:, span, :].reshape(fields * count, 2 * lat_cells),
            xrl[:, span, :].reshape(fields * count, 2 * lat_cells),
        )
        t = dot3(xc, (c_mat[0, l], c_mat[1, l]))
        t = t + dot3(xr, (r_mat[0, :, columns], r_mat[1, :, columns]))
        for h, half in enumerate(split2(t)):
            smoothed_lat[h, l, span, :] = jnp.concatenate(
                [half[f * count : (f + 1) * count] for f in range(fields)], axis=1
            )

    def rim_products(yr, span):
        def go(f, _):
            hi, lo = split2(fr[f, span, :] * yr[span, :])
            xrh[f, span, :], xrl[f, span, :] = hi, lo
            return 0

        lax.fori_loop(0, fields, go, 0)

    def apply_own(yc, yr, mats):
        rim_products(yr, own)

        def go(l, _):
            lat_part(yc, yr, mats[0], mats[1], l, own, lon_cells)
            return 0

        lax.fori_loop(0, levels, go, 0)

    def apply_rim(yc, yr, mats, finish):
        rim_products(yr, rim)

        def go(i, _):
            l = lax.rem(me + 1 + i, levels)
            lat_part(yc, yr, mats[0], mats[1], l, rim, 2 * RIM)
            u = dot3((mats[2][0, l], mats[2][1, l]), (smoothed_lat[0, l], smoothed_lat[1, l]))
            finish(i, l, [u[:, f * lat_cells : (f + 1) * lat_cells] for f in range(fields)])
            return 0

        lax.fori_loop(0, levels, go, 0)

    def unpack_lat(span, count):
        for ref, keep, lanes in ((recv_pl, has_low, low_lanes), (recv_ph, has_high, high_lanes)):
            def go(m, _):
                fr[m, span, lanes] = ref[m, span, :].astype(F32)
                return 0

            def clear(m, _):
                fr[m, span, lanes] = jnp.zeros((count, lat_cells), F32)
                return 0

            @pl.when(keep)
            def _():
                lax.fori_loop(0, members, go, 0)

            @pl.when(jnp.logical_not(keep))
            def _():
                lax.fori_loop(0, members, clear, 0)

    lat_a.wait()
    unpack_lat(own, lon_cells)
    for c in lat_sb:
        c.wait()
    apply_own(bc, br, (two_c, two_r, two_l))

    lon_wait(lon_a)

    def unpack_member(m, _):
        low, high = recv_al[m].astype(F32), recv_ah[m].astype(F32)
        for l in range(levels):
            fc[l, m, low_rows, :] = low[l * RIM : (l + 1) * RIM]
            fc[l, m, high_rows, :] = high[l * RIM : (l + 1) * RIM]
        return 0

    lax.fori_loop(0, members, unpack_member, 0)
    pack_member(rim, 2 * RIM)
    lat_a2 = Lat(pack_l.at[:, rim, :], pack_h.at[:, rim, :], recv_pl.at[:, rim, :], recv_ph.at[:, rim, :])
    lat_a2.start()
    lon_wait(lon_s)
    lon_wait(lon_b)
    fill_pack(0, read_s, rim, 2 * RIM)
    fill_pack(1, read_b, rim, 2 * RIM)
    lat_sb2 = [lat_field(0, fr, (members,), rim), lat_field(1, br, (), rim)]
    for c in lat_sb2:
        c.start()
    lat_a2.wait()
    unpack_lat(rim, 2 * RIM)
    for c in lat_sb2:
        c.wait()

    def piece(owner):
        return pl.ds(pl.multiple_of(owner * chunk, chunk), chunk)

    def mem_copy(src, dst, j, group):
        return pltpu.make_async_remote_copy(
            src_ref=src, dst_ref=dst, send_sem=csend.at[group, j], recv_sem=crecv.at[group, j],
            device_id={"mem": lax.rem(me + j, mem_n)}, device_id_type=MESH,
        )

    def sum_copy(dst, j, group):
        return mem_copy(part.at[piece(lax.rem(me + j, mem_n))], dst.at[j], j, group)

    by_level = levels == mem_n

    def finish_cov(dst, group):
        def finish(i, l, smoothed):
            acc = fc[l, 0, :lon_cells, :] * smoothed[0]
            for f in range(1, members):
                acc = acc + fc[l, f, :lon_cells, :] * smoothed[f]
            acc = acc * (coef_ens * coef_ens)
            acc = acc + fc[l, members, :lon_cells, :] * smoothed[members] * (coef_static**2 / mem_n)
            part[pl.ds(pl.multiple_of(l * lon_cells, lon_cells), lon_cells), :] = acc
            if by_level:
                @pl.when(i < mem_n - 1)
                def _():
                    sum_copy(dst, i + 1, group).start()

        return finish

    def scatter_sum(dst, group):
        copies = [sum_copy(dst, j, group) for j in range(1, mem_n)]
        if not by_level:
            for copy in copies:
                copy.start()
        acc = part[piece(me), :]
        for j, copy in enumerate(copies):
            copy.wait_recv()
            acc = acc + dst[j + 1]
        for copy in copies:
            copy.wait_send()
        return acc

    def dots_start(left, right, group):
        at = iota((2, lat_cells), 0)
        a = jnp.sum(left, axis=0, keepdims=True)
        b = jnp.sum(right, axis=0, keepdims=True)
        dsend[group] = jnp.where(at == 0, a, b)
        copies = []
        for step in range(1, total):
            copy = pltpu.make_async_remote_copy(
                src_ref=dsend.at[group], dst_ref=dslots.at[group, step],
                send_sem=dsems.at[group, step], recv_sem=drems.at[group, step],
                device_id=shifted(step), device_id_type=MESH,
            )
            copy.start()
            copies.append(copy)
        return copies

    def dots_end(copies, group):
        for copy in copies:
            copy.wait()
        block = dsend[group] + jnp.sum(dslots[group, 1:], axis=0)
        sums = jnp.sum(block, axis=1, keepdims=True)
        return sums[0:1], sums[1:2]

    two, one = (two_c, two_r, two_l), (one_c, one_r, one_l)
    apply_rim(bc, br, two, finish_cov(slots, 0))
    acc = scatter_sum(slots, 0)
    cov[piece(me), :] = acc
    back = [mem_copy(cov.at[piece(me)], cov.at[piece(me)], j, 1) for j in range(1, mem_n)]
    for copy in back:
        copy.start()
    rhs_mine, diag_mine, cov_mine = bflat[piece(me), :], dflat[piece(me), :], acc
    image_mine = rhs_mine + diag_mine * cov_mine
    dots0 = dots_start(rhs_mine * cov_mine, cov_mine * image_mine, 0)
    for copy in back:
        copy.wait()
    for l in range(levels):
        span = slice(l * lon_cells, (l + 1) * lon_cells)
        qc[l, :lon_cells, :] = bflat[span, :] + dflat[span, :] * cov[span, :]
    lon_q = lon_field(qc, ())
    lon_start(lon_q)
    fill_pack(2, read_q, own, lon_cells)
    lat_q = lat_field(2, qr, (), own)
    lat_q.start()
    lon_wait(lon_q)
    fill_pack(2, read_q, rim, 2 * RIM)
    lat_q2 = lat_field(2, qr, (), rim)
    lat_q2.start()
    lat_q.wait()

    apply_own(qc, qr, two)
    lat_q2.wait()
    apply_rim(qc, qr, two, finish_cov(slots2, 2))
    cov_q = scatter_sum(slots2, 2)
    norm0, curve0 = dots_end(dots0, 0)
    alpha0 = norm0 / curve0
    resid = rhs_mine - alpha0 * image_mine
    cov_r = cov_mine - alpha0 * cov_q
    norm1, curve1 = dots_end(dots_start(resid * cov_r, cov_r * (resid + diag_mine * cov_r), 1), 1)
    beta = norm1 / norm0
    alpha1 = norm1 / (curve1 - beta * norm1 / alpha0)

    def combine(b, q):
        return alpha0 * b + alpha1 * ((b - alpha0 * q) + beta * b)

    for l in range(levels):
        bc[l] = combine(bc[l], qc[l])
    br[...] = combine(br[...], qr[...])

    def finish_control(i, l, smoothed):
        for f in range(members):
            ens_ref[f, l] = coef_ens * smoothed[f]
        static_ref[l] = coef_static * smoothed[members]

    apply_own(bc, br, one)
    apply_rim(bc, br, one, finish_control)


def per_device(anomalies, spread, obs_index, innovation, obs_weight, band_width):
    members = anomalies.shape[0]
    levels, lon_cells, lat_cells = spread.shape
    sizes = tuple(lax.axis_size(a) for a in AXES)
    mem_n, total = sizes[2], math.prod(sizes)
    fields = members + 1
    ext = lon_cells + 2 * RIM
    rows = levels * lon_cells
    chunk = rows // mem_n
    v = pltpu.VMEM
    sem = pltpu.SemaphoreType.DMA
    edge = v((members, levels * RIM, lat_cells), BF16)
    packed = v((members, ext, lat_cells), BF16)
    field = v((levels, ext, lat_cells), F32)
    field_rim = v((ext, 2 * lat_cells), F32)
    mats = [
        v((2, levels, lat_cells, lat_cells), BF16),
        v((2, 2 * lat_cells, levels * lat_cells), BF16),
        v((2, levels, lon_cells, ext), BF16),
    ]
    flat = v((rows, lat_cells), F32)
    scratch = [
        v((levels, fields, ext, lat_cells), F32),
        v((fields, ext, 2 * lat_cells), F32),
        field, field_rim, field, field_rim,
        edge, edge, edge, edge,
        packed, packed, packed, packed,
        v((3, 2, ext, lat_cells), F32),
        v((fields, ext, 2 * lat_cells), BF16),
        v((fields, ext, 2 * lat_cells), BF16),
        *mats, *mats,
        flat, flat, flat, flat,
        v((mem_n, chunk, lat_cells), F32),
        v((mem_n, chunk, lat_cells), F32),
        v((2, total, 2, lat_cells), F32),
        v((2, 2, lat_cells), F32),
        v((2, levels, ext, fields * lat_cells), BF16),
        sem((32,)), sem((32,)), sem((3, mem_n)), sem((3, mem_n)), sem((2, total)), sem((2, total)),
    ]
    kernel = functools.partial(fused, dims=(members, levels, lon_cells, lat_cells, sizes))
    return pl.pallas_call(
        kernel,
        out_shape=[
            jax.ShapeDtypeStruct((members, levels, lon_cells, lat_cells), F32),
            jax.ShapeDtypeStruct((levels, lon_cells, lat_cells), F32),
        ],
        in_specs=[VMEM] * 5 + [pl.BlockSpec(memory_space=pltpu.SMEM)],
        out_specs=[VMEM] * 2,
        scratch_shapes=scratch,
        compiler_params=pltpu.CompilerParams(
            collective_id=0, has_side_effects=True, vmem_limit_bytes=60 * 2**20
        ),
    )(
        anomalies, spread, obs_index.reshape(1, -1), obs_weight.reshape(1, -1),
        innovation.reshape(1, -1), band_width,
    )


def paired(a_hbm, s_hbm, i_hbm, w_hbm, v_hbm, bw_hbm, ub_ref, uq_ref, st_ref, coef_ref, *scratch, dims):
    members, levels, lon_cells, lat_cells, sizes = dims
    (acen, arim, plo, phi, sfull, sedge, srim, srims, spack, spacks, oidx, ow, ov, at_row, grid, grim, gpack, cov, orecv,
     drecv, mat_c, mat_r, lon_t, lon_l, xr, xq, xo, tc, ts, to, bw_ref, send, recv, load, relay) = scratch
    lon_n, lat_n, mem_n = sizes
    half = members // lon_n
    full = lon_n * lon_cells
    group = lon_n * mem_n
    rows = levels * lon_cells
    wide = lat_cells
    edge = 16 * pl.cdiv(BAND, 16)
    reach = lon_cells + 2 * edge
    n_obs = oidx.shape[2]
    coef_ens = math.sqrt(hybrid_ens / (members * mem_n))
    coef_static = math.sqrt(hybrid_static)
    at_lon, lat_at, me = (lax.axis_index(a) for a in AXES)
    other = 1 - at_lon
    has_low, has_high = lat_at > 0, lat_at < lat_n - 1
    my_id = at_lon * mem_n + me

    def group_peer(step):
        peer = lax.rem(my_id + step, group)
        return {"lon": peer // mem_n, "mem": lax.rem(peer, mem_n)}

    def lat_peer(step):
        return {"lat": lax.rem(lat_at + step, lat_n)}

    own_rows, far_rows = pl.ds(0, lon_cells), pl.ds(lon_cells, lon_cells)
    first, second = pl.ds(0, half), pl.ds(half, half)
    loads = [
        pltpu.make_async_copy(src, dst, load.at[k])
        for k, (src, dst) in enumerate((
            (i_hbm, oidx.at[0]),
            (w_hbm, ow.at[0]),
            (v_hbm, ov.at[0]),
            (s_hbm, sfull.at[:, own_rows]),
            (a_hbm.at[pl.ds(other * half, half)], acen.at[second, :, own_rows, :]),
            (a_hbm.at[pl.ds(at_lon * half, half)], acen.at[first, :, own_rows, :]),
            (bw_hbm, bw_ref),
        ))
    ]
    for copy in loads:
        copy.start()

    near = [
        (True, {"lon": other}),
        (has_low, {"lat": lat_at - 1}),
        (has_high, {"lat": lat_at + 1}),
        (me > 0, {"mem": me - 1}),
        (me < mem_n - 1, {"mem": me + 1}),
    ]
    n_near = sum(jnp.asarray(there, jnp.int32) for there, _ in near)

    def greet(sem):
        for there, where in near:
            def go(where=where):
                pl.semaphore_signal(sem, inc=1, device_id=where, device_id_type=MESH)

            go() if there is True else pl.when(there)(go)

    def relay_round(r):
        pl.semaphore_wait(relay.at[r], n_near)
        if r + 1 < rounds:
            greet(relay.at[r + 1])

    rounds = max(lon_n + mem_n - 2, lat_n - 1) - 1
    barrier = pltpu.get_barrier_semaphore()
    greet(barrier)

    used = [0]

    def remote(src, dst, where):
        k = used[0]
        used[0] += 1
        return pltpu.make_async_remote_copy(
            src_ref=src, dst_ref=dst, send_sem=send.at[k], recv_sem=recv.at[k],
            device_id=where, device_id_type=MESH,
        )

    partner = {"lon": other}
    lat_low = {"lat": lax.rem(lat_at + lat_n - 1, lat_n)}
    lat_high = {"lat": lax.rem(lat_at + 1, lat_n)}
    low_lanes = pl.ds(0, wide)
    high_lanes = pl.ds(wide, wide)

    class Lat:
        def __init__(self, low_src, high_src, from_low, from_high):
            self.to_low = remote(low_src, from_high, lat_low)
            self.to_high = remote(high_src, from_low, lat_high)

        def start(self):
            pl.when(has_low)(self.to_low.start)
            pl.when(has_high)(self.to_high.start)

        def wait(self):
            pl.when(has_low)(self.to_low.wait_send)
            pl.when(has_high)(self.to_high.wait_send)
            pl.when(has_high)(self.to_low.wait_recv)
            pl.when(has_low)(self.to_high.wait_recv)

    def iota(shape, dim):
        return lax.broadcasted_iota(jnp.int32, shape, dim)

    def lane_pack(read, count, at_levels=None):
        lane = iota((count, wide), 1)
        low = jnp.zeros((count, wide), F32)
        high = low
        for l in range(levels) if at_levels is None else at_levels:
            x = read(l)
            here = (lane >= l * RIM) & (lane < (l + 1) * RIM)
            low = jnp.where(here, pltpu.roll(x, lax.rem(l * RIM, wide), 1), low)
            high = jnp.where(here, pltpu.roll(x, lax.rem((l + 1) * RIM, wide), 1), high)
        return low, high

    def pack_member(p, span, count):
        low, high = lane_pack(lambda l: acen[p, l, span, :].astype(F32), count)
        plo[p, span, :] = low.astype(BF16)
        phi[p, span, :] = high.astype(BF16)

    def pack_static(span, count):
        low, high = lane_pack(lambda l: sfull[me, span, :], count, [me])
        spack[0, span, :] = low
        spack[1, span, :] = high

    def pack_statics(ref, span, to_span, count):
        low, high = lane_pack(lambda l: ref[l, span, :], count)
        spacks[0, to_span, :] = low
        spacks[1, to_span, :] = high

    def lat_members(which, span):
        return Lat(
            plo.at[which, span, :], phi.at[which, span, :],
            arim.at[which, span, low_lanes], arim.at[which, span, high_lanes],
        )

    def lat_static(span, pack=spack, rim=srim):
        return Lat(
            pack.at[0, span, :], pack.at[1, span, :],
            rim.at[span, low_lanes], rim.at[span, high_lanes],
        )

    def lat_grid(g):
        return Lat(gpack.at[g, 0], gpack.at[g, 1], grim.at[g, :, low_lanes], grim.at[g, :, high_lanes])

    x_obs = [remote(ref.at[0], ref.at[1], partner) for ref in (oidx, ow, ov)]
    x_static = remote(sfull.at[me, own_rows], sfull.at[me, far_rows], partner)
    x_first = [
        remote(acen.at[half + p, :, own_rows, :], acen.at[p, :, far_rows, :], partner)
        for p in range(half)
    ]
    edges = pl.ds(lon_cells, 2 * edge)
    x_edge = []
    for src, k in ((0, 0), (lon_cells - edge, edge)):
        src, dst = pl.ds(src, edge), pl.ds(lon_cells + k, edge)
        x_edge.append(remote(acen.at[first, :, src, :], acen.at[second, :, dst, :], partner))
        x_edge.append(remote(sfull.at[:, src], sedge.at[:, pl.ds(k, edge)], partner))
    for copy in loads:
        copy.wait()
    pl.semaphore_wait(barrier, n_near)
    for copy in [*x_obs, *x_first, x_static]:
        copy.start()
    greet(relay.at[0])

    def pack_first(p, _):
        pack_member(p, own_rows, lon_cells)
        return 0

    lax.fori_loop(0, half, pack_first, 0)
    lat_a = lat_members(first, own_rows)
    lat_a.start()
    pack_static(own_rows, lon_cells)
    lat_s = lat_static(own_rows)
    lat_s.start()
    lax.fori_loop(half, members, pack_first, 0)
    lat_a3 = lat_members(second, own_rows)
    lat_a3.start()
    pack_statics(sfull, own_rows, own_rows, lon_cells)
    lat_s3 = lat_static(own_rows, spacks, srims)
    lat_s3.start()

    @pl.when(jnp.logical_not(has_low))
    def _():
        arim[:, :, low_lanes] = jnp.zeros((members, full, wide), BF16)
        srim[:, low_lanes] = jnp.zeros((full, wide), F32)
        srims[:, low_lanes] = jnp.zeros((reach, wide), F32)
        grim[:, :, low_lanes] = jnp.zeros((2, full, wide), F32)

    @pl.when(jnp.logical_not(has_high))
    def _():
        arim[:, :, high_lanes] = jnp.zeros((members, full, wide), BF16)
        srim[:, high_lanes] = jnp.zeros((full, wide), F32)
        srims[:, high_lanes] = jnp.zeros((reach, wide), F32)
        grim[:, :, high_lanes] = jnp.zeros((2, full, wide), F32)

    relay_round(0)
    slot_rows = (own_rows, far_rows)
    slot_tile = (at_lon, other)

    def mark_rows(s):
        row = oidx[s] // wide
        at_row[s] = (iota((rows, n_obs), 0) == row).astype(F32).astype(BF16)

    def scatter(s, value, g):
        at_lane = iota((wide, n_obs), 0) == oidx[s] % wide
        hi = value.astype(BF16).astype(F32)
        lo = value - hi
        placed = jnp.concatenate(
            [jnp.where(at_lane, hi, 0.0).astype(BF16), jnp.where(at_lane, lo, 0.0).astype(BF16)], axis=0
        )
        out = lax.dot_general(
            at_row[s], placed, (((1,), (1,)), ((), ())), preferred_element_type=F32
        )
        out = out[:, :wide] + out[:, wide:]
        for l in range(levels):
            grid[g, l, slot_rows[s], :] = out[l * lon_cells : (l + 1) * lon_cells]

    def gather(s, g):
        hi, lo = split2(cov[s].T)
        left = jnp.concatenate([hi, lo], axis=0)
        step = 512 if n_obs % 512 == 0 else n_obs
        for c in range(0, n_obs, step):
            part = jnp.dot(left, at_row[s, :, c : c + step], preferred_element_type=F32)
            lane = oidx[s, :, c : c + step] % wide
            here = iota((wide, step), 0) == lane
            value = jnp.where(here, part[:wide] + part[wide:], 0.0)
            orecv[g, my_id, slot_tile[s], :, c : c + step] = jnp.sum(value, axis=0, keepdims=True)

    def send_grid(g):
        low, high = lane_pack(lambda l: grid[g, l], full)
        gpack[g, 0] = low
        gpack[g, 1] = high
        copy = lat_grid(g)
        copy.start()
        return copy

    mark_rows(0)
    scatter(0, ow[0] * ov[0], 0)

    def make_matrices(l, _):
        taps = (iota((8, 128), 1) - BAND).astype(F32)

        def weights(kind):
            width = bw_ref[kind, l].astype(F32) + jnp.zeros((1, 1), F32)

            def raw(o):
                return jnp.where(jnp.abs(o) <= width, jnp.exp(-0.5 * (o / (0.5 * width)) ** 2), 0.0)

            norm = jnp.sum(raw(taps)[:1], axis=1, keepdims=True)
            return lambda o: raw(o.astype(F32)) / norm

        def put_lon(ref, count, value):
            hi, lo = split2(value)
            cols = value.shape[1]
            ref[l, :count, :] = jnp.concatenate([hi, hi], axis=1)
            ref[l, count:, :] = jnp.concatenate([lo, jnp.zeros((count, cols), BF16)], axis=1)

        w = weights(0)

        def ring(count, cols):
            c = iota((count, cols), 1)
            if cols < full:
                c = jnp.where(c < lon_cells + edge, c, c + full - cols)
            d = c - iota((count, cols), 0)
            d = jnp.where(d > full // 2, d - full, d)
            return w(jnp.where(d < -(full // 2), d + full, d))

        circle = split2(ring(full, full))
        put_lon(lon_t, full, dot3(circle, circle))
        put_lon(lon_l, lon_cells, ring(lon_cells, reach))

        def put_lat(ref, kind, hi_at, lo_at, value):
            hi, lo = split2(value)
            ref[kind, l, pl.ds(hi_at, wide), :wide] = hi
            ref[kind, l, pl.ds(hi_at, wide), wide:] = lo
            ref[kind, l, pl.ds(lo_at, wide), :wide] = hi
            ref[kind, l, pl.ds(lo_at, wide), wide:] = jnp.zeros((wide, wide), BF16)

        w = weights(1)
        mids = 128 * pl.cdiv(wide + 2 * BAND, 128)
        mid = iota((mids, wide), 0) - BAND
        place = lat_at * wide + mid
        keep = (place >= 0) & (place < wide * lat_n) & (mid < wide + BAND)
        back = split2(jnp.where(keep, w(mid - iota((mids, wide), 1)), 0.0))
        out = iota((wide, wide), 1)
        here = iota((wide, mids), 0) - (iota((wide, mids), 1) - BAND)
        put_lat(mat_c, 0, 0, wide, dot3(split2(w(here)), back))
        put_lat(mat_c, 1, 0, wide, w(iota((wide, wide), 0) - out))
        for side in range(2):
            shift = -RIM if side == 0 else wide

            def rim_at(shape):
                p = iota(shape, 0) - l * RIM
                return p + shift, (p >= 0) & (p < RIM)

            pos, ok = rim_at((wide, mids))
            there = jnp.where(ok, w(pos - (iota((wide, mids), 1) - BAND)), 0.0)
            put_lat(mat_r, 0, side * wide, (2 + side) * wide, dot3(split2(there), back))
            pos, ok = rim_at((wide, wide))
            put_lat(mat_r, 1, side * wide, (2 + side) * wide, jnp.where(ok, w(pos - out), 0.0))
        return 0

    lax.fori_loop(0, levels, make_matrices, 0)
    for r in range(1, rounds):
        relay_round(r)

    for copy in x_obs:
        copy.wait()
    mark_rows(1)
    scatter(1, ow[1] * ov[1], 0)
    lat_b = send_grid(0)

    def dot(a, b):
        return jnp.dot(a, b, preferred_element_type=F32)

    def fold(t):
        return t[:, :wide] + t[:, wide:]

    def pair(x):
        return jnp.concatenate(split2(x), axis=1)

    def stack(x):
        return jnp.concatenate(split2(x), axis=0)

    def reached(x):
        return jnp.concatenate([x[: lon_cells + edge], x[full - edge :]], axis=0)

    def rim_member(g, p):
        xr[p] = pair(arim[p].astype(F32) * grim[g])

    def center_member(g, p):
        for l in range(levels):
            tc[p, l] = fold(dot(pair(acen[p, l].astype(F32) * grid[g, l]), mat_c[0, l]))

    def lat_member(p, at):
        for l in range(levels):
            ts[l, :, at] = stack(tc[p, l] + fold(dot(xr[p], mat_r[0, l])))

    def cov_level(l):
        u = dot(lon_t[l], ts[l])
        u = u[:full] + u[full:]
        acc = acen[0, l].astype(F32) * u[:, :wide]
        for p in range(1, half):
            acc = acc + acen[p, l].astype(F32) * u[:, p * wide : (p + 1) * wide]
        acc = acc * (coef_ens * coef_ens)
        for j in range(lon_n):
            cov[j, l * lon_cells : (l + 1) * lon_cells, :] = acc[j * lon_cells : (j + 1) * lon_cells]

    def cov_static(g):
        t = dot(pair(sfull[me] * grid[g, me]), mat_c[0, me])
        t = t + dot(pair(srim[...] * grim[g]), mat_r[0, me])
        u = dot(lon_t[me], stack(fold(t)))
        acc = sfull[me] * (u[:full] + u[full:]) * (coef_static**2 / lon_n)
        at = pl.ds(pl.multiple_of(me * lon_cells, lon_cells), lon_cells)
        for j in range(lon_n):
            cov[j, at, :] = cov[j, at, :] + acc[j * lon_cells : (j + 1) * lon_cells]

    lat_a2 = []
    for p in range(half):
        x_first[p].wait()
        pack_member(p, far_rows, lon_cells)
        copy = lat_members(p, far_rows)
        copy.start()
        lat_a2.append(copy)
        center_member(0, p)
    x_static.wait()
    for copy in x_edge:
        copy.start()
    pack_static(far_rows, lon_cells)
    lat_s2 = lat_static(far_rows)
    lat_s2.start()

    def share(g):
        for s in range(lon_n):
            gather(s, g)
        copies = []
        for step in range(1, group):
            copy = remote(orecv.at[g, my_id], orecv.at[g, my_id], group_peer(step))
            copy.start()
            copies.append(copy)
        return copies

    def shared(copies, g):
        for copy in copies:
            copy.wait()
        sums = []
        for s in range(lon_n):
            acc = orecv[g, 0, slot_tile[s]]
            for k in range(1, group):
                acc = acc + orecv[g, k, slot_tile[s]]
            sums.append(acc)
        return sums

    def out_rows(l, cells, reads):
        n = len(reads)
        for p, read in enumerate(reads):
            xo[p * reach : (p + 1) * reach] = pair(read() * cells)
        t = fold(dot(xo[: n * reach], mat_c[1, l]) + dot(xq[: n * reach], mat_r[1, l]))
        for p in range(n):
            to[l, :, p * wide : (p + 1) * wide] = stack(t[p * reach : (p + 1) * reach])
        u = dot(lon_l[l], to[l, :, : n * wide])
        u = u[:lon_cells] + u[lon_cells:]
        return [u[:, p * wide : (p + 1) * wide] for p in range(n)]

    def out_first(g):
        out_ref = (ub_ref, uq_ref)[g]
        for p in range(half):
            xq[p * reach : (p + 1) * reach] = reached(xr[p])

        def go(l, _):
            reads = [lambda p=p: reached(acen[p, l]).astype(F32) for p in range(half)]
            for p, u in enumerate(out_rows(l, reached(grid[g, l]), reads)):
                out_ref[at_lon * half + p, l] = u * coef_ens
            return 0

        lax.fori_loop(0, levels, go, 0)

    def out_second(g):
        out_ref = (ub_ref, uq_ref)[g]
        near_rim = reached(grim[g])
        for p in range(half):
            xq[p * reach : (p + 1) * reach] = pair(arim[half + p, :reach].astype(F32) * near_rim)
        xq[half * reach :] = pair(srims[...] * near_rim)

        def go(l, _):
            reads = [lambda p=p: acen[half + p, l, :reach].astype(F32) for p in range(half)]
            reads.append(lambda: jnp.concatenate([sfull[l, :lon_cells], sedge[l]], axis=0))
            us = out_rows(l, reached(grid[g, l]), reads)
            for p in range(half):
                out_ref[other * half + p, l] = us[p] * coef_ens
            st_ref[g, l] = us[half] * coef_static
            return 0

        lax.fori_loop(0, levels, go, 0)

    def dots_start(g, left, right):
        def total(pairs):
            acc = None
            for x in pairs:
                for c in range(0, n_obs, 128):
                    part = x[:, c : c + 128]
                    acc = part if acc is None else acc + part
            return acc

        at = iota((2, 128), 0)
        drecv[g, lat_at] = jnp.where(at == 0, total(left), total(right))
        copies = []
        for step in range(1, lat_n):
            copy = remote(drecv.at[g, lat_at], drecv.at[g, lat_at], lat_peer(step))
            copy.start()
            copies.append(copy)
        return copies

    def dots_end(copies, g):
        for copy in copies:
            copy.wait()
        block = drecv[g, 0]
        for k in range(1, lat_n):
            block = block + drecv[g, k]
        sums = jnp.sum(block, axis=1, keepdims=True)
        return sums[0:1], sums[1:2]

    def rim_and_cov(g):
        for p in range(half):
            if g == 0:
                lat_a2[p].wait()
            rim_member(g, p)
            if g == 0:
                lat_member(p, slice(p * wide, (p + 1) * wide))
        if g > 0:
            rims = xr[:half].reshape(half * full, 4 * wide)
            for l in range(levels):
                t = fold(dot(rims, mat_r[0, l]))
                for p in range(half):
                    part = tc[p, l] + t[p * full : (p + 1) * full]
                    ts[l, :, p * wide : (p + 1) * wide] = stack(part)
        for l in range(levels):
            cov_level(l)
        if g == 0:
            lat_s.wait()
            lat_s2.wait()
        cov_static(g)
        return share(g)

    lat_b.wait()
    lat_a.wait()
    sharing = rim_and_cov(0)

    for copy in x_edge:
        copy.wait()

    def pack_second(p, _):
        pack_member(p, edges, 2 * edge)
        return 0

    lax.fori_loop(half, members, pack_second, 0)
    lat_a4 = lat_members(second, edges)
    lat_a4.start()
    pack_statics(sedge, slice(None), edges, 2 * edge)
    lat_s4 = lat_static(edges, spacks, srims)
    lat_s4.start()
    out_first(0)

    cz = shared(sharing, 0)
    z = [ow[s] * ov[s] for s in range(lon_n)]
    q = [z[s] + ow[s] * cz[s] for s in range(lon_n)]
    for s in range(lon_n):
        scatter(s, q[s], 1)
    lat_q = send_grid(1)
    dots0 = dots_start(0, [z[s] * cz[s] for s in range(lon_n)], [cz[s] * q[s] for s in range(lon_n)])

    def center_all(l, _):
        for p in range(half):
            xo[p * full : (p + 1) * full] = pair(acen[p, l].astype(F32) * grid[1, l])
        t = fold(dot(xo[: half * full], mat_c[0, l]))
        for p in range(half):
            tc[p, l] = t[p * full : (p + 1) * full]
        return 0

    lax.fori_loop(0, levels, center_all, 0)
    lat_q.wait()
    sharing = rim_and_cov(1)
    out_first(1)
    for copy in (lat_a3, lat_a4, lat_s3, lat_s4):
        copy.wait()
    out_second(1)

    cq = shared(sharing, 1)
    norm0, curve0 = dots_end(dots0, 0)
    alpha0 = norm0 / curve0
    resid = [z[s] - alpha0 * q[s] for s in range(lon_n)]
    cr = [cz[s] - alpha0 * cq[s] for s in range(lon_n)]
    dots1 = dots_start(
        1,
        [resid[s] * cr[s] for s in range(lon_n)],
        [cr[s] * (resid[s] + ow[s] * cr[s]) for s in range(lon_n)],
    )
    out_second(0)
    norm1, curve1 = dots_end(dots1, 1)
    beta = norm1 / norm0
    alpha1 = norm1 / (curve1 - beta * norm1 / alpha0)
    on_b = alpha0 + alpha1 * (1.0 + beta)
    on_q = -alpha0 * alpha1
    coef_ref[...] = jnp.where(iota((2, 128), 0) == 0, on_b, on_q)


def combine(ub_ref, uq_ref, st_ref, coef_ref, ens_ref, static_ref, ens, static, sems):
    on_b, on_q = coef_ref[0:1, :], coef_ref[1:2, :]
    members = ens.shape[0]
    copies = []
    for m in range(members):
        ens[m] = on_b * ub_ref[m] + on_q * uq_ref[m]
        copies.append(pltpu.make_async_copy(ens.at[m], ens_ref.at[m], sems.at[m]))
        copies[-1].start()
    static[...] = on_b * st_ref[0] + on_q * st_ref[1]
    copies.append(pltpu.make_async_copy(static, static_ref, sems.at[members]))
    copies[-1].start()
    for copy in copies:
        copy.wait()


def paired_device(anomalies, spread, obs_index, innovation, obs_weight, band_width):
    members = anomalies.shape[0]
    levels, lon_cells, lat_cells = spread.shape
    sizes = tuple(lax.axis_size(a) for a in AXES)
    lon_n, lat_n, mem_n = sizes
    half = members // lon_n
    full = lon_n * lon_cells
    group = lon_n * mem_n
    n_obs = obs_index.shape[-1]
    v = pltpu.VMEM
    sem = pltpu.SemaphoreType.DMA
    wide = lat_cells
    reach = lon_cells + 2 * 16 * pl.cdiv(BAND, 16)
    copies = 8 + half + 2 * (9 + half) + 2 * (group - 1 + lat_n - 1)
    scratch = [
        v((members, levels, full, wide), BF16),
        v((members, full, 2 * wide), BF16),
        v((members, full, wide), BF16),
        v((members, full, wide), BF16),
        v((levels, full, wide), F32),
        v((levels, reach - lon_cells, wide), F32),
        v((full, 2 * wide), F32),
        v((reach, 2 * wide), F32),
        v((2, full, wide), F32),
        v((2, reach, wide), F32),
        v((lon_n, 1, n_obs), jnp.int32),
        v((lon_n, 1, n_obs), F32),
        v((lon_n, 1, n_obs), F32),
        v((lon_n, levels * lon_cells, n_obs), BF16),
        v((2, levels, full, wide), F32),
        v((2, full, 2 * wide), F32),
        v((2, 2, full, wide), F32),
        v((lon_n, levels * lon_cells, wide), F32),
        v((2, group, lon_n, 1, n_obs), F32),
        v((2, lat_n, 2, 128), F32),
        v((2, levels, 2 * wide, 2 * wide), BF16),
        v((2, levels, 4 * wide, 2 * wide), BF16),
        v((levels, 2 * full, 2 * full), BF16),
        v((levels, 2 * lon_cells, 2 * reach), BF16),
        v((half, full, 4 * wide), BF16),
        v(((half + 1) * reach, 4 * wide), BF16),
        v((max(half * full, (half + 1) * reach), 2 * wide), BF16),
        v((half, levels, full, wide), F32),
        v((levels, 2 * full, half * wide), BF16),
        v((levels, 2 * reach, (half + 1) * wide), BF16),
        pltpu.SMEM(band_width.shape, jnp.int32),
        sem((copies,)), sem((copies,)), sem((7,)),
        pltpu.SemaphoreType.REGULAR((max(lon_n + mem_n - 2, lat_n - 1) - 1,)),
    ]
    hbm = pl.BlockSpec(memory_space=pltpu.HBM)
    kernel = functools.partial(paired, dims=(members, levels, lon_cells, lat_cells, sizes))
    ens = jax.ShapeDtypeStruct((members, levels, lon_cells, lat_cells), F32)
    static = jax.ShapeDtypeStruct((levels, lon_cells, lat_cells), F32)
    parts = pl.pallas_call(
        kernel,
        out_shape=[
            ens, ens,
            jax.ShapeDtypeStruct((2, levels, lon_cells, lat_cells), F32),
            jax.ShapeDtypeStruct((2, 128), F32),
        ],
        in_specs=[hbm] * 6,
        out_specs=[VMEM] * 4,
        scratch_shapes=scratch,
        compiler_params=pltpu.CompilerParams(
            collective_id=0, has_side_effects=True, vmem_limit_bytes=48 * 2**20
        ),
    )(*(
        pltpu.with_memory_space_constraint(x, pltpu.HBM)
        for x in (
            anomalies, spread, obs_index.reshape(1, -1), obs_weight.reshape(1, -1),
            innovation.reshape(1, -1), band_width,
        )
    ))
    return pl.pallas_call(
        combine,
        out_shape=[ens, static],
        in_specs=[VMEM] * 4,
        out_specs=[hbm] * 2,
        scratch_shapes=[
            v(ens.shape, F32), v(static.shape, F32), sem((members + 1,)),
        ],
        compiler_params=pltpu.CompilerParams(vmem_limit_bytes=8 * 2**20),
    )(*parts)


def pick(*args):
    members = args[0].shape[0]
    levels, lon_cells, lat_cells = args[1].shape
    lon_n, lat_n, mem_n = (lax.axis_size(a) for a in AXES)
    pairs = lon_n == 2 and members % 2 == 0 and levels == mem_n and lon_cells % 32 == 0 and lat_n > 2
    return (paired_device if pairs else per_device)(*args)


def solution(mesh):
    return jax.shard_map(
        pick,
        mesh=mesh,
        in_specs=(
            P("mem", None, "lon", "lat"),
            P(None, "lon", "lat"),
            P("lon", "lat", None),
            P("lon", "lat", None),
            P("lon", "lat", None),
            P(),
        ),
        out_specs=(P("mem", None, "lon", "lat"), P(None, "lon", "lat")),
        check_vma=False,
    )
```

```python
import functools
import math

import jax
import jax.numpy as jnp
from jax import lax
from jax.experimental import pallas as pl
from jax.experimental.pallas import tpu as pltpu
from jax.sharding import PartitionSpec as P

BAND = 12
RIM = 2 * BAND

hybrid_ens = 0.75
hybrid_static = 0.25

MESH = pl.DeviceIdType.MESH
VMEM = pl.BlockSpec(memory_space=pltpu.VMEM)
F32 = jnp.float32
BF16 = jnp.bfloat16


def split2(x):
    hi = x.astype(BF16)
    return hi, (x - hi.astype(F32)).astype(BF16)


def dot3(left, right):
    lh, ll = left
    rh, rl = right
    d = functools.partial(jnp.dot, preferred_element_type=F32)
    return d(lh, rh) + (d(ll, rh) + d(lh, rl))


AXES = ("lon", "lat", "mem")


def fused(a_ref, s_ref, i_ref, w_ref, v_ref, bw_ref, ens_ref, static_ref, *scratch, dims):
    members, levels, lon_cells, lat_cells, sizes = dims
    (fc, fr, bc, br, qc, qr, send_al, send_ah, recv_al, recv_ah, pack_l, pack_h, recv_pl, recv_ph,
     fpack, xrh, xrl, two_c, two_r, two_l, one_c, one_r, one_l, bflat, dflat, cov, part,
     slots, slots2, dslots, dsend, smoothed_lat, send, recv, csend, crecv, dsems, drems) = scratch
    lon_n, lat_n, mem_n = sizes
    total = lon_n * lat_n * mem_n
    fields = members + 1
    ext = lon_cells + 2 * RIM
    rows = levels * lon_cells
    chunk = rows // mem_n
    coef_ens = math.sqrt(hybrid_ens / (members * mem_n))
    coef_static = math.sqrt(hybrid_static)
    mine = [lax.axis_index(a) for a in AXES]
    lat_at, me = mine[1], mine[2]
    has_low, has_high = lat_at > 0, lat_at < lat_n - 1

    def shifted(step):
        parts, rest = [], step
        for size in reversed(sizes):
            parts.append(rest % size)
            rest //= size
        return tuple(lax.rem(m + s, size) for m, s, size in zip(mine, reversed(parts), sizes))

    barrier = pltpu.get_barrier_semaphore()
    for step in range(1, total):
        pl.semaphore_signal(barrier, inc=1, device_id=shifted(step), device_id_type=MESH)

    used = [0]

    def remote(src, dst, where):
        k = used[0]
        used[0] += 1
        return pltpu.make_async_remote_copy(
            src_ref=src, dst_ref=dst, send_sem=send.at[k], recv_sem=recv.at[k],
            device_id=where, device_id_type=MESH,
        )

    lon_low = {"lon": lax.rem(mine[0] + lon_n - 1, lon_n)}
    lon_high = {"lon": lax.rem(mine[0] + 1, lon_n)}
    lat_low = {"lat": lax.rem(lat_at + lat_n - 1, lat_n)}
    lat_high = {"lat": lax.rem(lat_at + 1, lat_n)}
    own = pl.ds(0, lon_cells)
    rim = pl.ds(lon_cells, 2 * RIM)
    low_rows = pl.ds(lon_cells, RIM)
    high_rows = pl.ds(lon_cells + RIM, RIM)
    first_rows = pl.ds(0, RIM)
    last_rows = pl.ds(lon_cells - RIM, RIM)
    low_lanes = pl.ds(0, lat_cells)
    high_lanes = pl.ds(lat_cells, lat_cells)

    def lon_start(copies):
        for c in copies:
            c.start()

    def lon_wait(copies):
        for c in copies:
            c.wait()

    class Lat:
        def __init__(self, low_src, high_src, from_low, from_high):
            self.to_low = remote(low_src, from_high, lat_low)
            self.to_high = remote(high_src, from_low, lat_high)

        def start(self):
            pl.when(has_low)(self.to_low.start)
            pl.when(has_high)(self.to_high.start)

        def wait(self):
            pl.when(has_low)(self.to_low.wait_send)
            pl.when(has_high)(self.to_high.wait_send)
            pl.when(has_high)(self.to_low.wait_recv)
            pl.when(has_low)(self.to_high.wait_recv)

    def lane_pack(read, count):
        lane = lax.broadcasted_iota(jnp.int32, (count, lat_cells), 1)
        low = jnp.zeros((count, lat_cells), F32)
        high = low
        for l in range(levels):
            x = read(l)
            here = (lane >= l * RIM) & (lane < (l + 1) * RIM)
            low = jnp.where(here, pltpu.roll(x, (l * RIM) % lat_cells, 1), low)
            high = jnp.where(here, pltpu.roll(x, ((l + 1) * RIM) % lat_cells, 1), high)
        return low, high

    def zero_edges(ref, lead=()):
        @pl.when(jnp.logical_not(has_low))
        def _():
            ref[(*lead, slice(None), low_lanes)] = jnp.zeros((ext, lat_cells), F32)

        @pl.when(jnp.logical_not(has_high))
        def _():
            ref[(*lead, slice(None), high_lanes)] = jnp.zeros((ext, lat_cells), F32)

    def load_member(m, _):
        lows, highs = [], []
        for l in range(levels):
            x = a_ref[m, l].astype(F32)
            fc[l, m, :lon_cells, :] = x
            lows.append(x[:RIM])
            highs.append(x[lon_cells - RIM :])
        send_al[m] = jnp.concatenate(lows, axis=0).astype(BF16)
        send_ah[m] = jnp.concatenate(highs, axis=0).astype(BF16)
        return 0

    lax.fori_loop(0, members, load_member, 0)
    for l in range(levels):
        fc[l, members, :lon_cells, :] = s_ref[l]

    def pack_member(span, count):
        def go(m, _):
            low, high = lane_pack(lambda l: fc[l, m, span, :], count)
            pack_l[m, span, :] = low.astype(BF16)
            pack_h[m, span, :] = high.astype(BF16)
            return 0

        lax.fori_loop(0, members, go, 0)

    def lon_field(ref, lead):
        at = lambda span: ref.at[(slice(None), *lead, span, slice(None))]
        return [
            remote(at(first_rows), at(high_rows), lon_low),
            remote(at(last_rows), at(low_rows), lon_high),
        ]

    def lat_field(slot, dst, lead, span):
        at = lambda lanes: dst.at[(*lead, span, lanes)]
        return Lat(
            fpack.at[slot, 0, span, :], fpack.at[slot, 1, span, :], at(low_lanes), at(high_lanes)
        )

    def fill_pack(slot, read, span, count):
        low, high = lane_pack(lambda l: read(l, span), count)
        fpack[slot, 0, span, :] = low
        fpack[slot, 1, span, :] = high

    read_s = lambda l, span: fc[l, members, span, :]
    read_b = lambda l, span: bc[l, span, :]
    read_q = lambda l, span: qc[l, span, :]

    pl.semaphore_wait(barrier, total - 1)
    lon_a = [remote(send_al, recv_ah, lon_low), remote(send_ah, recv_al, lon_high)]
    lon_start(lon_a)
    lon_s = lon_field(fc, (members,))
    lon_start(lon_s)
    pack_member(own, lon_cells)
    lat_a = Lat(pack_l.at[:, own, :], pack_h.at[:, own, :], recv_pl.at[:, own, :], recv_ph.at[:, own, :])
    lat_a.start()

    idx, val_w = i_ref[...], w_ref[...]
    n_obs = idx.shape[1]
    row, lane = idx // lat_cells, idx % lat_cells
    at_row = (lax.broadcasted_iota(jnp.int32, (rows, n_obs), 0) == row).astype(F32).astype(BF16)
    at_lane = lax.broadcasted_iota(jnp.int32, (lat_cells, n_obs), 0) == lane
    for val, out in ((val_w, dflat), (val_w * v_ref[...], bflat)):
        acc = None
        for _ in range(3):
            piece_val = val.astype(BF16).astype(F32)
            val = val - piece_val
            placed = jnp.where(at_lane, piece_val, 0.0).astype(BF16)
            term = lax.dot_general(
                at_row, placed, (((1,), (1,)), ((), ())), preferred_element_type=F32
            )
            acc = term if acc is None else acc + term
        out[...] = acc
    for l in range(levels):
        bc[l, :lon_cells, :] = bflat[l * lon_cells : (l + 1) * lon_cells, :]
    lon_b = lon_field(bc, ())
    lon_start(lon_b)
    fill_pack(0, read_s, own, lon_cells)
    fill_pack(1, read_b, own, lon_cells)
    lat_sb = [lat_field(0, fr, (members,), own), lat_field(1, br, (), own)]
    for c in lat_sb:
        c.start()
    zero_edges(fr, (members,))
    zero_edges(br)
    zero_edges(qr)

    def iota(shape, dim):
        return lax.broadcasted_iota(jnp.int32, shape, dim)

    def ext_place(index, cells):
        return jnp.where(index < cells, index, jnp.where(index < cells + RIM, index - cells - RIM, index - RIM))

    def make_matrices(l, _):
        taps = (iota((8, 128), 1) - BAND).astype(F32)

        def weights(kind):
            width = bw_ref[kind, l].astype(F32) + jnp.zeros((1, 1), F32)

            def raw(o):
                return jnp.where(jnp.abs(o) <= width, jnp.exp(-0.5 * (o / (0.5 * width)) ** 2), 0.0)

            norm = jnp.sum(raw(taps)[:1], axis=1, keepdims=True)
            return lambda o: raw(o.astype(F32)) / norm

        def put(ref, where, value):
            hi, lo = split2(value)
            ref[(0, *where)] = hi
            ref[(1, *where)] = lo

        w = weights(0)
        mids = 128 * pl.cdiv(lon_cells + 2 * BAND, 128)
        near = w(iota((lon_cells, mids), 0) - (iota((lon_cells, mids), 1) - BAND))
        near = jnp.where(iota((lon_cells, mids), 1) < lon_cells + 2 * BAND, near, 0.0)
        far = w(iota((mids, ext), 0) - BAND - ext_place(iota((mids, ext), 1), lon_cells))
        put(two_l, (l,), dot3(split2(near), split2(far)))
        put(one_l, (l,), w(iota((lon_cells, ext), 0) - ext_place(iota((lon_cells, ext), 1), lon_cells)))

        w = weights(1)
        mids = 128 * pl.cdiv(lat_cells + 2 * BAND, 128)
        mid = iota((mids, lat_cells), 0) - BAND
        place = lat_at * lat_cells + mid
        keep = (place >= 0) & (place < lat_cells * lat_n) & (mid < lat_cells + BAND)
        back = split2(jnp.where(keep, w(mid - iota((mids, lat_cells), 1)), 0.0))
        out = iota((lat_cells, lat_cells), 1)
        here = iota((lat_cells, mids), 0) - (iota((lat_cells, mids), 1) - BAND)
        put(two_c, (l,), dot3(split2(w(here)), back))
        put(one_c, (l,), w(iota((lat_cells, lat_cells), 0) - out))
        columns = pl.ds(pl.multiple_of(l * lat_cells, lat_cells), lat_cells)
        for side in range(2):
            shift = -RIM if side == 0 else lat_cells
            span = pl.ds(side * lat_cells, lat_cells)

            def rim_at(shape):
                p = iota(shape, 0) - l * RIM
                return p + shift, (p >= 0) & (p < RIM)

            pos, ok = rim_at((lat_cells, mids))
            there = jnp.where(ok, w(pos - (iota((lat_cells, mids), 1) - BAND)), 0.0)
            put(two_r, (span, columns), dot3(split2(there), back))
            pos, ok = rim_at((lat_cells, lat_cells))
            put(one_r, (span, columns), jnp.where(ok, w(pos - out), 0.0))
        return 0

    lax.fori_loop(0, levels, make_matrices, 0)

    def lat_part(yc, yr, c_mat, r_mat, l, span, count):
        columns = pl.ds(pl.multiple_of(l * lat_cells, lat_cells), lat_cells)
        xc = split2((fc[l, :, span, :] * yc[l, span, :][None]).reshape(fields * count, lat_cells))
        xr = (
            xrh[:, span, :].reshape(fields * count, 2 * lat_cells),
            xrl[:, span, :].reshape(fields * count, 2 * lat_cells),
        )
        t = dot3(xc, (c_mat[0, l], c_mat[1, l]))
        t = t + dot3(xr, (r_mat[0, :, columns], r_mat[1, :, columns]))
        for h, half in enumerate(split2(t)):
            smoothed_lat[h, l, span, :] = jnp.concatenate(
                [half[f * count : (f + 1) * count] for f in range(fields)], axis=1
            )

    def rim_products(yr, span):
        def go(f, _):
            hi, lo = split2(fr[f, span, :] * yr[span, :])
            xrh[f, span, :], xrl[f, span, :] = hi, lo
            return 0

        lax.fori_loop(0, fields, go, 0)

    def apply_own(yc, yr, mats):
        rim_products(yr, own)

        def go(l, _):
            lat_part(yc, yr, mats[0], mats[1], l, own, lon_cells)
            return 0

        lax.fori_loop(0, levels, go, 0)

    def apply_rim(yc, yr, mats, finish):
        rim_products(yr, rim)

        def go(i, _):
            l = lax.rem(me + 1 + i, levels)
            lat_part(yc, yr, mats[0], mats[1], l, rim, 2 * RIM)
            u = dot3((mats[2][0, l], mats[2][1, l]), (smoothed_lat[0, l], smoothed_lat[1, l]))
            finish(i, l, [u[:, f * lat_cells : (f + 1) * lat_cells] for f in range(fields)])
            return 0

        lax.fori_loop(0, levels, go, 0)

    def unpack_lat(span, count):
        for ref, keep, lanes in ((recv_pl, has_low, low_lanes), (recv_ph, has_high, high_lanes)):
            def go(m, _):
                fr[m, span, lanes] = ref[m, span, :].astype(F32)
                return 0

            def clear(m, _):
                fr[m, span, lanes] = jnp.zeros((count, lat_cells), F32)
                return 0

            @pl.when(keep)
            def _():
                lax.fori_loop(0, members, go, 0)

            @pl.when(jnp.logical_not(keep))
            def _():
                lax.fori_loop(0, members, clear, 0)

    lat_a.wait()
    unpack_lat(own, lon_cells)
    for c in lat_sb:
        c.wait()
    apply_own(bc, br, (two_c, two_r, two_l))

    lon_wait(lon_a)

    def unpack_member(m, _):
        low, high = recv_al[m].astype(F32), recv_ah[m].astype(F32)
        for l in range(levels):
            fc[l, m, low_rows, :] = low[l * RIM : (l + 1) * RIM]
            fc[l, m, high_rows, :] = high[l * RIM : (l + 1) * RIM]
        return 0

    lax.fori_loop(0, members, unpack_member, 0)
    pack_member(rim, 2 * RIM)
    lat_a2 = Lat(pack_l.at[:, rim, :], pack_h.at[:, rim, :], recv_pl.at[:, rim, :], recv_ph.at[:, rim, :])
    lat_a2.start()
    lon_wait(lon_s)
    lon_wait(lon_b)
    fill_pack(0, read_s, rim, 2 * RIM)
    fill_pack(1, read_b, rim, 2 * RIM)
    lat_sb2 = [lat_field(0, fr, (members,), rim), lat_field(1, br, (), rim)]
    for c in lat_sb2:
        c.start()
    lat_a2.wait()
    unpack_lat(rim, 2 * RIM)
    for c in lat_sb2:
        c.wait()

    def piece(owner):
        return pl.ds(pl.multiple_of(owner * chunk, chunk), chunk)

    def mem_copy(src, dst, j, group):
        return pltpu.make_async_remote_copy(
            src_ref=src, dst_ref=dst, send_sem=csend.at[group, j], recv_sem=crecv.at[group, j],
            device_id={"mem": lax.rem(me + j, mem_n)}, device_id_type=MESH,
        )

    def sum_copy(dst, j, group):
        return mem_copy(part.at[piece(lax.rem(me + j, mem_n))], dst.at[j], j, group)

    by_level = levels == mem_n

    def finish_cov(dst, group):
        def finish(i, l, smoothed):
            acc = fc[l, 0, :lon_cells, :] * smoothed[0]
            for f in range(1, members):
                acc = acc + fc[l, f, :lon_cells, :] * smoothed[f]
            acc = acc * (coef_ens * coef_ens)
            acc = acc + fc[l, members, :lon_cells, :] * smoothed[members] * (coef_static**2 / mem_n)
            part[pl.ds(pl.multiple_of(l * lon_cells, lon_cells), lon_cells), :] = acc
            if by_level:
                @pl.when(i < mem_n - 1)
                def _():
                    sum_copy(dst, i + 1, group).start()

        return finish

    def scatter_sum(dst, group):
        copies = [sum_copy(dst, j, group) for j in range(1, mem_n)]
        if not by_level:
            for copy in copies:
                copy.start()
        acc = part[piece(me), :]
        for j, copy in enumerate(copies):
            copy.wait_recv()
            acc = acc + dst[j + 1]
        for copy in copies:
            copy.wait_send()
        return acc

    def dots_start(left, right, group):
        at = iota((2, lat_cells), 0)
        a = jnp.sum(left, axis=0, keepdims=True)
        b = jnp.sum(right, axis=0, keepdims=True)
        dsend[group] = jnp.where(at == 0, a, b)
        copies = []
        for step in range(1, total):
            copy = pltpu.make_async_remote_copy(
                src_ref=dsend.at[group], dst_ref=dslots.at[group, step],
                send_sem=dsems.at[group, step], recv_sem=drems.at[group, step],
                device_id=shifted(step), device_id_type=MESH,
            )
            copy.start()
            copies.append(copy)
        return copies

    def dots_end(copies, group):
        for copy in copies:
            copy.wait()
        block = dsend[group] + jnp.sum(dslots[group, 1:], axis=0)
        sums = jnp.sum(block, axis=1, keepdims=True)
        return sums[0:1], sums[1:2]

    two, one = (two_c, two_r, two_l), (one_c, one_r, one_l)
    apply_rim(bc, br, two, finish_cov(slots, 0))
    acc = scatter_sum(slots, 0)
    cov[piece(me), :] = acc
    back = [mem_copy(cov.at[piece(me)], cov.at[piece(me)], j, 1) for j in range(1, mem_n)]
    for copy in back:
        copy.start()
    rhs_mine, diag_mine, cov_mine = bflat[piece(me), :], dflat[piece(me), :], acc
    image_mine = rhs_mine + diag_mine * cov_mine
    dots0 = dots_start(rhs_mine * cov_mine, cov_mine * image_mine, 0)
    for copy in back:
        copy.wait()
    for l in range(levels):
        span = slice(l * lon_cells, (l + 1) * lon_cells)
        qc[l, :lon_cells, :] = bflat[span, :] + dflat[span, :] * cov[span, :]
    lon_q = lon_field(qc, ())
    lon_start(lon_q)
    fill_pack(2, read_q, own, lon_cells)
    lat_q = lat_field(2, qr, (), own)
    lat_q.start()
    lon_wait(lon_q)
    fill_pack(2, read_q, rim, 2 * RIM)
    lat_q2 = lat_field(2, qr, (), rim)
    lat_q2.start()
    lat_q.wait()

    apply_own(qc, qr, two)
    lat_q2.wait()
    apply_rim(qc, qr, two, finish_cov(slots2, 2))
    cov_q = scatter_sum(slots2, 2)
    norm0, curve0 = dots_end(dots0, 0)
    alpha0 = norm0 / curve0
    resid = rhs_mine - alpha0 * image_mine
    cov_r = cov_mine - alpha0 * cov_q
    norm1, curve1 = dots_end(dots_start(resid * cov_r, cov_r * (resid + diag_mine * cov_r), 1), 1)
    beta = norm1 / norm0
    alpha1 = norm1 / (curve1 - beta * norm1 / alpha0)

    def combine(b, q):
        return alpha0 * b + alpha1 * ((b - alpha0 * q) + beta * b)

    for l in range(levels):
        bc[l] = combine(bc[l], qc[l])
    br[...] = combine(br[...], qr[...])

    def finish_control(i, l, smoothed):
        for f in range(members):
            ens_ref[f, l] = coef_ens * smoothed[f]
        static_ref[l] = coef_static * smoothed[members]

    apply_own(bc, br, one)
    apply_rim(bc, br, one, finish_control)


def per_device(anomalies, spread, obs_index, innovation, obs_weight, band_width):
    members = anomalies.shape[0]
    levels, lon_cells, lat_cells = spread.shape
    sizes = tuple(lax.axis_size(a) for a in AXES)
    mem_n, total = sizes[2], math.prod(sizes)
    fields = members + 1
    ext = lon_cells + 2 * RIM
    rows = levels * lon_cells
    chunk = rows // mem_n
    v = pltpu.VMEM
    sem = pltpu.SemaphoreType.DMA
    edge = v((members, levels * RIM, lat_cells), BF16)
    packed = v((members, ext, lat_cells), BF16)
    field = v((levels, ext, lat_cells), F32)
    field_rim = v((ext, 2 * lat_cells), F32)
    mats = [
        v((2, levels, lat_cells, lat_cells), BF16),
        v((2, 2 * lat_cells, levels * lat_cells), BF16),
        v((2, levels, lon_cells, ext), BF16),
    ]
    flat = v((rows, lat_cells), F32)
    scratch = [
        v((levels, fields, ext, lat_cells), F32),
        v((fields, ext, 2 * lat_cells), F32),
        field, field_rim, field, field_rim,
        edge, edge, edge, edge,
        packed, packed, packed, packed,
        v((3, 2, ext, lat_cells), F32),
        v((fields, ext, 2 * lat_cells), BF16),
        v((fields, ext, 2 * lat_cells), BF16),
        *mats, *mats,
        flat, flat, flat, flat,
        v((mem_n, chunk, lat_cells), F32),
        v((mem_n, chunk, lat_cells), F32),
        v((2, total, 2, lat_cells), F32),
        v((2, 2, lat_cells), F32),
        v((2, levels, ext, fields * lat_cells), BF16),
        sem((32,)), sem((32,)), sem((3, mem_n)), sem((3, mem_n)), sem((2, total)), sem((2, total)),
    ]
    kernel = functools.partial(fused, dims=(members, levels, lon_cells, lat_cells, sizes))
    return pl.pallas_call(
        kernel,
        out_shape=[
            jax.ShapeDtypeStruct((members, levels, lon_cells, lat_cells), F32),
            jax.ShapeDtypeStruct((levels, lon_cells, lat_cells), F32),
        ],
        in_specs=[VMEM] * 5 + [pl.BlockSpec(memory_space=pltpu.SMEM)],
        out_specs=[VMEM] * 2,
        scratch_shapes=scratch,
        compiler_params=pltpu.CompilerParams(
            collective_id=0, has_side_effects=True, vmem_limit_bytes=60 * 2**20
        ),
    )(
        anomalies, spread, obs_index.reshape(1, -1), obs_weight.reshape(1, -1),
        innovation.reshape(1, -1), band_width,
    )


def paired(a_hbm, s_hbm, i_hbm, w_hbm, v_hbm, bw_hbm, ub_ref, uq_ref, st_ref, coef_ref, *scratch, dims):
    members, levels, lon_cells, lat_cells, sizes = dims
    (acen, arim, plo, phi, sfull, sedge, srim, srims, spack, spacks, oidx, ow, ov, at_row, grid, grim, gpack, cov, orecv,
     drecv, mat_c, mat_r, lon_t, lon_l, xr, xq, xo, tc, ts, to, bw_ref, send, recv, load, relay) = scratch
    lon_n, lat_n, mem_n = sizes
    half = members // lon_n
    full = lon_n * lon_cells
    group = lon_n * mem_n
    rows = levels * lon_cells
    wide = lat_cells
    edge = 16 * pl.cdiv(BAND, 16)
    reach = lon_cells + 2 * edge
    n_obs = oidx.shape[2]
    coef_ens = math.sqrt(hybrid_ens / (members * mem_n))
    coef_static = math.sqrt(hybrid_static)
    at_lon, lat_at, me = (lax.axis_index(a) for a in AXES)
    other = 1 - at_lon
    has_low, has_high = lat_at > 0, lat_at < lat_n - 1
    my_id = at_lon * mem_n + me

    def group_peer(step):
        peer = lax.rem(my_id + step, group)
        return {"lon": peer // mem_n, "mem": lax.rem(peer, mem_n)}

    def lat_peer(step):
        return {"lat": lax.rem(lat_at + step, lat_n)}

    own_rows, far_rows = pl.ds(0, lon_cells), pl.ds(lon_cells, lon_cells)
    first, second = pl.ds(0, half), pl.ds(half, half)
    loads = [
        pltpu.make_async_copy(src, dst, load.at[k])
        for k, (src, dst) in enumerate((
            (i_hbm, oidx.at[0]),
            (w_hbm, ow.at[0]),
            (v_hbm, ov.at[0]),
            (s_hbm, sfull.at[:, own_rows]),
            (a_hbm.at[pl.ds(other * half, half)], acen.at[second, :, own_rows, :]),
            (a_hbm.at[pl.ds(at_lon * half, half)], acen.at[first, :, own_rows, :]),
            (bw_hbm, bw_ref),
        ))
    ]
    for copy in loads:
        copy.start()

    near = [
        (True, {"lon": other}),
        (has_low, {"lat": lat_at - 1}),
        (has_high, {"lat": lat_at + 1}),
        (me > 0, {"mem": me - 1}),
        (me < mem_n - 1, {"mem": me + 1}),
    ]
    n_near = sum(jnp.asarray(there, jnp.int32) for there, _ in near)

    def greet(sem):
        for there, where in near:
            def go(where=where):
                pl.semaphore_signal(sem, inc=1, device_id=where, device_id_type=MESH)

            go() if there is True else pl.when(there)(go)

    def relay_round(r):
        pl.semaphore_wait(relay.at[r], n_near)
        if r + 1 < rounds:
            greet(relay.at[r + 1])

    rounds = max(lon_n + mem_n - 2, lat_n - 1) - 1
    barrier = pltpu.get_barrier_semaphore()
    greet(barrier)

    used = [0]

    def remote(src, dst, where):
        k = used[0]
        used[0] += 1
        return pltpu.make_async_remote_copy(
            src_ref=src, dst_ref=dst, send_sem=send.at[k], recv_sem=recv.at[k],
            device_id=where, device_id_type=MESH,
        )

    partner = {"lon": other}
    lat_low = {"lat": lax.rem(lat_at + lat_n - 1, lat_n)}
    lat_high = {"lat": lax.rem(lat_at + 1, lat_n)}
    low_lanes = pl.ds(0, wide)
    high_lanes = pl.ds(wide, wide)

    class Lat:
        def __init__(self, low_src, high_src, from_low, from_high):
            self.to_low = remote(low_src, from_high, lat_low)
            self.to_high = remote(high_src, from_low, lat_high)

        def start(self):
            pl.when(has_low)(self.to_low.start)
            pl.when(has_high)(self.to_high.start)

        def wait(self):
            pl.when(has_low)(self.to_low.wait_send)
            pl.when(has_high)(self.to_high.wait_send)
            pl.when(has_high)(self.to_low.wait_recv)
            pl.when(has_low)(self.to_high.wait_recv)

    def iota(shape, dim):
        return lax.broadcasted_iota(jnp.int32, shape, dim)

    def lane_pack(read, count, at_levels=None):
        lane = iota((count, wide), 1)
        low = jnp.zeros((count, wide), F32)
        high = low
        for l in range(levels) if at_levels is None else at_levels:
            x = read(l)
            here = (lane >= l * RIM) & (lane < (l + 1) * RIM)
            low = jnp.where(here, pltpu.roll(x, lax.rem(l * RIM, wide), 1), low)
            high = jnp.where(here, pltpu.roll(x, lax.rem((l + 1) * RIM, wide), 1), high)
        return low, high

    def pack_member(p, span, count):
        low, high = lane_pack(lambda l: acen[p, l, span, :].astype(F32), count)
        plo[p, span, :] = low.astype(BF16)
        phi[p, span, :] = high.astype(BF16)

    def pack_static(span, count):
        low, high = lane_pack(lambda l: sfull[me, span, :], count, [me])
        spack[0, span, :] = low
        spack[1, span, :] = high

    def pack_statics(ref, span, to_span, count):
        low, high = lane_pack(lambda l: ref[l, span, :], count)
        spacks[0, to_span, :] = low
        spacks[1, to_span, :] = high

    def lat_members(which, span):
        return Lat(
            plo.at[which, span, :], phi.at[which, span, :],
            arim.at[which, span, low_lanes], arim.at[which, span, high_lanes],
        )

    def lat_static(span, pack=spack, rim=srim):
        return Lat(
            pack.at[0, span, :], pack.at[1, span, :],
            rim.at[span, low_lanes], rim.at[span, high_lanes],
        )

    def lat_grid(g):
        return Lat(gpack.at[g, 0], gpack.at[g, 1], grim.at[g, :, low_lanes], grim.at[g, :, high_lanes])

    x_obs = [remote(ref.at[0], ref.at[1], partner) for ref in (oidx, ow, ov)]
    x_static = remote(sfull.at[me, own_rows], sfull.at[me, far_rows], partner)
    x_first = [
        remote(acen.at[half + p, :, own_rows, :], acen.at[p, :, far_rows, :], partner)
        for p in range(half)
    ]
    edges = pl.ds(lon_cells, 2 * edge)
    x_edge = []
    for src, k in ((0, 0), (lon_cells - edge, edge)):
        src, dst = pl.ds(src, edge), pl.ds(lon_cells + k, edge)
        x_edge.append(remote(acen.at[first, :, src, :], acen.at[second, :, dst, :], partner))
        x_edge.append(remote(sfull.at[:, src], sedge.at[:, pl.ds(k, edge)], partner))
    for copy in loads:
        copy.wait()
    pl.semaphore_wait(barrier, n_near)
    for copy in [*x_obs, *x_first, x_static]:
        copy.start()
    greet(relay.at[0])

    def pack_first(p, _):
        pack_member(p, own_rows, lon_cells)
        return 0

    lax.fori_loop(0, half, pack_first, 0)
    lat_a = lat_members(first, own_rows)
    lat_a.start()
    pack_static(own_rows, lon_cells)
    lat_s = lat_static(own_rows)
    lat_s.start()
    lax.fori_loop(half, members, pack_first, 0)
    lat_a3 = lat_members(second, own_rows)
    lat_a3.start()
    pack_statics(sfull, own_rows, own_rows, lon_cells)
    lat_s3 = lat_static(own_rows, spacks, srims)
    lat_s3.start()

    @pl.when(jnp.logical_not(has_low))
    def _():
        arim[:, :, low_lanes] = jnp.zeros((members, full, wide), BF16)
        srim[:, low_lanes] = jnp.zeros((full, wide), F32)
        srims[:, low_lanes] = jnp.zeros((reach, wide), F32)
        grim[:, :, low_lanes] = jnp.zeros((2, full, wide), F32)

    @pl.when(jnp.logical_not(has_high))
    def _():
        arim[:, :, high_lanes] = jnp.zeros((members, full, wide), BF16)
        srim[:, high_lanes] = jnp.zeros((full, wide), F32)
        srims[:, high_lanes] = jnp.zeros((reach, wide), F32)
        grim[:, :, high_lanes] = jnp.zeros((2, full, wide), F32)

    relay_round(0)
    slot_rows = (own_rows, far_rows)
    slot_tile = (at_lon, other)

    def mark_rows(s):
        row = oidx[s] // wide
        at_row[s] = (iota((rows, n_obs), 0) == row).astype(F32).astype(BF16)

    def scatter(s, value, g):
        at_lane = iota((wide, n_obs), 0) == oidx[s] % wide
        hi = value.astype(BF16).astype(F32)
        lo = value - hi
        placed = jnp.concatenate(
            [jnp.where(at_lane, hi, 0.0).astype(BF16), jnp.where(at_lane, lo, 0.0).astype(BF16)], axis=0
        )
        out = lax.dot_general(
            at_row[s], placed, (((1,), (1,)), ((), ())), preferred_element_type=F32
        )
        out = out[:, :wide] + out[:, wide:]
        for l in range(levels):
            grid[g, l, slot_rows[s], :] = out[l * lon_cells : (l + 1) * lon_cells]

    def gather(s, g):
        hi, lo = split2(cov[s].T)
        left = jnp.concatenate([hi, lo], axis=0)
        step = 512 if n_obs % 512 == 0 else n_obs
        for c in range(0, n_obs, step):
            part = jnp.dot(left, at_row[s, :, c : c + step], preferred_element_type=F32)
            lane = oidx[s, :, c : c + step] % wide
            here = iota((wide, step), 0) == lane
            value = jnp.where(here, part[:wide] + part[wide:], 0.0)
            orecv[g, my_id, slot_tile[s], :, c : c + step] = jnp.sum(value, axis=0, keepdims=True)

    def send_grid(g):
        low, high = lane_pack(lambda l: grid[g, l], full)
        gpack[g, 0] = low
        gpack[g, 1] = high
        copy = lat_grid(g)
        copy.start()
        return copy

    mark_rows(0)
    scatter(0, ow[0] * ov[0], 0)

    def make_matrices(l, _):
        taps = (iota((8, 128), 1) - BAND).astype(F32)

        def weights(kind):
            width = bw_ref[kind, l].astype(F32) + jnp.zeros((1, 1), F32)

            def raw(o):
                return jnp.where(jnp.abs(o) <= width, jnp.exp(-0.5 * (o / (0.5 * width)) ** 2), 0.0)

            norm = jnp.sum(raw(taps)[:1], axis=1, keepdims=True)
            return lambda o: raw(o.astype(F32)) / norm

        def put_lon(ref, count, value):
            hi, lo = split2(value)
            cols = value.shape[1]
            ref[l, :count, :] = jnp.concatenate([hi, hi], axis=1)
            ref[l, count:, :] = jnp.concatenate([lo, jnp.zeros((count, cols), BF16)], axis=1)

        w = weights(0)

        def ring(count, cols):
            c = iota((count, cols), 1)
            if cols < full:
                c = jnp.where(c < lon_cells + edge, c, c + full - cols)
            d = c - iota((count, cols), 0)
            d = jnp.where(d > full // 2, d - full, d)
            return w(jnp.where(d < -(full // 2), d + full, d))

        circle = split2(ring(full, full))
        put_lon(lon_t, full, dot3(circle, circle))
        put_lon(lon_l, lon_cells, ring(lon_cells, reach))

        def put_lat(ref, kind, hi_at, lo_at, value):
            hi, lo = split2(value)
            ref[kind, l, pl.ds(hi_at, wide), :wide] = hi
            ref[kind, l, pl.ds(hi_at, wide), wide:] = lo
            ref[kind, l, pl.ds(lo_at, wide), :wide] = hi
            ref[kind, l, pl.ds(lo_at, wide), wide:] = jnp.zeros((wide, wide), BF16)

        w = weights(1)
        mids = 128 * pl.cdiv(wide + 2 * BAND, 128)
        mid = iota((mids, wide), 0) - BAND
        place = lat_at * wide + mid
        keep = (place >= 0) & (place < wide * lat_n) & (mid < wide + BAND)
        back = split2(jnp.where(keep, w(mid - iota((mids, wide), 1)), 0.0))
        out = iota((wide, wide), 1)
        here = iota((wide, mids), 0) - (iota((wide, mids), 1) - BAND)
        put_lat(mat_c, 0, 0, wide, dot3(split2(w(here)), back))
        put_lat(mat_c, 1, 0, wide, w(iota((wide, wide), 0) - out))
        for side in range(2):
            shift = -RIM if side == 0 else wide

            def rim_at(shape):
                p = iota(shape, 0) - l * RIM
                return p + shift, (p >= 0) & (p < RIM)

            pos, ok = rim_at((wide, mids))
            there = jnp.where(ok, w(pos - (iota((wide, mids), 1) - BAND)), 0.0)
            put_lat(mat_r, 0, side * wide, (2 + side) * wide, dot3(split2(there), back))
            pos, ok = rim_at((wide, wide))
            put_lat(mat_r, 1, side * wide, (2 + side) * wide, jnp.where(ok, w(pos - out), 0.0))
        return 0

    lax.fori_loop(0, levels, make_matrices, 0)
    for r in range(1, rounds):
        relay_round(r)

    for copy in x_obs:
        copy.wait()
    mark_rows(1)
    scatter(1, ow[1] * ov[1], 0)
    lat_b = send_grid(0)

    def dot(a, b):
        return jnp.dot(a, b, preferred_element_type=F32)

    def fold(t):
        return t[:, :wide] + t[:, wide:]

    def pair(x):
        return jnp.concatenate(split2(x), axis=1)

    def stack(x):
        return jnp.concatenate(split2(x), axis=0)

    def reached(x):
        return jnp.concatenate([x[: lon_cells + edge], x[full - edge :]], axis=0)

    def rim_member(g, p):
        xr[p] = pair(arim[p].astype(F32) * grim[g])

    def center_member(g, p):
        for l in range(levels):
            tc[p, l] = fold(dot(pair(acen[p, l].astype(F32) * grid[g, l]), mat_c[0, l]))

    def lat_member(p, at):
        for l in range(levels):
            ts[l, :, at] = stack(tc[p, l] + fold(dot(xr[p], mat_r[0, l])))

    def cov_level(l):
        u = dot(lon_t[l], ts[l])
        u = u[:full] + u[full:]
        acc = acen[0, l].astype(F32) * u[:, :wide]
        for p in range(1, half):
            acc = acc + acen[p, l].astype(F32) * u[:, p * wide : (p + 1) * wide]
        acc = acc * (coef_ens * coef_ens)
        for j in range(lon_n):
            cov[j, l * lon_cells : (l + 1) * lon_cells, :] = acc[j * lon_cells : (j + 1) * lon_cells]

    def cov_static(g):
        t = dot(pair(sfull[me] * grid[g, me]), mat_c[0, me])
        t = t + dot(pair(srim[...] * grim[g]), mat_r[0, me])
        u = dot(lon_t[me], stack(fold(t)))
        acc = sfull[me] * (u[:full] + u[full:]) * (coef_static**2 / lon_n)
        at = pl.ds(pl.multiple_of(me * lon_cells, lon_cells), lon_cells)
        for j in range(lon_n):
            cov[j, at, :] = cov[j, at, :] + acc[j * lon_cells : (j + 1) * lon_cells]

    lat_a2 = []
    for p in range(half):
        x_first[p].wait()
        pack_member(p, far_rows, lon_cells)
        copy = lat_members(p, far_rows)
        copy.start()
        lat_a2.append(copy)
        center_member(0, p)
    x_static.wait()
    for copy in x_edge:
        copy.start()
    pack_static(far_rows, lon_cells)
    lat_s2 = lat_static(far_rows)
    lat_s2.start()

    def share(g):
        for s in range(lon_n):
            gather(s, g)
        copies = []
        for step in range(1, group):
            copy = remote(orecv.at[g, my_id], orecv.at[g, my_id], group_peer(step))
            copy.start()
            copies.append(copy)
        return copies

    def shared(copies, g):
        for copy in copies:
            copy.wait()
        sums = []
        for s in range(lon_n):
            acc = orecv[g, 0, slot_tile[s]]
            for k in range(1, group):
                acc = acc + orecv[g, k, slot_tile[s]]
            sums.append(acc)
        return sums

    def out_rows(l, cells, reads):
        n = len(reads)
        for p, read in enumerate(reads):
            xo[p * reach : (p + 1) * reach] = pair(read() * cells)
        t = fold(dot(xo[: n * reach], mat_c[1, l]) + dot(xq[: n * reach], mat_r[1, l]))
        for p in range(n):
            to[l, :, p * wide : (p + 1) * wide] = stack(t[p * reach : (p + 1) * reach])
        u = dot(lon_l[l], to[l, :, : n * wide])
        u = u[:lon_cells] + u[lon_cells:]
        return [u[:, p * wide : (p + 1) * wide] for p in range(n)]

    def out_first(g):
        out_ref = (ub_ref, uq_ref)[g]
        for p in range(half):
            xq[p * reach : (p + 1) * reach] = reached(xr[p])

        def go(l, _):
            reads = [lambda p=p: reached(acen[p, l]).astype(F32) for p in range(half)]
            for p, u in enumerate(out_rows(l, reached(grid[g, l]), reads)):
                out_ref[at_lon * half + p, l] = u * coef_ens
            return 0

        lax.fori_loop(0, levels, go, 0)

    def out_second(g, start, stop):
        out_ref = (ub_ref, uq_ref)[g]
        near_rim = reached(grim[g])
        for p in range(half):
            xq[p * reach : (p + 1) * reach] = pair(arim[half + p, :reach].astype(F32) * near_rim)
        xq[half * reach :] = pair(srims[...] * near_rim)

        def go(l, _):
            reads = [lambda p=p: acen[half + p, l, :reach].astype(F32) for p in range(half)]
            reads.append(lambda: jnp.concatenate([sfull[l, :lon_cells], sedge[l]], axis=0))
            us = out_rows(l, reached(grid[g, l]), reads)
            for p in range(half):
                out_ref[other * half + p, l] = us[p] * coef_ens
            st_ref[g, l] = us[half] * coef_static
            return 0

        lax.fori_loop(start, stop, go, 0)

    def dots_start(g, left, right):
        def total(pairs):
            acc = None
            for x in pairs:
                for c in range(0, n_obs, 128):
                    part = x[:, c : c + 128]
                    acc = part if acc is None else acc + part
            return acc

        at = iota((2, 128), 0)
        drecv[g, lat_at] = jnp.where(at == 0, total(left), total(right))
        copies = []
        for step in range(1, lat_n):
            copy = remote(drecv.at[g, lat_at], drecv.at[g, lat_at], lat_peer(step))
            copy.start()
            copies.append(copy)
        return copies

    def dots_end(copies, g):
        for copy in copies:
            copy.wait()
        block = drecv[g, 0]
        for k in range(1, lat_n):
            block = block + drecv[g, k]
        sums = jnp.sum(block, axis=1, keepdims=True)
        return sums[0:1], sums[1:2]

    def rim_and_cov(g):
        for p in range(half):
            if g == 0:
                lat_a2[p].wait()
            rim_member(g, p)
            if g == 0:
                lat_member(p, slice(p * wide, (p + 1) * wide))
        if g > 0:
            rims = xr[:half].reshape(half * full, 4 * wide)
            for l in range(levels):
                t = fold(dot(rims, mat_r[0, l]))
                for p in range(half):
                    part = tc[p, l] + t[p * full : (p + 1) * full]
                    ts[l, :, p * wide : (p + 1) * wide] = stack(part)
        if g == 0:
            lat_s.wait()
            lat_s2.wait()
        for l in range(levels):
            cov_level(l)
        cov_static(g)
        return share(g)

    lat_b.wait()
    lat_a.wait()
    sharing = rim_and_cov(0)

    out_first(0)
    for copy in x_edge:
        copy.wait()

    def pack_second(p, _):
        pack_member(p, edges, 2 * edge)
        return 0

    lax.fori_loop(half, members, pack_second, 0)
    lat_a4 = lat_members(second, edges)
    lat_a4.start()
    pack_statics(sedge, slice(None), edges, 2 * edge)
    lat_s4 = lat_static(edges, spacks, srims)
    lat_s4.start()

    cz = shared(sharing, 0)
    z = [ow[s] * ov[s] for s in range(lon_n)]
    q = [z[s] + ow[s] * cz[s] for s in range(lon_n)]
    for s in range(lon_n):
        scatter(s, q[s], 1)
    lat_q = send_grid(1)
    dots0 = dots_start(0, [z[s] * cz[s] for s in range(lon_n)], [cz[s] * q[s] for s in range(lon_n)])

    def center_all(l, _):
        for p in range(half):
            xo[p * full : (p + 1) * full] = pair(acen[p, l].astype(F32) * grid[1, l])
        t = fold(dot(xo[: half * full], mat_c[0, l]))
        for p in range(half):
            tc[p, l] = t[p * full : (p + 1) * full]
        return 0

    lax.fori_loop(0, levels, center_all, 0)
    for copy in (lat_a3, lat_a4, lat_s3, lat_s4):
        copy.wait()
    out_second(0, 0, levels // 2)
    lat_q.wait()
    sharing = rim_and_cov(1)
    out_first(1)
    out_second(1, 0, levels - 1)

    cq = shared(sharing, 1)
    norm0, curve0 = dots_end(dots0, 0)
    alpha0 = norm0 / curve0
    resid = [z[s] - alpha0 * q[s] for s in range(lon_n)]
    cr = [cz[s] - alpha0 * cq[s] for s in range(lon_n)]
    dots1 = dots_start(
        1,
        [resid[s] * cr[s] for s in range(lon_n)],
        [cr[s] * (resid[s] + ow[s] * cr[s]) for s in range(lon_n)],
    )
    out_second(0, levels // 2, levels)
    out_second(1, levels - 1, levels)
    norm1, curve1 = dots_end(dots1, 1)
    beta = norm1 / norm0
    alpha1 = norm1 / (curve1 - beta * norm1 / alpha0)
    on_b = alpha0 + alpha1 * (1.0 + beta)
    on_q = -alpha0 * alpha1
    coef_ref[...] = jnp.where(iota((2, 128), 0) == 0, on_b, on_q)


def combine(ub_ref, uq_ref, st_ref, coef_ref, ens_ref, static_ref, ens, static, sems):
    on_b, on_q = coef_ref[0:1, :], coef_ref[1:2, :]
    members = ens.shape[0]
    copies = []
    for m in range(members):
        ens[m] = on_b * ub_ref[m] + on_q * uq_ref[m]
        copies.append(pltpu.make_async_copy(ens.at[m], ens_ref.at[m], sems.at[m]))
        copies[-1].start()
    static[...] = on_b * st_ref[0] + on_q * st_ref[1]
    copies.append(pltpu.make_async_copy(static, static_ref, sems.at[members]))
    copies[-1].start()
    for copy in copies:
        copy.wait()


def paired_device(anomalies, spread, obs_index, innovation, obs_weight, band_width):
    members = anomalies.shape[0]
    levels, lon_cells, lat_cells = spread.shape
    sizes = tuple(lax.axis_size(a) for a in AXES)
    lon_n, lat_n, mem_n = sizes
    half = members // lon_n
    full = lon_n * lon_cells
    group = lon_n * mem_n
    n_obs = obs_index.shape[-1]
    v = pltpu.VMEM
    sem = pltpu.SemaphoreType.DMA
    wide = lat_cells
    reach = lon_cells + 2 * 16 * pl.cdiv(BAND, 16)
    copies = 8 + half + 2 * (9 + half) + 2 * (group - 1 + lat_n - 1)
    scratch = [
        v((members, levels, full, wide), BF16),
        v((members, full, 2 * wide), BF16),
        v((members, full, wide), BF16),
        v((members, full, wide), BF16),
        v((levels, full, wide), F32),
        v((levels, reach - lon_cells, wide), F32),
        v((full, 2 * wide), F32),
        v((reach, 2 * wide), F32),
        v((2, full, wide), F32),
        v((2, reach, wide), F32),
        v((lon_n, 1, n_obs), jnp.int32),
        v((lon_n, 1, n_obs), F32),
        v((lon_n, 1, n_obs), F32),
        v((lon_n, levels * lon_cells, n_obs), BF16),
        v((2, levels, full, wide), F32),
        v((2, full, 2 * wide), F32),
        v((2, 2, full, wide), F32),
        v((lon_n, levels * lon_cells, wide), F32),
        v((2, group, lon_n, 1, n_obs), F32),
        v((2, lat_n, 2, 128), F32),
        v((2, levels, 2 * wide, 2 * wide), BF16),
        v((2, levels, 4 * wide, 2 * wide), BF16),
        v((levels, 2 * full, 2 * full), BF16),
        v((levels, 2 * lon_cells, 2 * reach), BF16),
        v((half, full, 4 * wide), BF16),
        v(((half + 1) * reach, 4 * wide), BF16),
        v((max(half * full, (half + 1) * reach), 2 * wide), BF16),
        v((half, levels, full, wide), F32),
        v((levels, 2 * full, half * wide), BF16),
        v((levels, 2 * reach, (half + 1) * wide), BF16),
        pltpu.SMEM(band_width.shape, jnp.int32),
        sem((copies,)), sem((copies,)), sem((7,)),
        pltpu.SemaphoreType.REGULAR((max(lon_n + mem_n - 2, lat_n - 1) - 1,)),
    ]
    hbm = pl.BlockSpec(memory_space=pltpu.HBM)
    kernel = functools.partial(paired, dims=(members, levels, lon_cells, lat_cells, sizes))
    ens = jax.ShapeDtypeStruct((members, levels, lon_cells, lat_cells), F32)
    static = jax.ShapeDtypeStruct((levels, lon_cells, lat_cells), F32)
    parts = pl.pallas_call(
        kernel,
        out_shape=[
            ens, ens,
            jax.ShapeDtypeStruct((2, levels, lon_cells, lat_cells), F32),
            jax.ShapeDtypeStruct((2, 128), F32),
        ],
        in_specs=[hbm] * 6,
        out_specs=[VMEM] * 4,
        scratch_shapes=scratch,
        compiler_params=pltpu.CompilerParams(
            collective_id=0, has_side_effects=True, vmem_limit_bytes=48 * 2**20
        ),
    )(*(
        pltpu.with_memory_space_constraint(x, pltpu.HBM)
        for x in (
            anomalies, spread, obs_index.reshape(1, -1), obs_weight.reshape(1, -1),
            innovation.reshape(1, -1), band_width,
        )
    ))
    return pl.pallas_call(
        combine,
        out_shape=[ens, static],
        in_specs=[VMEM] * 4,
        out_specs=[hbm] * 2,
        scratch_shapes=[
            v(ens.shape, F32), v(static.shape, F32), sem((members + 1,)),
        ],
        compiler_params=pltpu.CompilerParams(vmem_limit_bytes=8 * 2**20),
    )(*parts)


def pick(*args):
    members = args[0].shape[0]
    levels, lon_cells, lat_cells = args[1].shape
    lon_n, lat_n, mem_n = (lax.axis_size(a) for a in AXES)
    pairs = lon_n == 2 and members % 2 == 0 and levels == mem_n and lon_cells % 32 == 0 and lat_n > 2
    return (paired_device if pairs else per_device)(*args)


def solution(mesh):
    return jax.shard_map(
        pick,
        mesh=mesh,
        in_specs=(
            P("mem", None, "lon", "lat"),
            P(None, "lon", "lat"),
            P("lon", "lat", None),
            P("lon", "lat", None),
            P("lon", "lat", None),
            P(),
        ),
        out_specs=(P("mem", None, "lon", "lat"), P(None, "lon", "lat")),
        check_vma=False,
    )
```
